32 devices in a mesh: dp: 4 (over x, core), ctx: 4 (over z), mp: 2 (over y).
Axes of the slice: x: 2, y: 2, z: 4, core: 2. Of those that a mesh axis runs over, the one named last changes fastest.
Arguments:
- block_input: bfloat16 [8, 512, 2048], P('dp', 'ctx'), may hold values from -6 to 6
- doc_positions: int32 [8, 512], P('dp', 'ctx'), may hold values from 0 to 383, as said below
- out_cotangent: bfloat16 [8, 512, 2048], P('dp', 'ctx'), may hold values from -6 to 6
- attn_gain: bfloat16 [2048], P(('dp', 'ctx')), may hold values from 0.099609375 to 1.8984375
- mlp_gain: bfloat16 [2048], P(('dp', 'ctx')), may hold values from 0.099609375 to 1.8984375
- query_gain: bfloat16 [128], P(('dp', 'ctx')), may hold values from 0.099609375 to 1.8984375
- key_gain: bfloat16 [128], P(('dp', 'ctx')), may hold values from 0.099609375 to 1.8984375
- w_query: bfloat16 [2048, 2048], P(('dp', 'ctx'), 'mp'), may hold values from -0.125 to 0.125
- w_key: bfloat16 [2048, 1024], P(('dp', 'ctx'), 'mp'), may hold values from -0.125 to 0.125
- w_value: bfloat16 [2048, 1024], P(('dp', 'ctx'), 'mp'), may hold values from -0.125 to 0.125
- w_out: bfloat16 [2048, 2048], P('mp', ('dp', 'ctx')), may hold values from -2 to 2
- w_gate: bfloat16 [2048, 6144], P(('dp', 'ctx'), 'mp'), may hold values from -0.125 to 0.125
- w_up: bfloat16 [2048, 6144], P(('dp', 'ctx'), 'mp'), may hold values from -0.125 to 0.125
- w_down: bfloat16 [6144, 2048], P('mp', ('dp', 'ctx')), may hold values from -0.078125 to 0.078125
Outputs:
- block_output: bfloat16 [8, 512, 2048], P('dp', 'ctx')
- input_grad: float32 [8, 512, 2048], P('dp', 'ctx')
- attn_gain_grad: float32 [2048], P(('dp', 'ctx'))
- mlp_gain_grad: float32 [2048], P(('dp', 'ctx'))
- query_gain_grad: float32 [128], P(('dp', 'ctx'))
- key_gain_grad: float32 [128], P(('dp', 'ctx'))
- w_query_grad: float32 [2048, 2048], P(('dp', 'ctx'), 'mp')
- w_key_grad: float32 [2048, 1024], P(('dp', 'ctx'), 'mp')
- w_value_grad: float32 [2048, 1024], P(('dp', 'ctx'), 'mp')
- w_out_grad: float32 [2048, 2048], P('mp', ('dp', 'ctx'))
- w_gate_grad: float32 [2048, 6144], P(('dp', 'ctx'), 'mp')
- w_up_grad: float32 [2048, 6144], P(('dp', 'ctx'), 'mp')
- w_down_grad: float32 [6144, 2048], P('mp', ('dp', 'ctx'))
The draws below stay inside these ranges and needn't reach their ends.
Inputs may be any that keep to these rules, and one draw needn't show every extreme that they name: `doc_positions`: each sequence holds two documents: positions count up from 0 at its start and again from 0 at a boundary between 128 and 384; the first sequence's boundary is at 128.
All inputs are finite; a program needn't handle non-finite values.
Results may differ from the reference program's by a relative error of at most 0.019.
Values may be sent and summed in bfloat16 or wider, within the bound.
A program may use at most 256 MiB of HBM per device.

```python
import jax
import jax.numpy as jnp
from jax import lax

D = 2048
H = 16
KVH = 8
HD = 128
FF = 6144
TOK_CTX = 128
SEQS = 8
LEN = 512


def draw_doc_positions(key, part):
    boundary = jax.random.randint(key, (SEQS, 1), LEN // 4, 3 * LEN // 4 + 1)
    first_row = jnp.arange(SEQS, dtype=jnp.int32)[:, None] == 0
    boundary = jnp.where(first_row, LEN // 4, boundary).astype(jnp.int32)
    columns = jnp.arange(LEN, dtype=jnp.int32)[None, :]
    return jnp.where(columns < boundary, columns, columns - boundary).astype(jnp.int32)


def strengthened(result, rng, source, target, parts, factor):
    def block_of(position):
        return (jnp.arange(result.shape[position]) // (result.shape[position] // parts)).reshape((-1,) + (1,) * (result.ndim - 1 - position))

    one_side = jax.random.permutation(rng, parts)[block_of(target)]
    second = (block_of(target) + parts // 2) % parts
    return jnp.where((block_of(source) == one_side) | (block_of(source) == second), factor * result, result)


def block_scale(own_key, extent, shards, smallest, largest):
    level = 1.0
    for dim, shards_of in shards:
        draws = jax.random.uniform(jax.random.fold_in(jax.random.fold_in(own_key, 6), dim), (shards_of,), jnp.float32, smallest / len(shards), largest / len(shards))
        level = level * jnp.repeat(jnp.exp(draws), extent[dim] // shards_of).reshape((-1,) + (1,) * (len(extent) - 1 - dim))
    return level


def gaussian(own_key, dims, deviation, most, split=(), held_as=jnp.bfloat16):
    factor_of = block_scale(own_key, dims, split, -0.22, 0.18) if split else 1.0
    result = jax.random.normal(own_key, dims, jnp.float32) * deviation * factor_of
    return jnp.minimum(jnp.maximum(result, -most), most).astype(held_as)


def noise_with(stream_key, extent, deviation, most, pieces, heavy, kind=jnp.bfloat16):
    array = deviation * jax.random.normal(stream_key, extent, jnp.float32)
    if pieces:
        array = array * block_scale(stream_key, extent, pieces, -0.22, 0.18)
    return jnp.clip(strengthened(array, jax.random.fold_in(stream_key, 3), *heavy), -most, most).astype(kind)


def setup_inputs(seed: int = 0) -> dict:
    seeds = jax.random.split(jax.random.key(seed), 15)
    block_input = gaussian(seeds[0], (SEQS, LEN, D), 1.0, 6.0, ((0, 4), (1, 4)))
    doc_positions = draw_doc_positions(jax.random.fold_in(seeds[14], 71), 0)
    out_cotangent = noise_with(seeds[2], (SEQS, LEN, D), 1.0, 6.0, ((0, 4), (1, 4)), (1, 2, 4, 2.0))
    attn_gain = jnp.clip(1.0 + 0.18 * jax.random.normal(seeds[3], (D,), jnp.float32), 0.099609375, 1.8984375).astype(jnp.bfloat16)
    mlp_gain = jnp.clip(1.0 + 0.18 * jax.random.normal(seeds[4], (D,), jnp.float32), 0.099609375, 1.8984375).astype(jnp.bfloat16)
    query_gain = jnp.clip(1.0 + 0.18 * jax.random.normal(seeds[5], (HD,), jnp.float32), 0.099609375, 1.8984375).astype(jnp.bfloat16)
    key_gain = jnp.clip(1.0 + 0.18 * jax.random.normal(seeds[6], (HD,), jnp.float32), 0.099609375, 1.8984375).astype(jnp.bfloat16)
    w_query = gaussian(seeds[7], (D, H * HD), D ** -0.5, 0.125, ((0, 16), (1, 2)))
    w_key = gaussian(seeds[8], (D, KVH * HD), D ** -0.5, 0.125, ((0, 16), (1, 2)))
    w_value = gaussian(seeds[9], (D, KVH * HD), D ** -0.5, 0.125, ((0, 16), (1, 2)))
    w_out = gaussian(seeds[10], (H * HD, D), (max(H * HD // 256, 1)) ** -0.5, 2.0, ((0, 2), (1, 16)))
    w_gate = gaussian(seeds[11], (D, FF), D ** -0.5, 0.125, ((0, 16), (1, 2)))
    w_up = gaussian(seeds[12], (D, FF), D ** -0.5, 0.125, ((0, 16), (1, 2)))
    w_down = gaussian(seeds[13], (FF, D), FF ** -0.5, 0.078125, ((0, 2), (1, 16)))
    return {"block_input": block_input, "doc_positions": doc_positions, "out_cotangent": out_cotangent, "attn_gain": attn_gain, "mlp_gain": mlp_gain, "query_gain": query_gain, "key_gain": key_gain, "w_query": w_query, "w_key": w_key, "w_value": w_value, "w_out": w_out, "w_gate": w_gate, "w_up": w_up, "w_down": w_down}


eps_norm = 1e-06
rope_base = 1000000.0

def rms_scale(value_rows):
    return lax.rsqrt(lax.optimization_barrier(jnp.mean(value_rows * value_rows, axis=-1, keepdims=True)) + eps_norm)

def rope_tables(places, head_size):
    half_size = head_size // 2
    inverse = rope_base ** (-2.0 * jnp.arange(half_size).astype(jnp.float32) / head_size)
    angles = places.astype(jnp.float32)[:, None] * inverse[None, :]
    angles = jnp.concatenate([angles, angles], axis=-1)
    return (jnp.cos(angles), jnp.sin(angles))

def rotate(values, cosine, sine):
    half_size = values.shape[-1] // 2
    turned = jnp.concatenate([-values[..., half_size:], values[..., :half_size]], axis=-1)
    return values * cosine[:, None, :] + turned * sine[:, None, :]

def rotate_back(grads, cosine, sine):
    half_size = grads.shape[-1] // 2
    weighted = grads * sine[:, None, :]
    return grads * cosine[:, None, :] + jnp.concatenate([weighted[..., half_size:], -weighted[..., :half_size]], axis=-1)

def block_mask(query_index, lowest, key_index):
    return (key_index[None, :] <= query_index[:, None]) & (key_index[None, :] >= lowest[:, None])

def attention_forward(query_rot, key_rot, value_heads, places):
    length, head_count, head_size = query_rot.shape
    kv_count = key_rot.shape[1]
    group_size = head_count // kv_count
    scaling = head_size ** (-0.5)
    block_count = length // TOK_CTX
    keys_wide = key_rot.astype(jnp.float32)
    values_wide = value_heads.astype(jnp.float32)
    key_index = jnp.arange(length, dtype=jnp.int32)

    def one_block(block_id):
        start = block_id * TOK_CTX
        query_block = lax.dynamic_slice_in_dim(query_rot, start, TOK_CTX, 0).reshape(TOK_CTX, kv_count, group_size, head_size).astype(jnp.float32)
        place_block = lax.dynamic_slice_in_dim(places, start, TOK_CTX, 0)
        query_index = start + jnp.arange(TOK_CTX, dtype=jnp.int32)
        allowed = block_mask(query_index, query_index - place_block, key_index)
        scores = jnp.einsum('qkgd,jkd->kgqj', query_block, keys_wide) * scaling
        peak = lax.optimization_barrier(jnp.max(jnp.where(allowed, scores, -jnp.inf), axis=-1))
        probs = jnp.where(allowed, jnp.exp(scores - peak[..., None]), 0.0)
        total = lax.optimization_barrier(jnp.sum(probs, axis=-1))
        probs_half = lax.optimization_barrier(probs.astype(jnp.bfloat16)).astype(jnp.float32)
        running = jnp.einsum('kgqj,jkd->qkgd', probs_half, values_wide)
        rows_out = (running / jnp.transpose(total, (2, 0, 1))[..., None]).astype(jnp.bfloat16)
        return (rows_out.reshape(TOK_CTX, head_count * head_size), peak + jnp.log(total))
    outputs, log_total = lax.map(one_block, jnp.arange(block_count, dtype=jnp.int32))
    return (outputs.reshape(length, head_count * head_size), log_total)

def attention_backward(query_rot, key_rot, value_heads, places, attn_rows, attn_grad, log_total):
    length, head_count, head_size = query_rot.shape
    kv_count = key_rot.shape[1]
    group_size = head_count // kv_count
    scaling = head_size ** (-0.5)
    block_count = length // TOK_CTX
    keys_wide = key_rot.astype(jnp.float32)
    values_wide = value_heads.astype(jnp.float32)
    key_index = jnp.arange(length, dtype=jnp.int32)

    def one_block(carry, block_id):
        key_sum, value_sum = carry
        start = block_id * TOK_CTX
        query_block = lax.dynamic_slice_in_dim(query_rot, start, TOK_CTX, 0).reshape(TOK_CTX, kv_count, group_size, head_size).astype(jnp.float32)
        grad_block = lax.dynamic_slice_in_dim(attn_grad, start, TOK_CTX, 0).reshape(TOK_CTX, kv_count, group_size, head_size).astype(jnp.float32)
        rows_block = lax.dynamic_slice_in_dim(attn_rows, start, TOK_CTX, 0).reshape(TOK_CTX, kv_count, group_size, head_size).astype(jnp.float32)
        place_block = lax.dynamic_slice_in_dim(places, start, TOK_CTX, 0)
        query_index = start + jnp.arange(TOK_CTX, dtype=jnp.int32)
        allowed = block_mask(query_index, query_index - place_block, key_index)
        scores = jnp.einsum('qkgd,jkd->kgqj', query_block, keys_wide) * scaling
        probs = jnp.where(allowed, jnp.exp(scores - log_total[block_id][..., None]), 0.0)
        probs_half = lax.optimization_barrier(probs.astype(jnp.bfloat16)).astype(jnp.float32)
        value_sum = value_sum + jnp.einsum('kgqj,qkgd->jkd', probs_half, grad_block)
        prob_grad = jnp.einsum('qkgd,jkd->kgqj', grad_block, values_wide)
        row_dot = jnp.einsum('qkgd,qkgd->kgq', grad_block, rows_block)
        score_half = lax.optimization_barrier((probs * (prob_grad - row_dot[..., None])).astype(jnp.bfloat16)).astype(jnp.float32)
        query_part = jnp.einsum('kgqj,jkd->qkgd', score_half, keys_wide) * scaling
        key_sum = key_sum + jnp.einsum('kgqj,qkgd->jkd', score_half, query_block) * scaling
        return ((key_sum, value_sum), query_part.reshape(TOK_CTX, head_count, head_size))
    zero_rows = jnp.zeros((length, kv_count, head_size), jnp.float32)
    sums, query_parts = lax.scan(one_block, (zero_rows, zero_rows), jnp.arange(block_count, dtype=jnp.int32))
    return (query_parts.reshape(length, head_count, head_size), sums[0], sums[1])

def sequence_pass(inputs, places, cotangent, gain_list, weight_list):
    float_type = jnp.float32
    half_type = jnp.bfloat16
    gain_attn = gain_list[0].astype(float_type)
    gain_mlp = gain_list[1].astype(float_type)
    gain_query = gain_list[2].astype(float_type)
    gain_key = gain_list[3].astype(float_type)
    query_proj, key_proj, value_proj, out_proj, gate_proj, up_proj, down_proj = weight_list
    head_size = gain_query.shape[0]
    head_count = query_proj.shape[1] // head_size
    kv_count = key_proj.shape[1] // head_size
    length = inputs.shape[0]
    residual_in = inputs.astype(float_type)
    scale_attn = rms_scale(residual_in)
    normed_attn = residual_in * scale_attn
    attn_input = (normed_attn * gain_attn).astype(half_type)
    query_raw = jnp.dot(attn_input, query_proj, preferred_element_type=float_type).reshape(length, head_count, head_size)
    key_raw = jnp.dot(attn_input, key_proj, preferred_element_type=float_type).reshape(length, kv_count, head_size)
    value_rows = jnp.dot(attn_input, value_proj, preferred_element_type=float_type).astype(half_type)
    query_scale = rms_scale(query_raw)
    query_normed = query_raw * query_scale
    key_scale = rms_scale(key_raw)
    key_normed = key_raw * key_scale
    cosine, sine = rope_tables(places, head_size)
    query_rot = rotate(query_normed * gain_query, cosine, sine).astype(half_type)
    key_rot = rotate(key_normed * gain_key, cosine, sine).astype(half_type)
    value_heads = value_rows.reshape(length, kv_count, head_size)
    attn_rows, log_total = attention_forward(query_rot, key_rot, value_heads, places)
    middle = residual_in + jnp.dot(attn_rows, out_proj, preferred_element_type=float_type)
    scale_mlp = rms_scale(middle)
    normed_mlp = middle * scale_mlp
    mlp_input = (normed_mlp * gain_mlp).astype(half_type)
    gate_rows = jnp.dot(mlp_input, gate_proj, preferred_element_type=float_type)
    up_rows = jnp.dot(mlp_input, up_proj, preferred_element_type=float_type)
    sigmoid_gate = jax.nn.sigmoid(gate_rows)
    hidden_rows = (gate_rows * sigmoid_gate * up_rows).astype(half_type)
    block_output = (middle + jnp.dot(hidden_rows, down_proj, preferred_element_type=float_type)).astype(half_type)
    down_grad = jnp.dot(hidden_rows.T, cotangent, preferred_element_type=float_type)
    hidden_grad = jnp.dot(cotangent, down_proj.T, preferred_element_type=float_type)
    gate_grad = (hidden_grad * up_rows * sigmoid_gate * (1.0 + gate_rows * (1.0 - sigmoid_gate))).astype(half_type)
    up_grad = (hidden_grad * gate_rows * sigmoid_gate).astype(half_type)
    gate_proj_grad = jnp.dot(mlp_input.T, gate_grad, preferred_element_type=float_type)
    up_proj_grad = jnp.dot(mlp_input.T, up_grad, preferred_element_type=float_type)
    mlp_in_grad = jnp.dot(gate_grad, gate_proj.T, preferred_element_type=float_type) + jnp.dot(up_grad, up_proj.T, preferred_element_type=float_type)
    mlp_gain_grad = lax.optimization_barrier(jnp.sum(mlp_in_grad * normed_mlp, axis=0))
    normed_grad = mlp_in_grad * gain_mlp
    middle_grad = cotangent.astype(float_type) + scale_mlp * (normed_grad - normed_mlp * lax.optimization_barrier(jnp.mean(normed_grad * normed_mlp, axis=-1, keepdims=True)))
    middle_half = middle_grad.astype(half_type)
    out_proj_grad = jnp.dot(attn_rows.T, middle_half, preferred_element_type=float_type)
    attn_grad = jnp.dot(middle_half, out_proj.T, preferred_element_type=float_type).astype(half_type)
    query_grad, key_rot_grad, value_grad = attention_backward(query_rot, key_rot, value_heads, places, attn_rows, attn_grad, log_total)
    value_half = value_grad.reshape(length, kv_count * head_size).astype(half_type)
    query_back = rotate_back(query_grad, cosine, sine)
    key_back = rotate_back(key_rot_grad, cosine, sine)
    query_gain_grad = lax.optimization_barrier(jnp.sum(query_back * query_normed, axis=(0, 1)))
    key_gain_grad = lax.optimization_barrier(jnp.sum(key_back * key_normed, axis=(0, 1)))
    query_ngrad = query_back * gain_query
    key_ngrad = key_back * gain_key
    query_half = (query_scale * (query_ngrad - query_normed * lax.optimization_barrier(jnp.mean(query_ngrad * query_normed, axis=-1, keepdims=True)))).reshape(length, head_count * head_size).astype(half_type)
    key_half = (key_scale * (key_ngrad - key_normed * lax.optimization_barrier(jnp.mean(key_ngrad * key_normed, axis=-1, keepdims=True)))).reshape(length, kv_count * head_size).astype(half_type)
    query_proj_grad = jnp.dot(attn_input.T, query_half, preferred_element_type=float_type)
    key_proj_grad = jnp.dot(attn_input.T, key_half, preferred_element_type=float_type)
    value_proj_grad = jnp.dot(attn_input.T, value_half, preferred_element_type=float_type)
    attn_in_grad = jnp.dot(query_half, query_proj.T, preferred_element_type=float_type) + jnp.dot(key_half, key_proj.T, preferred_element_type=float_type) + jnp.dot(value_half, value_proj.T, preferred_element_type=float_type)
    attn_gain_grad = lax.optimization_barrier(jnp.sum(attn_in_grad * normed_attn, axis=0))
    normed_in_grad = attn_in_grad * gain_attn
    input_grad = middle_grad + scale_attn * (normed_in_grad - normed_attn * lax.optimization_barrier(jnp.mean(normed_in_grad * normed_attn, axis=-1, keepdims=True)))
    grads = (attn_gain_grad, mlp_gain_grad, query_gain_grad, key_gain_grad, query_proj_grad, key_proj_grad, value_proj_grad, out_proj_grad, gate_proj_grad, up_proj_grad, down_grad)
    return (block_output, input_grad, grads)

def reference(block_input, doc_positions, out_cotangent, attn_gain, mlp_gain, query_gain, key_gain, w_query, w_key, w_value, w_out, w_gate, w_up, w_down):
    gain_list = (attn_gain, mlp_gain, query_gain, key_gain)
    weight_list = (w_query, w_key, w_value, w_out, w_gate, w_up, w_down)
    zero_grads = tuple((jnp.zeros(entry.shape, jnp.float32) for entry in gain_list + weight_list))

    def one_sequence(carry, inputs):
        output_rows, input_rows, addition = sequence_pass(inputs[0], inputs[1], inputs[2], gain_list, weight_list)
        return (tuple((earlier + later for earlier, later in zip(carry, addition))), (output_rows, input_rows))
    totals, stacked = lax.scan(one_sequence, zero_grads, (block_input, doc_positions, out_cotangent))
    return (stacked[0], stacked[1], totals[0], totals[1], totals[2], totals[3], totals[4], totals[5], totals[6], totals[7], totals[8], totals[9], totals[10])
```

```python
import functools

import jax
import jax.numpy as jnp
from jax import lax
from jax.experimental import pallas as pl
from jax.experimental.pallas import tpu as pltpu
from jax.sharding import PartitionSpec as P

eps_norm = 1e-06
rope_base = 1000000.0
MESH = pl.DeviceIdType.MESH
f32 = jnp.float32
bf16 = jnp.bfloat16
PIECES = ((0, 0), (0, 1), (1, 0), (1, 1))


def flip(value, bit):
    return 1 - value if bit else value


def place():
    dp = lax.axis_index("dp")
    ctx = lax.axis_index("ctx")
    return {
        "dp": dp,
        "ctx": ctx,
        "y": lax.axis_index("mp"),
        "x": dp // 2,
        "c": dp % 2,
        "zh": ctx // 2,
        "zl": ctx % 2,
    }


def run_start(at, dx, dzh, dc, ctx_count, block):
    start = ((flip(at["x"], dx) * 2 + flip(at["c"], dc)) * ctx_count + flip(at["zh"], dzh) * 2) * block
    return pl.multiple_of(start, 2 * block)


def load_runs(at, pieces, target, sems, ctx_count, block, by_rows):
    copies = []
    for n, (dx, dzh) in enumerate(PIECES):
        for dc in (0, 1):
            run = pl.ds(run_start(at, dx, dzh, dc, ctx_count, block), 2 * block)
            spot = target.at[run] if by_rows else target.at[:, run]
            copy = pltpu.make_async_copy(pieces[n].at[dc], spot, sems.at[2 * n + dc])
            copy.start()
            copies.append(copy)
    return copies


def finish(copies):
    for copy in copies:
        copy.wait()


def nn(left, right):
    return lax.dot_general(left, right, (((1,), (0,)), ((), ())), preferred_element_type=f32)


def nt(left, right):
    return lax.dot_general(left, right, (((1,), (1,)), ((), ())), preferred_element_type=f32)


def tn(left, right):
    return lax.dot_general(left, right, (((0,), (0,)), ((), ())), preferred_element_type=f32)


def root_scale(values):
    return lax.rsqrt(jnp.mean(values * values, axis=-1, keepdims=True) + eps_norm)


def turn(values, cosine, sine):
    return values * cosine + pltpu.roll(values, values.shape[-1] // 2, 1) * sine


def turn_back(values, cosine, sine):
    return values * cosine + pltpu.roll(values * sine, values.shape[-1] // 2, 1)


def qkv_kernel(ctx_count, block, x0, x1, x2, x3, gain, cosine, sine, gain_q, gain_k, w0, w1, w2, w3,
               a_ref, raw_ref, q_ref, kv_ref, weight, sems):
    at = place()
    copies = load_runs(at, (w0, w1, w2, w3), weight, sems, ctx_count, block, True)
    rows = x0.shape[0]
    head = gain_q.shape[1]
    q_width = q_ref.shape[1]
    for n, x_ref in enumerate((x0, x1, x2, x3)):
        wide = x_ref[...].astype(f32)
        a_ref[pl.ds(n * rows, rows), :] = (wide * root_scale(wide) * gain[...]).astype(bf16)
    finish(copies)

    @pl.loop(0, 4)
    def _(n):
        span = pl.ds(pl.multiple_of(n * rows, rows), rows)
        raw = nn(a_ref[span, :], weight[...])
        raw_ref[span, :] = raw[:, : q_width + head]
        cos = cosine[span, :]
        sin = sine[span, :]
        for h in range(q_width // head):
            u = raw[:, h * head : (h + 1) * head]
            q_ref[span, pl.ds(h * head, head)] = turn(u * root_scale(u) * gain_q[...], cos, sin).astype(bf16)
        u = raw[:, q_width : q_width + head]
        kv_ref[span, pl.ds(0, head)] = turn(u * root_scale(u) * gain_k[...], cos, sin).astype(bf16)
        kv_ref[span, pl.ds(head, head)] = raw[:, q_width + head :].astype(bf16)


def pair_rows(ref, base, part, span):
    far = base + 2 * part
    return jnp.concatenate(
        [ref[pl.ds(base, part), :][:, span[0] : span[1]], ref[pl.ds(far, part), :][:, span[0] : span[1]]], axis=0
    )


def allowed_pairs(at, base, part, heads, pos_ref):
    def fold(index, size, times):
        for n in range(times - 1, 0, -1):
            index = jnp.where(index >= n * size, index - n * size, index)
        return index

    row = lax.broadcasted_iota(jnp.int32, (heads * 2 * part, 4 * part), 0)
    col = lax.broadcasted_iota(jnp.int32, (heads * 2 * part, 4 * part), 1)
    near = at["zl"] * part
    far = (1 - at["zl"]) * part
    row = fold(row, 2 * part, heads)
    query = jnp.where(row < part, row + near, row - part + far) + at["zh"] * 2 * part
    inner = fold(col, 2 * part, 2)
    key = jnp.where(inner < part, inner + near, inner - part + far)
    key = key + jnp.where(col < 2 * part, at["zh"], 1 - at["zh"]) * (2 * part)
    spot = jnp.concatenate([pos_ref[pl.ds(base, part), :], pos_ref[pl.ds(base + 2 * part, part), :]], axis=0)
    spot = jnp.concatenate([spot] * heads, axis=0)[:, :1]
    return (key <= query) & (key >= query - spot)


def stack_heads(ref, base, part, head):
    heads = ref.shape[1] // head
    return jnp.concatenate([pair_rows(ref, base, part, (h * head, (h + 1) * head)) for h in range(heads)], axis=0)


def unstack(ref, base, part, head, values):
    heads = ref.shape[1] // head
    for h in range(heads):
        top = 2 * part * h
        ref[pl.ds(base, part), pl.ds(h * head, head)] = values[top : top + part].astype(ref.dtype)
        ref[pl.ds(base + 2 * part, part), pl.ds(h * head, head)] = values[top + part : top + 2 * part].astype(ref.dtype)


def attend_kernel(ctx_count, block, part, head, q_ref, kv_ref, kvp_ref, pos_ref, w0, w1, w2, w3,
                  o_ref, lse_ref, out_ref, weight, sems):
    at = place()
    copies = load_runs(at, (w0, w1, w2, w3), weight, sems, ctx_count, block, False)
    heads = q_ref.shape[1] // head
    scaling = head ** (-0.5)

    @pl.loop(0, 2)
    def _(n):
      @pl.loop(0, 2)
      def _(m):
        base = pl.multiple_of(n * (4 * part) + m * part, part)
        q = stack_heads(q_ref, base, part, head)
        k = jnp.concatenate(
            [pair_rows(kv_ref, base, part, (0, head)), pair_rows(kvp_ref, base, part, (0, head))], axis=0
        )
        v = jnp.concatenate(
            [pair_rows(kv_ref, base, part, (head, 2 * head)), pair_rows(kvp_ref, base, part, (head, 2 * head))], axis=0
        )
        allowed = allowed_pairs(at, base, part, heads, pos_ref)
        scores = jnp.where(allowed, nt(q, k) * scaling, -jnp.inf)
        peak = jnp.max(scores, axis=-1, keepdims=True)
        weights = jnp.exp(scores - peak)
        total = jnp.sum(weights, axis=-1, keepdims=True)
        o = nn(weights.astype(bf16), v) / total
        unstack(o_ref, base, part, head, o)
        unstack(lse_ref, base, part, head, jnp.broadcast_to(peak + jnp.log(total), o.shape))

    finish(copies)

    @pl.loop(0, 4)
    def _(n):
        span = pl.ds(pl.multiple_of(n * 2 * part, 2 * part), 2 * part)
        out_ref[span, :] = nn(o_ref[span, :], weight[...]).astype(bf16)


def gate_kernel(ctx_count, block, b_ref, w0, w1, w2, w3, z_ref, gu_ref, weight, sems):
    at = place()
    finish(load_runs(at, (w0, w1, w2, w3), weight, sems, ctx_count, block, True))
    hidden = z_ref.shape[1]
    rows = 256

    @pl.loop(0, b_ref.shape[0] // rows)
    def _(n):
        span = pl.ds(pl.multiple_of(n * rows, rows), rows)
        b = b_ref[span, :]
        g = nn(b, weight[:, :hidden])
        gu_ref[span, pl.ds(0, hidden)] = g
        u = nn(b, weight[:, hidden:])
        gu_ref[span, pl.ds(hidden, hidden)] = u
        z_ref[span, :] = (g * jax.nn.sigmoid(g) * u).astype(bf16)


def grad_cols_kernel(ctx_count, block, left_ref, r0, r1, r2, r3, q0, q1, q2, q3):
    at = place()
    rows = r0.shape[0]
    for n, (dx, dzh) in enumerate(PIECES):
        for dc in (0, 1):
            run = pl.ds(run_start(at, dx, dzh, dc, ctx_count, block), 2 * block)
            total = tn(left_ref[pl.ds(0, rows), :], r0[:, run])
            for m, right in ((1, r1), (2, r2), (3, r3)):
                total = total + tn(left_ref[pl.ds(m * rows, rows), :], right[:, run])
            (q0, q1, q2, q3)[n][dc] = total.astype(bf16)


def grad_rows_kernel(ctx_count, block, left_ref, right_ref, q0, q1, q2, q3):
    at = place()
    for n, (dx, dzh) in enumerate(PIECES):
        for dc in (0, 1):
            run = pl.ds(run_start(at, dx, dzh, dc, ctx_count, block), 2 * block)
            (q0, q1, q2, q3)[n][dc] = tn(left_ref[:, run], right_ref[...]).astype(bf16)


def grad_wide_kernel(ctx_count, block, left_ref, right_ref, q0, q1, q2, q3):
    at = place()
    for n, (dx, dzh) in enumerate(PIECES):
        for dc in (0, 1):
            run = pl.ds(run_start(at, dx, dzh, dc, ctx_count, block), 2 * block)
            (q0, q1, q2, q3)[n][dc] = tn(left_ref[...], right_ref[:, run]).astype(bf16)


def gate_back_kernel(ctx_count, block, c0, c1, c2, c3, gu_ref, d0, d1, d2, d3, w0, w1, w2, w3,
                     dgu_ref, part_ref, down, weight, sems):
    at = place()
    first = load_runs(at, (d0, d1, d2, d3), down, sems.at[0], ctx_count, block, False)
    second = load_runs(at, (w0, w1, w2, w3), weight, sems.at[1], ctx_count, block, True)
    rows = c0.shape[0]
    hidden = down.shape[0]
    finish(first)
    for n, c_ref in enumerate((c0, c1, c2, c3)):
        span = pl.ds(n * rows, rows)
        dz = nt(c_ref[...], down[...])
        g = gu_ref[span, pl.ds(0, hidden)]
        u = gu_ref[span, pl.ds(hidden, hidden)]
        s = jax.nn.sigmoid(g)
        dgu_ref[span, pl.ds(0, hidden)] = (dz * u * s * (1.0 + g * (1.0 - s))).astype(bf16)
        dgu_ref[span, pl.ds(hidden, hidden)] = (dz * g * s).astype(bf16)
    finish(second)

    @pl.loop(0, 4)
    def _(n):
        span = pl.ds(pl.multiple_of(n * rows, rows), rows)
        part_ref[span, :] = nt(dgu_ref[span, :], weight[...]).astype(bf16)


def down_kernel(ctx_count, block, z_ref, d0, d1, d2, d3, part_ref, down, sems):
    at = place()
    finish(load_runs(at, (d0, d1, d2, d3), down, sems, ctx_count, block, False))
    rows = 256

    @pl.loop(0, z_ref.shape[0] // rows)
    def _(n):
        span = pl.ds(pl.multiple_of(n * rows, rows), rows)
        part_ref[span, :] = nn(z_ref[span, :], down[...]).astype(bf16)


def attend_back_kernel(ctx_count, block, part, head, dh_ref, o_ref, q_ref, kv_ref, kvp_ref, lse_ref, pos_ref,
                       w0, w1, w2, w3, dq_ref, dkv_ref, dkvp_ref, weight, do_ref, sems):
    at = place()
    finish(load_runs(at, (w0, w1, w2, w3), weight, sems, ctx_count, block, False))
    heads = q_ref.shape[1] // head
    scaling = head ** (-0.5)

    @pl.loop(0, 4)
    def _(n):
        span = pl.ds(pl.multiple_of(n * 2 * part, 2 * part), 2 * part)
        do_ref[span, :] = nt(dh_ref[span, :], weight[...]).astype(bf16)

    @pl.loop(0, 2)
    def _(n):
      @pl.loop(0, 2)
      def _(m):
        base = pl.multiple_of(n * (4 * part) + m * part, part)
        q = stack_heads(q_ref, base, part, head)
        o = stack_heads(o_ref, base, part, head)
        do = stack_heads(do_ref, base, part, head)
        lse = stack_heads(lse_ref, base, part, head)[:, :1]
        k = jnp.concatenate(
            [pair_rows(kv_ref, base, part, (0, head)), pair_rows(kvp_ref, base, part, (0, head))], axis=0
        )
        v = jnp.concatenate(
            [pair_rows(kv_ref, base, part, (head, 2 * head)), pair_rows(kvp_ref, base, part, (head, 2 * head))], axis=0
        )
        allowed = allowed_pairs(at, base, part, heads, pos_ref)
        probs = jnp.where(allowed, jnp.exp(jnp.where(allowed, nt(q, k) * scaling - lse, 0.0)), 0.0)
        dv = tn(probs.astype(bf16), do)
        row_dot = jnp.sum(do.astype(f32) * o.astype(f32), axis=-1, keepdims=True)
        ds = (probs * (nt(do, v) - row_dot)).astype(bf16)
        unstack(dq_ref, base, part, head, nn(ds, k) * scaling)
        dk = tn(ds, q) * scaling
        for ref, top in ((dkv_ref, 0), (dkvp_ref, 2 * part)):
            for m in (0, 1):
                spot = pl.ds(base + m * 2 * part, part)
                low = top + m * part
                ref[spot, pl.ds(0, head)] = dk[low : low + part].astype(ref.dtype)
                ref[spot, pl.ds(head, head)] = dv[low : low + part].astype(ref.dtype)


def qkv_back_kernel(ctx_count, block, dq_ref, dkv_ref, got_ref, raw_ref, cosine, sine, gain_q, gain_k, w0, w1, w2, w3,
                    dqkv_ref, part_ref, gq_ref, gk_ref, weight, sems):
    at = place()
    copies = load_runs(at, (w0, w1, w2, w3), weight, sems, ctx_count, block, True)
    head = gain_q.shape[1]
    q_width = dq_ref.shape[1]
    rows = 256
    gq_ref[...] = jnp.zeros_like(gq_ref)
    gk_ref[...] = jnp.zeros_like(gk_ref)

    def through(u, w, gain, total_ref, cos, sin):
        r = root_scale(u)
        n = u * r
        e = turn_back(w, cos, sin)
        total_ref[...] += jnp.sum(e * n, axis=0, keepdims=True)
        f = e * gain
        return (r * (f - n * jnp.mean(f * n, axis=-1, keepdims=True))).astype(bf16)

    @pl.loop(0, dq_ref.shape[0] // rows)
    def _(n):
        span = pl.ds(pl.multiple_of(n * rows, rows), rows)
        cos = cosine[span, :]
        sin = sine[span, :]
        for h in range(q_width // head):
            cols = pl.ds(h * head, head)
            dqkv_ref[span, cols] = through(raw_ref[span, cols], dq_ref[span, cols], gain_q[...], gq_ref, cos, sin)
        dk = dkv_ref[span, pl.ds(0, head)] + got_ref[span, pl.ds(0, head)].astype(f32)
        dv = dkv_ref[span, pl.ds(head, head)] + got_ref[span, pl.ds(head, head)].astype(f32)
        cols = pl.ds(q_width, head)
        dqkv_ref[span, cols] = through(raw_ref[span, cols], dk, gain_k[...], gk_ref, cos, sin)
        dqkv_ref[span, pl.ds(q_width + head, head)] = dv.astype(bf16)

    finish(copies)

    @pl.loop(0, dq_ref.shape[0] // rows)
    def _(n):
        span = pl.ds(pl.multiple_of(n * rows, rows), rows)
        part_ref[span, :] = nt(dqkv_ref[span, :], weight[...]).astype(bf16)


def partners(at):
    return (
        {"dp": at["dp"] + 1 - 2 * at["c"]},
        {"ctx": at["ctx"] + 1 - 2 * at["zl"]},
        {"mp": 1 - at["y"]},
    )


def meet(at):
    barrier = pltpu.get_barrier_semaphore()
    for device in partners(at):
        pl.semaphore_signal(barrier, inc=1, device_id=device, device_id_type=MESH)
    pl.semaphore_wait(barrier, 3)


def sender(send, recv):
    def start(source, target, number, device):
        copy = pltpu.make_async_remote_copy(
            src_ref=source,
            dst_ref=target,
            send_sem=send.at[number],
            recv_sem=recv.at[number],
            device_id=device,
            device_id_type=MESH,
        )
        copy.start()
        return copy

    return start


def sum_group(at, part, from_core, kept, second, from_z, from_y, last, start):
    core, low, across = partners(at)
    half = part.shape[2] // 2
    a, b = pl.ds(0, half), pl.ds(half, half)
    first = {k: start(part.at[4 + k], from_core.at[k], k, core) for k in (3, 1, 2, 0)}

    def total(k):
        first[k].wait_recv()
        return part[k].astype(f32) + from_core[k].astype(f32)

    kept[2] = total(3).astype(bf16)
    z1 = start(kept.at[2, :, a], from_z.at[1], 4, low)
    y1 = start(kept.at[2, :, b], from_y.at[1], 5, across)
    kept[0] = total(1).astype(bf16)
    y0 = start(kept.at[0, :, b], from_y.at[0], 6, across)
    kept[1] = total(2).astype(bf16)
    z0 = start(kept.at[1, :, a], from_z.at[0], 7, low)
    z1.wait_recv()
    second[0] = (kept[0, :, a].astype(f32) + from_z[1].astype(f32)).astype(bf16)
    y2 = start(second.at[0], last.at[0], 8, across)
    y1.wait_recv()
    second[1] = (kept[1, :, b].astype(f32) + from_y[1].astype(f32)).astype(bf16)
    z2 = start(second.at[1], last.at[1], 9, low)
    mine = total(0)
    z0.wait_recv()
    y0.wait_recv()
    y2.wait_recv()
    z2.wait_recv()
    left = mine[:, :half] + from_z[0].astype(f32) + last[0].astype(f32)
    right = mine[:, half:] + from_y[0].astype(f32) + last[1].astype(f32)
    for copy in (*first.values(), z1, y1, y0, z0, y2, z2):
        copy.wait_send()
    return jnp.concatenate([left, right], axis=1)


def spread_group(at, out, start):
    core, low, across = partners(at)
    half = out.shape[2] // 2
    a, b = pl.ds(0, half), pl.ds(half, half)
    ya = start(out.at[0, :, a], out.at[1, :, a], 10, across)
    zb = start(out.at[0, :, b], out.at[2, :, b], 11, low)
    yb = start(out.at[0, :, b], out.at[1, :, b], 12, across)
    za = start(out.at[0, :, a], out.at[2, :, a], 13, low)
    c0 = start(out.at[0], out.at[4], 14, core)
    ya.wait_recv()
    zc = start(out.at[1, :, a], out.at[3, :, a], 15, low)
    zb.wait_recv()
    yc = start(out.at[2, :, b], out.at[3, :, b], 16, across)
    yb.wait_recv()
    c1 = start(out.at[1], out.at[5], 17, core)
    za.wait_recv()
    c2 = start(out.at[2], out.at[6], 18, core)
    zc.wait_recv()
    yc.wait_recv()
    c3 = start(out.at[3], out.at[7], 19, core)
    for copy in (c0, c1, c2, c3):
        copy.wait_recv()
    for copy in (ya, zb, yb, za, c0, zc, yc, c1, c2, c3):
        copy.wait_send()


def sum_spread_kernel(part, x_ref, gain, h_ref, out, from_core, kept, second, from_z, from_y, last, send, recv):
    at = place()
    meet(at)
    start = sender(send, recv)
    h = x_ref[...].astype(f32) + sum_group(at, part, from_core, kept, second, from_z, from_y, last, start)
    h_ref[...] = h
    out[0] = (h * root_scale(h) * gain[...]).astype(bf16)
    spread_group(at, out, start)


def sum_spread_back_kernel(part, h_ref, c_ref, gain, dh_ref, out, grad_ref,
                           from_core, kept, second, from_z, from_y, last, send, recv):
    at = place()
    meet(at)
    start = sender(send, recv)
    db = sum_group(at, part, from_core, kept, second, from_z, from_y, last, start)
    h = h_ref[...]
    r = root_scale(h)
    n = h * r
    grad_ref[...] = jnp.sum(db * n, axis=0, keepdims=True)
    t = db * gain[...]
    dh = c_ref[...].astype(f32) + r * (t - n * jnp.mean(t * n, axis=-1, keepdims=True))
    dh_ref[...] = dh
    out[0] = dh.astype(bf16)
    spread_group(at, out, start)


def sum_out_kernel(part, h_ref, out_ref, from_core, kept, second, from_z, from_y, last, send, recv):
    at = place()
    meet(at)
    start = sender(send, recv)
    total = sum_group(at, part, from_core, kept, second, from_z, from_y, last, start)
    out_ref[...] = (h_ref[...] + total).astype(bf16)


def sum_in_kernel(part, dh_ref, x_ref, gain, out_ref, grad_ref,
                  from_core, kept, second, from_z, from_y, last, send, recv):
    at = place()
    meet(at)
    start = sender(send, recv)
    da = sum_group(at, part, from_core, kept, second, from_z, from_y, last, start)
    wide = x_ref[...].astype(f32)
    r = root_scale(wide)
    n = wide * r
    grad_ref[...] = jnp.sum(da * n, axis=0, keepdims=True)
    f = da * gain[...]
    out_ref[...] = (dh_ref[...] + r * (f - n * jnp.mean(f * n, axis=-1, keepdims=True))).astype(bf16)


VM = pl.BlockSpec(memory_space=pltpu.VMEM)
HB = pl.BlockSpec(memory_space=pl.ANY)


def shaped(shape, dtype):
    return jax.ShapeDtypeStruct(shape, dtype)


def local_call(kernel, outs, args, specs, scratch=()):
    return pl.pallas_call(
        kernel,
        out_shape=tuple(outs),
        in_specs=list(specs),
        out_specs=tuple(VM for _ in outs),
        scratch_shapes=list(scratch),
        compiler_params=pltpu.CompilerParams(vmem_limit_bytes=60 * 1024 * 1024),
    )(*args)


def group_call(kernel, number, outs, args, part, width, copies):
    half = width // 2
    return pl.pallas_call(
        kernel,
        out_shape=tuple(outs),
        in_specs=[VM for _ in args],
        out_specs=tuple(VM for _ in outs),
        scratch_shapes=[
            pltpu.VMEM((4, part, width), bf16),
            pltpu.VMEM((3, part, width), bf16),
            pltpu.VMEM((2, part, half), bf16),
            pltpu.VMEM((2, part, half), bf16),
            pltpu.VMEM((2, part, half), bf16),
            pltpu.VMEM((2, part, half), bf16),
            pltpu.SemaphoreType.DMA((copies,)),
            pltpu.SemaphoreType.DMA((copies,)),
        ],
        compiler_params=pltpu.CompilerParams(
            collective_id=number, has_side_effects=True, vmem_limit_bytes=60 * 1024 * 1024
        ),
    )(*args)


def split_device(
    block_input, doc_positions, out_cotangent, attn_gain, mlp_gain, query_gain, key_gain,
    w_query, w_key, w_value, w_out, w_gate, w_up, w_down,
):
    dp_count = lax.axis_size("dp")
    ctx_count = lax.axis_size("ctx")
    rank_count = dp_count * ctx_count
    ZL, ZH, C, X = 1, 2, ctx_count, 2 * ctx_count
    at = place()
    rank = at["dp"] * ctx_count + at["ctx"]
    slot = at["c"] * 2 + at["zl"]
    upper = at["y"] == 1
    zl_on = at["zl"] == 1
    c_on = at["c"] == 1
    seqs, part, width = block_input.shape
    block = attn_gain.shape[0]
    head_piece = query_gain.shape[0]
    head = head_piece * rank_count
    masks = (0, ZL, C, C | ZL)

    def swap(value, mask):
        return lax.ppermute(value, ("dp", "ctx"), [(i, i ^ mask) for i in range(rank_count)])

    def swap_y(value):
        return lax.ppermute(value, "mp", [(0, 1), (1, 0)])

    def tie(value, after):
        return lax.optimization_barrier((value, after))[0]

    def group_slices(slices):
        sent = [lax.dynamic_index_in_dim(slices, slot ^ k, 0, keepdims=False) for k in range(4)]
        return [sent[0]] + [swap(sent[k], masks[k]) for k in (1, 2, 3)]

    def make_piece(got, axis):
        runs = []
        for dc in (0, 1):
            near, far = got[2 * dc], got[2 * dc + 1]
            runs.append(jnp.concatenate([jnp.where(zl_on, far, near), jnp.where(zl_on, near, far)], axis=axis))
        return jnp.stack(runs)

    def all_pieces(piece):
        over_z = swap(piece, ZH)
        over_x = swap(piece, X)
        return (piece, over_z, over_x, swap(over_z, X))

    def cut_cols(array):
        return array.reshape(array.shape[0], 4, array.shape[1] // 4).transpose(1, 0, 2)

    def cut_rows(array):
        return array.reshape(4, array.shape[0] // 4, array.shape[1])

    own_x = jnp.where(upper, block_input[::-1], block_input)
    own_c = jnp.where(upper, out_cotangent[::-1], out_cotangent)
    own_p = jnp.where(upper, doc_positions[::-1], doc_positions)

    def group_tokens(own):
        far = swap(own, ZL)
        return (own, far, swap(own, C), swap(far, C))

    slices_qkv = jnp.concatenate([cut_cols(w_query), cut_cols(w_key), cut_cols(w_value)], axis=2)
    got_qkv = group_slices(slices_qkv)
    gains = jnp.stack(
        [
            attn_gain,
            mlp_gain,
            jnp.pad(query_gain, (0, block - head_piece)),
            jnp.pad(key_gain, (0, block - head_piece)),
        ]
    )[None]
    for mask in (ZL, ZH, C, X):
        gains = jnp.concatenate([gains, swap(gains, mask)], axis=0)
    gains = jnp.take(gains, jnp.arange(rank_count) ^ rank, axis=0).astype(f32)
    gain_attn = gains[:, 0].reshape(1, width)
    gain_mlp = gains[:, 1].reshape(1, width)
    gain_q = gains[:, 2, :head_piece].reshape(1, head)
    gain_k = gains[:, 3, :head_piece].reshape(1, head)

    xs = [t.reshape(seqs * part, width) for t in group_tokens(own_x)]
    spots = jnp.concatenate([t.reshape(seqs * part) for t in group_tokens(own_p)])
    pieces_qkv = all_pieces(make_piece(got_qkv, 0))

    inverse = rope_base ** (-2.0 * jnp.arange(head // 2).astype(f32) / head)
    angles = spots.astype(f32)[:, None] * inverse[None, :]
    cos_half, sin_half = jnp.cos(angles), jnp.sin(angles)
    cosine = jnp.concatenate([cos_half, cos_half], axis=1)
    sine = jnp.concatenate([-sin_half, sin_half], axis=1)
    spots = jnp.broadcast_to(spots[:, None], (spots.shape[0], 128))

    after = (pieces_qkv[3],)
    slices_out = tie(cut_rows(w_out), after)
    slices_gate = jnp.concatenate([cut_cols(w_gate), cut_cols(w_up)], axis=2)
    slices_gate = tie(slices_gate, after)
    slices_down = tie(cut_rows(w_down), after)
    pieces_out = all_pieces(make_piece(group_slices(slices_out), 1))
    pieces_gate = all_pieces(make_piece(group_slices(slices_gate), 0))
    pieces_down = all_pieces(make_piece(group_slices(slices_down), 1))
    cs = [t.reshape(seqs * part, width) for t in group_tokens(tie(own_c, after))]

    tokens = 4 * seqs * part
    q_width = w_query.shape[1] // 4
    hidden = w_gate.shape[1] // 4
    eight = pltpu.SemaphoreType.DMA((8,))
    bound = functools.partial

    a, raw, q, kv = local_call(
        bound(qkv_kernel, ctx_count, block),
        [
            shaped((tokens, width), bf16),
            shaped((tokens, q_width + head), f32),
            shaped((tokens, q_width), bf16),
            shaped((tokens, 2 * head), bf16),
        ],
        (*xs, gain_attn, cosine, sine, gain_q, gain_k, *pieces_qkv),
        [VM] * 9 + [HB] * 4,
        [pltpu.VMEM((width, q_width + 2 * head), bf16), eight],
    )
    kvp = swap(kv, ZH)
    o, lse, part_o = local_call(
        bound(attend_kernel, ctx_count, block, part, head),
        [shaped((tokens, q_width), bf16), shaped((tokens, q_width), f32), shaped((tokens, width), bf16)],
        (q, kv, kvp, spots, *pieces_out),
        [VM] * 4 + [HB] * 4,
        [pltpu.VMEM((q_width, width), bf16), eight],
    )
    eighths = (8, part, width)
    x_mine = xs[0][:part]
    c_mine = cs[0][:part]
    h, b_all = group_call(
        sum_spread_kernel, 0, [shaped((part, width), f32), shaped(eighths, bf16)],
        (part_o.reshape(eighths), x_mine, gain_mlp), part, width, 20,
    )
    b_all = b_all.reshape(tokens, width)
    z, gu = local_call(
        bound(gate_kernel, ctx_count, block),
        [shaped((tokens, hidden), bf16), shaped((tokens, 2 * hidden), f32)],
        (b_all, *pieces_gate),
        [VM] + [HB] * 4,
        [pltpu.VMEM((width, 2 * hidden), bf16), eight],
    )

    def plus(*values):
        total = values[0].astype(f32)
        for value in values[1:]:
            total = total + value.astype(f32)
        return total.astype(bf16)

    def home(quarters, axis):
        far = swap(quarters[3], X)
        near = swap(quarters[2], X)
        over_z = swap(plus(quarters[1], far), ZH)
        piece = plus(quarters[0], near, over_z)
        sent = []
        for dc in (0, 1):
            lo, hi = jnp.split(piece[dc], 2, axis=axis)
            sent += [jnp.where(zl_on, hi, lo), jnp.where(zl_on, lo, hi)]
        got = [sent[0]] + [swap(sent[k], masks[k]) for k in (1, 2, 3)]
        got = [
            jnp.where(zl_on, got[1], got[0]), jnp.where(zl_on, got[0], got[1]),
            jnp.where(zl_on, got[3], got[2]), jnp.where(zl_on, got[2], got[3]),
        ]
        return [jnp.where(c_on, got[k ^ 2], got[k]) for k in range(4)]

    quarter = [shaped((2, hidden, 2 * block), bf16)] * 4
    grads_down = local_call(bound(grad_cols_kernel, ctx_count, block), quarter, (z, *cs), [VM] * 5)
    dgu, part_b = local_call(
        bound(gate_back_kernel, ctx_count, block),
        [shaped((tokens, 2 * hidden), bf16), shaped((tokens, width), bf16)],
        (*cs, gu, *pieces_down, *pieces_gate),
        [VM] * 5 + [HB] * 8,
        [
            pltpu.VMEM((hidden, width), bf16),
            pltpu.VMEM((width, 2 * hidden), bf16),
            pltpu.SemaphoreType.DMA((2, 8)),
        ],
    )
    quarter = [shaped((2, 2 * block, 2 * hidden), bf16)] * 4
    grads_gate = local_call(bound(grad_rows_kernel, ctx_count, block), quarter, (b_all, dgu), [VM] * 2)
    dh, dh_all, mlp_gain_part = group_call(
        sum_spread_back_kernel, 1,
        [shaped((part, width), f32), shaped(eighths, bf16), shaped((1, width), f32)],
        (part_b.reshape(eighths), h, c_mine, gain_mlp), part, width, 20,
    )
    dh_all = dh_all.reshape(tokens, width)
    dq, dkv, dkvp = local_call(
        bound(attend_back_kernel, ctx_count, block, part, head),
        [shaped((tokens, q_width), f32), shaped((tokens, 2 * head), f32), shaped((tokens, 2 * head), bf16)],
        (dh_all, o, q, kv, kvp, lse, spots, *pieces_out),
        [VM] * 7 + [HB] * 4,
        [pltpu.VMEM((q_width, width), bf16), pltpu.VMEM((tokens, q_width), bf16), eight],
    )
    got_kv = swap(dkvp, ZH)
    quarter = [shaped((2, q_width, 2 * block), bf16)] * 4
    grads_out = local_call(bound(grad_wide_kernel, ctx_count, block), quarter, (o, dh_all), [VM] * 2)
    (part_d,) = local_call(
        bound(down_kernel, ctx_count, block), [shaped((tokens, width), bf16)],
        (z, *pieces_down), [VM] + [HB] * 4, [pltpu.VMEM((hidden, width), bf16), eight],
    )
    (out_mine,) = group_call(
        sum_out_kernel, 2, [shaped((part, width), bf16)], (part_d.reshape(eighths), h), part, width, 10,
    )
    dqkv, part_a, gq_part, gk_part = local_call(
        bound(qkv_back_kernel, ctx_count, block),
        [
            shaped((tokens, q_width + 2 * head), bf16),
            shaped((tokens, width), bf16),
            shaped((1, head), f32),
            shaped((1, head), f32),
        ],
        (dq, dkv, got_kv, raw, cosine, sine, gain_q, gain_k, *pieces_qkv),
        [VM] * 8 + [HB] * 4,
        [pltpu.VMEM((width, q_width + 2 * head), bf16), eight],
    )
    quarter = [shaped((2, 2 * block, q_width + 2 * head), bf16)] * 4
    grads_qkv = local_call(bound(grad_rows_kernel, ctx_count, block), quarter, (a, dqkv), [VM] * 2)
    in_mine, attn_gain_part = group_call(
        sum_in_kernel, 3, [shaped((part, width), bf16), shaped((1, width), f32)],
        (part_a.reshape(eighths), dh, x_mine, gain_attn), part, width, 10,
    )

    def both(mine):
        other = swap_y(mine)
        return jnp.stack([jnp.where(upper, other, mine), jnp.where(upper, mine, other)])

    block_output = both(out_mine)
    input_grad = both(in_mine).astype(f32)
    home_down = home(grads_down, 1)
    home_gate = home(grads_gate, 0)
    home_out = home(grads_out, 1)
    home_qkv = home(grads_qkv, 0)

    totals = jnp.concatenate(
        [
            attn_gain_part.reshape(rank_count, block),
            mlp_gain_part.reshape(rank_count, block),
            gq_part.reshape(rank_count, head_piece),
            gk_part.reshape(rank_count, head_piece),
        ],
        axis=1,
    )
    totals = jnp.take(totals, jnp.arange(rank_count) ^ rank, axis=0)
    for mask in (X, C, ZH, ZL):
        many = totals.shape[0] // 2
        totals = totals[:many] + swap(totals[many:], mask)
    totals = (totals + swap_y(totals))[0]

    def side(blocks, low, high):
        return jnp.concatenate([t[:, low:high] for t in blocks], axis=1).astype(f32)

    return (
        block_output,
        input_grad,
        totals[:block],
        totals[block : 2 * block],
        totals[2 * block : 2 * block + head_piece],
        totals[2 * block + head_piece :],
        side(home_qkv, 0, q_width),
        side(home_qkv, q_width, q_width + head),
        side(home_qkv, q_width + head, q_width + 2 * head),
        jnp.concatenate(home_out, axis=0).astype(f32),
        side(home_gate, 0, hidden),
        side(home_gate, hidden, 2 * hidden),
        jnp.concatenate(home_down, axis=0).astype(f32),
    )


def rms_scale(value_rows):
    return lax.rsqrt(jnp.mean(value_rows * value_rows, axis=-1, keepdims=True) + eps_norm)


def rope_tables(places, head_size):
    half_size = head_size // 2
    inverse = rope_base ** (-2.0 * jnp.arange(half_size).astype(jnp.float32) / head_size)
    angles = places.astype(jnp.float32)[:, None] * inverse[None, :]
    angles = jnp.concatenate([angles, angles], axis=-1)
    return (jnp.cos(angles), jnp.sin(angles))


def rotate(values, cosine, sine):
    half_size = values.shape[-1] // 2
    turned = jnp.concatenate([-values[..., half_size:], values[..., :half_size]], axis=-1)
    return values * cosine[:, None, :] + turned * sine[:, None, :]


def rotate_back(grads, cosine, sine):
    half_size = grads.shape[-1] // 2
    weighted = grads * sine[:, None, :]
    return grads * cosine[:, None, :] + jnp.concatenate(
        [weighted[..., half_size:], -weighted[..., :half_size]], axis=-1
    )


def block_mask(query_index, lowest, key_index):
    return (key_index[None, :] <= query_index[:, None]) & (key_index[None, :] >= lowest[:, None])


def dot_nt(left, right):
    return lax.dot_general(
        left, right, (((1,), (1,)), ((), ())), preferred_element_type=jnp.float32
    )


def dot_tn(left, right):
    return lax.dot_general(
        left, right, (((0,), (0,)), ((), ())), preferred_element_type=jnp.float32
    )


def micro_pass(inputs_seq, places, cotangent, shards, totals):
    float_type = jnp.float32
    half_type = jnp.bfloat16
    fetched = (
        lax.all_gather(shards[0], ("dp", "ctx"), axis=0, tiled=True),
        lax.all_gather(shards[1], ("dp", "ctx"), axis=0, tiled=True),
        lax.all_gather(shards[2], ("dp", "ctx"), axis=0, tiled=True),
        lax.all_gather(shards[3], ("dp", "ctx"), axis=0, tiled=True),
        lax.all_gather(shards[4], ("dp", "ctx"), axis=0, tiled=True),
        lax.all_gather(shards[5], ("dp", "ctx"), axis=0, tiled=True),
        lax.all_gather(shards[6], ("dp", "ctx"), axis=0, tiled=True),
        lax.all_gather(shards[7], ("dp", "ctx"), axis=1, tiled=True),
        lax.all_gather(shards[8], ("dp", "ctx"), axis=0, tiled=True),
        lax.all_gather(shards[9], ("dp", "ctx"), axis=0, tiled=True),
        lax.all_gather(shards[10], ("dp", "ctx"), axis=1, tiled=True),
    )
    gain_attn = fetched[0].astype(float_type)
    gain_mlp = fetched[1].astype(float_type)
    gain_query = fetched[2].astype(float_type)
    gain_key = fetched[3].astype(float_type)
    query_proj, key_proj, value_proj, out_proj, gate_proj, up_proj, down_proj = fetched[4:]
    head_size = gain_query.shape[0]
    head_count = query_proj.shape[1] // head_size
    kv_count = key_proj.shape[1] // head_size
    group_size = head_count // kv_count
    token_count = inputs_seq.shape[0]
    ctx_count = lax.axis_size("ctx")
    ctx_rank = lax.axis_index("ctx")
    scaling = head_size ** (-0.5)
    query_index = ctx_rank * token_count + jnp.arange(token_count, dtype=jnp.int32)
    lowest = query_index - places
    last_query = ctx_rank * token_count + token_count - 1
    residual_in = inputs_seq.astype(float_type)
    scale_attn = rms_scale(residual_in)
    normed_attn = residual_in * scale_attn
    attn_input = (normed_attn * gain_attn).astype(half_type)
    query_raw = jnp.dot(attn_input, query_proj, preferred_element_type=float_type).reshape(
        token_count, head_count, head_size
    )
    key_raw = jnp.dot(attn_input, key_proj, preferred_element_type=float_type).reshape(
        token_count, kv_count, head_size
    )
    value_rows = jnp.dot(attn_input, value_proj, preferred_element_type=float_type).astype(
        half_type
    )
    query_scale = rms_scale(query_raw)
    query_normed = query_raw * query_scale
    key_scale = rms_scale(key_raw)
    key_normed = key_raw * key_scale
    cosine, sine = rope_tables(places, head_size)
    query_rot = rotate(query_normed * gain_query, cosine, sine).astype(half_type)
    key_rot = (
        rotate(key_normed * gain_key, cosine, sine)
        .astype(half_type)
        .reshape(token_count, kv_count * head_size)
    )
    query_group = query_rot.reshape(token_count, kv_count, group_size, head_size)
    initial = (
        jnp.full((kv_count, group_size, token_count), -1e30, float_type),
        jnp.zeros((kv_count, group_size, token_count), float_type),
        jnp.zeros((token_count, kv_count, group_size, head_size), float_type),
    )
    pieces = (
        lax.all_gather(key_rot, "ctx", axis=0, tiled=True),
        lax.all_gather(value_rows, "ctx", axis=0, tiled=True),
    )
    row_count = pieces[0].shape[0]
    key_piece = pieces[0].reshape(row_count, kv_count, head_size)
    value_piece = pieces[1].reshape(row_count, kv_count, head_size)

    def fold_attend(state):
        peak, total, running = state
        scores = (
            jnp.einsum("qkgd,jkd->kgqj", query_group, key_piece, preferred_element_type=float_type)
            * scaling
        )
        allowed = block_mask(query_index, lowest, jnp.arange(row_count, dtype=jnp.int32))
        new_peak = jnp.maximum(peak, jnp.max(jnp.where(allowed, scores, -jnp.inf), axis=-1))
        weights = jnp.where(allowed, jnp.exp(scores - new_peak[..., None]), 0.0)
        total = jnp.sum(weights, axis=-1)
        running = jnp.einsum(
            "kgqj,jkd->qkgd",
            weights.astype(half_type),
            value_piece,
            preferred_element_type=float_type,
        )
        return (new_peak, total, running)

    peak, total, running = lax.cond(
        jnp.int32(0) <= last_query, fold_attend, lambda state: state, initial
    )
    attn_rows = (
        (running / jnp.transpose(total, (2, 0, 1))[..., None])
        .astype(half_type)
        .reshape(token_count, head_count * head_size)
    )
    log_total = peak + jnp.log(total)
    attn_out = lax.psum(
        jnp.dot(attn_rows, out_proj, preferred_element_type=float_type).astype(jnp.bfloat16), "mp"
    ).astype(jnp.float32)
    middle = residual_in + attn_out
    scale_mlp = rms_scale(middle)
    normed_mlp = middle * scale_mlp
    mlp_input = (normed_mlp * gain_mlp).astype(half_type)
    gate_rows = jnp.dot(mlp_input, gate_proj, preferred_element_type=float_type)
    up_rows = jnp.dot(mlp_input, up_proj, preferred_element_type=float_type)
    sigmoid_gate = jax.nn.sigmoid(gate_rows)
    hidden_rows = (gate_rows * sigmoid_gate * up_rows).astype(half_type)
    mlp_out = lax.psum(
        jnp.dot(hidden_rows, down_proj, preferred_element_type=float_type).astype(jnp.bfloat16),
        "mp",
    ).astype(jnp.float32)
    block_output = (middle + mlp_out).astype(half_type)
    refetched = (
        lax.all_gather(shards[0], ("dp", "ctx"), axis=0, tiled=True),
        lax.all_gather(shards[1], ("dp", "ctx"), axis=0, tiled=True),
        lax.all_gather(shards[2], ("dp", "ctx"), axis=0, tiled=True),
        lax.all_gather(shards[3], ("dp", "ctx"), axis=0, tiled=True),
        lax.all_gather(shards[4], ("dp", "ctx"), axis=0, tiled=True),
        lax.all_gather(shards[5], ("dp", "ctx"), axis=0, tiled=True),
        lax.all_gather(shards[6], ("dp", "ctx"), axis=0, tiled=True),
        lax.all_gather(shards[7], ("dp", "ctx"), axis=1, tiled=True),
        lax.all_gather(shards[8], ("dp", "ctx"), axis=0, tiled=True),
        lax.all_gather(shards[9], ("dp", "ctx"), axis=0, tiled=True),
        lax.all_gather(shards[10], ("dp", "ctx"), axis=1, tiled=True),
    )
    gain_attn = refetched[0].astype(float_type)
    gain_mlp = refetched[1].astype(float_type)
    gain_query = refetched[2].astype(float_type)
    gain_key = refetched[3].astype(float_type)
    query_proj, key_proj, value_proj, out_proj, gate_proj, up_proj, down_proj = refetched[4:]
    down_grad = dot_tn(hidden_rows, cotangent)
    hidden_grad = dot_nt(cotangent, down_proj)
    gate_grad = (
        hidden_grad * up_rows * sigmoid_gate * (1.0 + gate_rows * (1.0 - sigmoid_gate))
    ).astype(half_type)
    up_grad = (hidden_grad * gate_rows * sigmoid_gate).astype(half_type)
    gate_proj_grad = dot_tn(mlp_input, gate_grad)
    up_proj_grad = dot_tn(mlp_input, up_grad)
    mlp_in_grad = lax.psum(
        (dot_nt(gate_grad, gate_proj) + dot_nt(up_grad, up_proj)).astype(jnp.bfloat16), "mp"
    ).astype(jnp.float32)
    mlp_gain_grad = jnp.sum(mlp_in_grad * normed_mlp, axis=0)
    normed_grad = mlp_in_grad * gain_mlp
    middle_grad = cotangent.astype(float_type) + scale_mlp * (
        normed_grad - normed_mlp * jnp.mean(normed_grad * normed_mlp, axis=-1, keepdims=True)
    )
    middle_half = middle_grad.astype(half_type)
    out_proj_grad = dot_tn(attn_rows, middle_half)
    attn_grad = dot_nt(middle_half, out_proj).astype(half_type)
    grad_group = attn_grad.reshape(token_count, kv_count, group_size, head_size)
    attn_group = attn_rows.reshape(token_count, kv_count, group_size, head_size)
    row_dot = jnp.einsum(
        "qkgd,qkgd->kgq", grad_group, attn_group, preferred_element_type=float_type
    )
    key_back, value_back = (
        lax.all_gather(key_rot, "ctx", axis=0, tiled=True),
        lax.all_gather(value_rows, "ctx", axis=0, tiled=True),
    )

    def back_block(query_sum, block_id):
        start = block_id * token_count
        key_piece = lax.dynamic_slice_in_dim(key_back, start, token_count, 0).reshape(
            token_count, kv_count, head_size
        )
        value_piece = lax.dynamic_slice_in_dim(value_back, start, token_count, 0).reshape(
            token_count, kv_count, head_size
        )

        def back_attend(running):
            scores = (
                jnp.einsum(
                    "qkgd,jkd->kgqj", query_group, key_piece, preferred_element_type=float_type
                )
                * scaling
            )
            allowed = block_mask(
                query_index, lowest, start + jnp.arange(token_count, dtype=jnp.int32)
            )
            probs = jnp.where(allowed, jnp.exp(scores - log_total[..., None]), 0.0)
            value_part = jnp.einsum(
                "kgqj,qkgd->jkd",
                probs.astype(half_type),
                grad_group,
                preferred_element_type=float_type,
            )
            prob_grad = jnp.einsum(
                "qkgd,jkd->kgqj", grad_group, value_piece, preferred_element_type=float_type
            )
            score_half = (probs * (prob_grad - row_dot[..., None])).astype(half_type)
            query_part = (
                jnp.einsum(
                    "kgqj,jkd->qkgd", score_half, key_piece, preferred_element_type=float_type
                )
                * scaling
            )
            key_part = (
                jnp.einsum(
                    "kgqj,qkgd->jkd", score_half, query_group, preferred_element_type=float_type
                )
                * scaling
            )
            return (
                running + query_part,
                jnp.concatenate(
                    [
                        key_part.reshape(token_count, kv_count * head_size),
                        value_part.reshape(token_count, kv_count * head_size),
                    ],
                    axis=-1,
                ),
            )

        def passing(running):
            return (running, jnp.zeros((token_count, 2 * kv_count * head_size), float_type))

        return lax.cond(start <= last_query, back_attend, passing, query_sum)

    query_grad, kv_terms = lax.scan(
        back_block,
        jnp.zeros((token_count, kv_count, group_size, head_size), float_type),
        jnp.arange(ctx_count, dtype=jnp.int32),
    )
    kv_grad = lax.psum_scatter(
        kv_terms.reshape(ctx_count * token_count, 2 * kv_count * head_size).astype(jnp.bfloat16),
        "ctx",
        scatter_dimension=0,
        tiled=True,
    ).astype(jnp.float32)
    key_rot_grad = kv_grad[:, : kv_count * head_size].reshape(token_count, kv_count, head_size)
    value_half = kv_grad[:, kv_count * head_size :].astype(half_type)
    query_back = rotate_back(query_grad.reshape(token_count, head_count, head_size), cosine, sine)
    key_grad_back = rotate_back(key_rot_grad, cosine, sine)
    query_gain_part = jnp.sum(query_back * query_normed, axis=(0, 1))
    key_gain_part = jnp.sum(key_grad_back * key_normed, axis=(0, 1))
    query_ngrad = query_back * gain_query
    key_ngrad = key_grad_back * gain_key
    query_half = (
        (
            query_scale
            * (
                query_ngrad
                - query_normed * jnp.mean(query_ngrad * query_normed, axis=-1, keepdims=True)
            )
        )
        .reshape(token_count, head_count * head_size)
        .astype(half_type)
    )
    key_half = (
        (
            key_scale
            * (key_ngrad - key_normed * jnp.mean(key_ngrad * key_normed, axis=-1, keepdims=True))
        )
        .reshape(token_count, kv_count * head_size)
        .astype(half_type)
    )
    query_proj_grad = dot_tn(attn_input, query_half)
    key_proj_grad = dot_tn(attn_input, key_half)
    value_proj_grad = dot_tn(attn_input, value_half)
    attn_in_grad, query_gain_sum, key_gain_sum = (
        lax.psum(
            (
                dot_nt(query_half, query_proj)
                + dot_nt(key_half, key_proj)
                + dot_nt(value_half, value_proj)
            ).astype(jnp.bfloat16),
            "mp",
        ).astype(jnp.float32),
        lax.psum(query_gain_part.astype(jnp.bfloat16), "mp").astype(jnp.float32),
        lax.psum(key_gain_part.astype(jnp.bfloat16), "mp").astype(jnp.float32),
    )
    attn_gain_grad = jnp.sum(attn_in_grad * normed_attn, axis=0)
    normed_in_grad = attn_in_grad * gain_attn
    input_grad = middle_grad + scale_attn * (
        normed_in_grad
        - normed_attn * jnp.mean(normed_in_grad * normed_attn, axis=-1, keepdims=True)
    )
    addition = (
        attn_gain_grad,
        mlp_gain_grad,
        query_gain_sum,
        key_gain_sum,
        query_proj_grad,
        key_proj_grad,
        value_proj_grad,
        out_proj_grad,
        gate_proj_grad,
        up_proj_grad,
        down_grad,
    )
    totals = tuple((earlier + later for earlier, later in zip(totals, addition)))
    return (block_output, input_grad, totals)


def on_device(
    block_input,
    doc_positions,
    out_cotangent,
    attn_gain,
    mlp_gain,
    query_gain,
    key_gain,
    w_query,
    w_key,
    w_value,
    w_out,
    w_gate,
    w_up,
    w_down,
):
    shards = (
        attn_gain,
        mlp_gain,
        query_gain,
        key_gain,
        w_query,
        w_key,
        w_value,
        w_out,
        w_gate,
        w_up,
        w_down,
    )
    head_size = query_gain.shape[0] * lax.axis_size(("dp", "ctx"))
    model_width = block_input.shape[2]
    query_width = w_query.shape[1]
    kv_width = w_key.shape[1]
    hidden_width = w_gate.shape[1]
    totals = (
        jnp.zeros((model_width,), jnp.float32),
        jnp.zeros((model_width,), jnp.float32),
        jnp.zeros((head_size,), jnp.float32),
        jnp.zeros((head_size,), jnp.float32),
        jnp.zeros((model_width, query_width), jnp.float32),
        jnp.zeros((model_width, kv_width), jnp.float32),
        jnp.zeros((model_width, kv_width), jnp.float32),
        jnp.zeros((query_width, model_width), jnp.float32),
        jnp.zeros((model_width, hidden_width), jnp.float32),
        jnp.zeros((model_width, hidden_width), jnp.float32),
        jnp.zeros((hidden_width, model_width), jnp.float32),
    )
    output_list = []
    grad_list = []
    for micro in range(block_input.shape[0]):
        output_rows, input_rows, totals = micro_pass(
            block_input[micro], doc_positions[micro], out_cotangent[micro], shards, totals
        )
        output_list.append(output_rows)
        grad_list.append(input_rows)
    owned = (
        lax.psum_scatter(totals[0], ("dp", "ctx"), scatter_dimension=0, tiled=True),
        lax.psum_scatter(totals[1], ("dp", "ctx"), scatter_dimension=0, tiled=True),
        lax.psum_scatter(totals[2], ("dp", "ctx"), scatter_dimension=0, tiled=True),
        lax.psum_scatter(totals[3], ("dp", "ctx"), scatter_dimension=0, tiled=True),
        lax.psum_scatter(totals[4], ("dp", "ctx"), scatter_dimension=0, tiled=True),
        lax.psum_scatter(totals[5], ("dp", "ctx"), scatter_dimension=0, tiled=True),
        lax.psum_scatter(totals[6], ("dp", "ctx"), scatter_dimension=0, tiled=True),
        lax.psum_scatter(totals[7], ("dp", "ctx"), scatter_dimension=1, tiled=True),
        lax.psum_scatter(totals[8], ("dp", "ctx"), scatter_dimension=0, tiled=True),
        lax.psum_scatter(totals[9], ("dp", "ctx"), scatter_dimension=0, tiled=True),
        lax.psum_scatter(totals[10], ("dp", "ctx"), scatter_dimension=1, tiled=True),
    )
    return (
        jnp.stack(output_list),
        jnp.stack(grad_list),
        owned[0],
        owned[1],
        owned[2],
        owned[3],
        owned[4],
        owned[5],
        owned[6],
        owned[7],
        owned[8],
        owned[9],
        owned[10],
    )


def choose(mesh, arrays):
    dp, ctx, mp = mesh.shape["dp"], mesh.shape["ctx"], mesh.shape["mp"]
    width = arrays[0].shape[2]
    paired = dp == 4 and ctx == 4 and mp == 2
    return split_device if paired and width % (dp * ctx * 128) == 0 else on_device


def solution(mesh):
    in_specs = (
        P("dp", "ctx", None),
        P("dp", "ctx"),
        P("dp", "ctx", None),
        P(("dp", "ctx")),
        P(("dp", "ctx")),
        P(("dp", "ctx")),
        P(("dp", "ctx")),
        P(("dp", "ctx"), "mp"),
        P(("dp", "ctx"), "mp"),
        P(("dp", "ctx"), "mp"),
        P("mp", ("dp", "ctx")),
        P(("dp", "ctx"), "mp"),
        P(("dp", "ctx"), "mp"),
        P("mp", ("dp", "ctx")),
    )
    out_specs = (
        P("dp", "ctx", None),
        P("dp", "ctx", None),
        P(("dp", "ctx")),
        P(("dp", "ctx")),
        P(("dp", "ctx")),
        P(("dp", "ctx")),
        P(("dp", "ctx"), "mp"),
        P(("dp", "ctx"), "mp"),
        P(("dp", "ctx"), "mp"),
        P("mp", ("dp", "ctx")),
        P(("dp", "ctx"), "mp"),
        P(("dp", "ctx"), "mp"),
        P("mp", ("dp", "ctx")),
    )

    def run(*arrays):
        return jax.shard_map(
            choose(mesh, arrays), mesh=mesh, in_specs=in_specs, out_specs=out_specs, check_vma=False
        )(*arrays)

    return run
```

```python
import functools

import jax
import jax.numpy as jnp
from jax import lax
from jax.experimental import pallas as pl
from jax.experimental.pallas import tpu as pltpu
from jax.sharding import PartitionSpec as P

eps_norm = 1e-06
rope_base = 1000000.0
MESH = pl.DeviceIdType.MESH
f32 = jnp.float32
bf16 = jnp.bfloat16
PIECES = ((0, 0), (0, 1), (1, 0), (1, 1))


def flip(value, bit):
    return 1 - value if bit else value


def place():
    dp = lax.axis_index("dp")
    ctx = lax.axis_index("ctx")
    return {
        "dp": dp,
        "ctx": ctx,
        "y": lax.axis_index("mp"),
        "x": dp // 2,
        "c": dp % 2,
        "zh": ctx // 2,
        "zl": ctx % 2,
    }


def run_start(at, dx, dzh, dc, ctx_count, block):
    start = ((flip(at["x"], dx) * 2 + flip(at["c"], dc)) * ctx_count + flip(at["zh"], dzh) * 2) * block
    return pl.multiple_of(start, 2 * block)


def finish(copies):
    for copy in copies:
        copy.wait()


def nn(left, right):
    return lax.dot_general(left, right, (((1,), (0,)), ((), ())), preferred_element_type=f32)


def nt(left, right):
    return lax.dot_general(left, right, (((1,), (1,)), ((), ())), preferred_element_type=f32)


def tn(left, right):
    return lax.dot_general(left, right, (((0,), (0,)), ((), ())), preferred_element_type=f32)


def root_scale(values):
    return lax.rsqrt(jnp.mean(values * values, axis=-1, keepdims=True) + eps_norm)


def turn(values, cosine, sine):
    return values * cosine + pltpu.roll(values, values.shape[-1] // 2, 1) * sine


def turn_back(values, cosine, sine):
    return values * cosine + pltpu.roll(values * sine, values.shape[-1] // 2, 1)


def pair_rows(ref, base, part, span):
    far = base + 2 * part
    return jnp.concatenate(
        [ref[pl.ds(base, part), :][:, span[0] : span[1]], ref[pl.ds(far, part), :][:, span[0] : span[1]]], axis=0
    )


def allowed_pairs(at, n, m, part, heads, extra):
    def fold(index, size, times):
        for k in range(times - 1, 0, -1):
            index = jnp.where(index >= k * size, index - k * size, index)
        return index

    row = lax.broadcasted_iota(jnp.int32, (heads * 2 * part, 4 * part), 0)
    col = lax.broadcasted_iota(jnp.int32, (heads * 2 * part, 4 * part), 1)
    near = at["zl"] * part
    far = (1 - at["zl"]) * part
    row = fold(row, 2 * part, heads)
    query = jnp.where(row < part, row + near, row - part + far) + at["zh"] * 2 * part
    inner = fold(col, 2 * part, 2)
    key = jnp.where(inner < part, inner + near, inner - part + far)
    key = key + jnp.where(col < 2 * part, at["zh"], 1 - at["zh"]) * (2 * part)
    query, key = query.astype(f32), key.astype(f32)
    spot = jnp.concatenate([extra[n * 4 + m, 1], extra[n * 4 + 2 + m, 1]] * heads, axis=0)[:, :1]
    return (key <= query) & (key >= query - spot)


def stack_heads(ref, base, part, head):
    heads = ref.shape[1] // head
    return jnp.concatenate([pair_rows(ref, base, part, (h * head, (h + 1) * head)) for h in range(heads)], axis=0)


def unstack(ref, base, part, head, values):
    heads = ref.shape[1] // head
    for h in range(heads):
        top = 2 * part * h
        ref[pl.ds(base, part), pl.ds(h * head, head)] = values[top : top + part].astype(ref.dtype)
        ref[pl.ds(base + 2 * part, part), pl.ds(h * head, head)] = values[top + part : top + 2 * part].astype(ref.dtype)


def grad_cols_kernel(ctx_count, block, left_ref, r0, r1, r2, r3, q0, q1, q2, q3):
    at = place()
    rows = r0.shape[0]
    for n, (dx, dzh) in enumerate(PIECES):
        for dc in (0, 1):
            run = pl.ds(run_start(at, dx, dzh, dc, ctx_count, block), 2 * block)
            total = tn(left_ref[pl.ds(0, rows), :], r0[:, run])
            for m, right in ((1, r1), (2, r2), (3, r3)):
                total = total + tn(left_ref[pl.ds(m * rows, rows), :], right[:, run])
            (q0, q1, q2, q3)[n][dc] = total.astype(bf16)


def grad_rows_kernel(ctx_count, block, left_ref, right_ref, q0, q1, q2, q3):
    at = place()
    for n, (dx, dzh) in enumerate(PIECES):
        for dc in (0, 1):
            run = pl.ds(run_start(at, dx, dzh, dc, ctx_count, block), 2 * block)
            (q0, q1, q2, q3)[n][dc] = tn(left_ref[:, run], right_ref[...]).astype(bf16)


def grad_wide_kernel(ctx_count, block, left_ref, right_ref, q0, q1, q2, q3):
    at = place()
    for n, (dx, dzh) in enumerate(PIECES):
        for dc in (0, 1):
            run = pl.ds(run_start(at, dx, dzh, dc, ctx_count, block), 2 * block)
            (q0, q1, q2, q3)[n][dc] = tn(left_ref[...], right_ref[:, run]).astype(bf16)


def gate_back_kernel(ctx_count, block, c0, c1, c2, c3, gu_ref, down, weight, dgu_ref, part_ref):
    at = place()
    rows = c0.shape[0]
    hidden = down.shape[0]
    for n, c_ref in enumerate((c0, c1, c2, c3)):
        span = pl.ds(n * rows, rows)
        dz = nt(c_ref[...], down[...])
        g = gu_ref[span, pl.ds(0, hidden)].astype(f32)
        u = gu_ref[span, pl.ds(hidden, hidden)].astype(f32)
        s = jax.nn.sigmoid(g)
        dgu_ref[span, pl.ds(0, hidden)] = (dz * u * s * (1.0 + g * (1.0 - s))).astype(bf16)
        dgu_ref[span, pl.ds(hidden, hidden)] = (dz * g * s).astype(bf16)

    @pl.loop(0, 4)
    def _(n):
        span = pl.ds(pl.multiple_of(n * rows, rows), rows)
        part_ref[span, :] = nt(dgu_ref[span, :], weight[...]).astype(bf16)


def down_kernel(ctx_count, block, z_ref, down, part_ref):
    at = place()
    rows = 256

    @pl.loop(0, z_ref.shape[0] // rows)
    def _(n):
        span = pl.ds(pl.multiple_of(n * rows, rows), rows)
        part_ref[span, :] = nn(z_ref[span, :], down[...]).astype(bf16)


def attend_back_kernel(ctx_count, block, part, head, dh_ref, o_ref, q_ref, kv_ref, kvp_ref, lse_ref, extra,
                       weight, dq_ref, dkv_ref, dkvp_ref, do_ref):
    at = place()
    heads = q_ref.shape[1] // head
    scaling = head ** (-0.5)

    @pl.loop(0, 4)
    def _(n):
        span = pl.ds(pl.multiple_of(n * 2 * part, 2 * part), 2 * part)
        do_ref[span, :] = nt(dh_ref[span, :], weight[...]).astype(bf16)

    @pl.loop(0, 2)
    def _(n):
      @pl.loop(0, 2)
      def _(m):
        base = pl.multiple_of(n * (4 * part) + m * part, part)
        q = stack_heads(q_ref, base, part, head)
        o = stack_heads(o_ref, base, part, head)
        do = stack_heads(do_ref, base, part, head)
        lse = stack_heads(lse_ref, base, part, head)[:, :1]
        k = jnp.concatenate(
            [pair_rows(kv_ref, base, part, (0, head)), pair_rows(kvp_ref, base, part, (0, head))], axis=0
        )
        v = jnp.concatenate(
            [pair_rows(kv_ref, base, part, (head, 2 * head)), pair_rows(kvp_ref, base, part, (head, 2 * head))], axis=0
        )
        allowed = allowed_pairs(at, n, m, part, heads, extra)
        probs = jnp.where(allowed, jnp.exp(jnp.where(allowed, nt(q, k) * scaling - lse, 0.0)), 0.0)
        dv = tn(probs.astype(bf16), do)
        row_dot = jnp.sum(do.astype(f32) * o.astype(f32), axis=-1, keepdims=True)
        ds = (probs * (nt(do, v) - row_dot)).astype(bf16)
        unstack(dq_ref, base, part, head, nn(ds, k) * scaling)
        dk = tn(ds, q) * scaling
        for ref, top in ((dkv_ref, 0), (dkvp_ref, 2 * part)):
            for i in (0, 1):
                spot = pl.ds(base + i * 2 * part, part)
                low = top + i * part
                ref[spot, pl.ds(0, head)] = dk[low : low + part].astype(ref.dtype)
                ref[spot, pl.ds(head, head)] = dv[low : low + part].astype(ref.dtype)


def qkv_back_kernel(ctx_count, block, dq_ref, dkv_ref, got_ref, raw_ref, extra, gains, weight, dqkv_ref, part_ref, gq_ref, gk_ref):
    at = place()
    head = gq_ref.shape[1]
    q_width = dq_ref.shape[1]
    rows = 128
    gain_q, gain_k = gains[2:3, 0:head], gains[3:4, 0:head]
    gq_ref[...] = jnp.zeros_like(gq_ref)
    gk_ref[...] = jnp.zeros_like(gk_ref)

    def through(u, w, gain, total_ref, cos, sin):
        r = root_scale(u)
        n = u * r
        e = turn_back(w, cos, sin)
        total_ref[...] += jnp.sum(e * n, axis=0, keepdims=True)
        f = e * gain
        return (r * (f - n * jnp.mean(f * n, axis=-1, keepdims=True))).astype(bf16)

    @pl.loop(0, dq_ref.shape[0] // rows)
    def _(n):
        span = pl.ds(pl.multiple_of(n * rows, rows), rows)
        cos, sin = tables(extra, n)
        for h in range(q_width // head):
            cols = pl.ds(h * head, head)
            dqkv_ref[span, cols] = through(raw_ref[span, cols], dq_ref[span, cols], gain_q, gq_ref, cos, sin)
        dk = dkv_ref[span, pl.ds(0, head)] + got_ref[span, pl.ds(0, head)].astype(f32)
        dv = dkv_ref[span, pl.ds(head, head)] + got_ref[span, pl.ds(head, head)].astype(f32)
        cols = pl.ds(q_width, head)
        dqkv_ref[span, cols] = through(raw_ref[span, cols], dk, gain_k, gk_ref, cos, sin)
        dqkv_ref[span, pl.ds(q_width + head, head)] = dv.astype(bf16)

    @pl.loop(0, dq_ref.shape[0] // rows)
    def _(n):
        span = pl.ds(pl.multiple_of(n * rows, rows), rows)
        part_ref[span, :] = nt(dqkv_ref[span, :], weight[...]).astype(bf16)


def partners(at):
    return (
        {"dp": at["dp"] + 1 - 2 * at["c"]},
        {"ctx": at["ctx"] + 1 - 2 * at["zl"]},
        {"mp": 1 - at["y"]},
    )


def meet(at):
    barrier = pltpu.get_barrier_semaphore()
    for device in partners(at):
        pl.semaphore_signal(barrier, inc=1, device_id=device, device_id_type=MESH)
    pl.semaphore_wait(barrier, 3)


def sender(send, recv):
    def start(source, target, number, device):
        copy = pltpu.make_async_remote_copy(
            src_ref=source,
            dst_ref=target,
            send_sem=send.at[number],
            recv_sem=recv.at[number],
            device_id=device,
            device_id_type=MESH,
        )
        copy.start()
        return copy

    return start


def sum_group(at, part, from_core, kept, second, from_z, from_y, last, start):
    core, low, across = partners(at)
    half = part.shape[2] // 2
    a, b = pl.ds(0, half), pl.ds(half, half)
    first = {k: start(part.at[4 + k], from_core.at[k], k, core) for k in (3, 1, 2, 0)}

    def total(k):
        first[k].wait_recv()
        return part[k].astype(f32) + from_core[k].astype(f32)

    kept[2] = total(3).astype(bf16)
    z1 = start(kept.at[2, :, a], from_z.at[1], 4, low)
    y1 = start(kept.at[2, :, b], from_y.at[1], 5, across)
    kept[0] = total(1).astype(bf16)
    y0 = start(kept.at[0, :, b], from_y.at[0], 6, across)
    kept[1] = total(2).astype(bf16)
    z0 = start(kept.at[1, :, a], from_z.at[0], 7, low)
    z1.wait_recv()
    second[0] = (kept[0, :, a].astype(f32) + from_z[1].astype(f32)).astype(bf16)
    y2 = start(second.at[0], last.at[0], 8, across)
    y1.wait_recv()
    second[1] = (kept[1, :, b].astype(f32) + from_y[1].astype(f32)).astype(bf16)
    z2 = start(second.at[1], last.at[1], 9, low)
    mine = total(0)
    z0.wait_recv()
    y0.wait_recv()
    y2.wait_recv()
    z2.wait_recv()
    left = mine[:, :half] + from_z[0].astype(f32) + last[0].astype(f32)
    right = mine[:, half:] + from_y[0].astype(f32) + last[1].astype(f32)
    for copy in (*first.values(), z1, y1, y0, z0, y2, z2):
        copy.wait_send()
    return jnp.concatenate([left, right], axis=1)


def spread_group(at, out, start):
    core, low, across = partners(at)
    half = out.shape[2] // 2
    a, b = pl.ds(0, half), pl.ds(half, half)
    ya = start(out.at[0, :, a], out.at[1, :, a], 10, across)
    zb = start(out.at[0, :, b], out.at[2, :, b], 11, low)
    yb = start(out.at[0, :, b], out.at[1, :, b], 12, across)
    za = start(out.at[0, :, a], out.at[2, :, a], 13, low)
    c0 = start(out.at[0], out.at[4], 14, core)
    ya.wait_recv()
    zc = start(out.at[1, :, a], out.at[3, :, a], 15, low)
    zb.wait_recv()
    yc = start(out.at[2, :, b], out.at[3, :, b], 16, across)
    yb.wait_recv()
    c1 = start(out.at[1], out.at[5], 17, core)
    za.wait_recv()
    c2 = start(out.at[2], out.at[6], 18, core)
    zc.wait_recv()
    yc.wait_recv()
    c3 = start(out.at[3], out.at[7], 19, core)
    for copy in (c0, c1, c2, c3):
        copy.wait_recv()
    for copy in (ya, zb, yb, za, c0, zc, yc, c1, c2, c3):
        copy.wait_send()


def sum_spread_back_kernel(part, h_ref, c_ref, gain, dh_ref, out, grad_ref,
                           from_core, kept, second, from_z, from_y, last, send, recv):
    at = place()
    meet(at)
    start = sender(send, recv)
    db = sum_group(at, part, from_core, kept, second, from_z, from_y, last, start)
    h = h_ref[...]
    r = root_scale(h)
    n = h * r
    grad_ref[...] = jnp.sum(db * n, axis=0, keepdims=True)
    t = db * gain[...]
    dh = c_ref[...].astype(f32) + r * (t - n * jnp.mean(t * n, axis=-1, keepdims=True))
    dh_ref[...] = dh
    out[0] = dh.astype(bf16)
    spread_group(at, out, start)


def sum_out_kernel(part, h_ref, out_ref, from_core, kept, second, from_z, from_y, last, send, recv):
    at = place()
    meet(at)
    start = sender(send, recv)
    total = sum_group(at, part, from_core, kept, second, from_z, from_y, last, start)
    out_ref[...] = (h_ref[...] + total).astype(bf16)


def sum_in_kernel(part, dh_ref, x_ref, gain, out_ref, grad_ref,
                  from_core, kept, second, from_z, from_y, last, send, recv):
    at = place()
    meet(at)
    start = sender(send, recv)
    da = sum_group(at, part, from_core, kept, second, from_z, from_y, last, start)
    wide = x_ref[...].astype(f32)
    r = root_scale(wide)
    n = wide * r
    grad_ref[...] = jnp.sum(da * n, axis=0, keepdims=True)
    f = da * gain[...]
    out_ref[...] = (dh_ref[...] + r * (f - n * jnp.mean(f * n, axis=-1, keepdims=True))).astype(bf16)


class Lines:
    def __init__(self, send, recv):
        self.send, self.recv, self.used, self.open = send, recv, 0, []

    def start(self, source, target, device):
        copy = pltpu.make_async_remote_copy(
            src_ref=source,
            dst_ref=target,
            send_sem=self.send.at[self.used],
            recv_sem=self.recv.at[self.used],
            device_id=device,
            device_id_type=MESH,
        )
        copy.start()
        self.used += 1
        self.open.append(copy)
        return copy

    def close(self):
        self.settle(list(self.open))

    def settle(self, copies):
        for copy in copies:
            copy.wait_send()
        self.open = [copy for copy in self.open if all(copy is not done for done in copies)]


class Moves:
    def __init__(self, sems):
        self.sems, self.used, self.open = sems, 0, []

    def start(self, source, target):
        copy = pltpu.make_async_copy(source, target, self.sems.at[self.used])
        copy.start()
        self.used += 1
        return copy

    def save(self, source, target):
        self.open.append(self.start(source, target))

    def close(self):
        finish(self.open)


def arrive(copies):
    for copy in copies:
        copy.wait_recv()


def neighbours(at):
    core, low, across = partners(at)
    return {
        "core": core,
        "low": low,
        "across": across,
        "diag": {**core, **low},
        "high": {"ctx": at["ctx"] + 2 - 4 * at["zh"]},
        "x": {"dp": at["dp"] + 2 - 4 * at["x"]},
    }


def meet_all(near, names):
    barrier = pltpu.get_barrier_semaphore()
    for name in names:
        pl.semaphore_signal(barrier, inc=1, device_id=near[name], device_id_type=MESH)
    pl.semaphore_wait(barrier, len(names))


class Weight:
    def __init__(self, env, shard, target, by_rows, low, size):
        self.env, self.shard, self.target, self.by_rows, self.low, self.size = env, shard, target, by_rows, low, size
        self.over_z, self.own_x, self.far_x = [None, None], [None, None], [None, None]

    def mine(self):
        at, ctx_count, block = self.env["at"], self.env["ctx_count"], self.env["block"]
        spot = pl.ds(pl.multiple_of((at["dp"] * ctx_count + at["ctx"]) * block, block), block)
        return self.target.at[spot, pl.ds(self.low, self.size)] if self.by_rows else self.target.at[:, spot]

    def run(self, dx, dzh, dc):
        spot = pl.ds(run_start(self.env["at"], dx, dzh, dc, self.env["ctx_count"], self.env["block"]), 2 * self.env["block"])
        return self.target.at[spot, pl.ds(self.low, self.size)] if self.by_rows else self.target.at[:, spot]

    def cut(self, dc, dzl):
        at = self.env["at"]
        start = pl.multiple_of((flip(at["c"], dc) * 2 + flip(at["zl"], dzl)) * self.size, 128)
        return self.shard.at[:, pl.ds(start, self.size)] if self.by_rows else self.shard.at[pl.ds(start, self.size), :]

    def exchange(self):
        near, lines = self.env["near"], self.env["lines"]
        self.local = self.env["moves"].start(self.cut(0, 0), self.mine())
        self.got = [
            lines.start(self.cut(dc, dzl), self.mine(), near[name])
            for dc, dzl, name in ((0, 1, "low"), (1, 0, "core"), (1, 1, "diag"))
        ]

    def ready(self):
        self.local.wait()
        arrive(self.got)

    def send_z(self, dc):
        self.over_z[dc] = self.env["lines"].start(self.run(0, 0, dc), self.run(0, 0, dc), self.env["near"]["high"])

    def send_x(self, dc):
        self.own_x[dc] = self.env["lines"].start(self.run(0, 0, dc), self.run(0, 0, dc), self.env["near"]["x"])

    def pass_x(self, dc):
        self.over_z[dc].wait_recv()
        self.far_x[dc] = self.env["lines"].start(self.run(0, 1, dc), self.run(0, 1, dc), self.env["near"]["x"])

    def complete(self):
        arrive(self.own_x + self.far_x)


class Gains(Weight):
    def mine(self):
        return self.target.at[self.env["at"]["dp"] * self.env["ctx_count"] + self.env["at"]["ctx"]]

    def run(self, dx, dzh, dc):
        at = self.env["at"]
        return self.target.at[
            pl.ds((flip(at["x"], dx) * 2 + flip(at["c"], dc)) * self.env["ctx_count"] + flip(at["zh"], dzh) * 2, 2)
        ]

    def cut(self, dc, dzl):
        return self.shard


def tables(extra, n):
    packed = extra[n, 0]
    turned = pltpu.roll(packed, packed.shape[1] // 2, 1)
    first = lax.broadcasted_iota(jnp.int32, packed.shape, 1) < packed.shape[1] // 2
    return jnp.where(first, packed, turned), jnp.where(first, -turned, packed)


def forward_kernel(
    ctx_count, block, head,
    x_hbm, c_hbm, extra_hbm, gain_hbm, wq, wk, wv, wo, wg, wu, wd,
    a_out, raw_out, q_out, kv_out, kvp_out, o_out, lse_out, h_out, b_out, z_out, gu_out, c_out, extra_out, gains_out,
    wqkv_out, wo_out, wgu_out, wd_out,
    x, extra, gain_all, wqkv, w_o, wgu, w_d, a, raw, q, kv, kvp, o, lse, from_core, kept, second, from_z, from_y, last,
    h, b_all, z, gu, c, gains, send, recv, local,
):
    at = place()
    near = neighbours(at)
    lines, moves = Lines(send, recv), Moves(local)
    env = {"at": at, "near": near, "lines": lines, "moves": moves, "ctx_count": ctx_count, "block": block}
    part, width = x.shape[1], x.shape[2]
    q_width = q.shape[1]
    hidden = z.shape[1]
    rows = 2 * part
    meet_all(near, ("core", "low", "across", "diag", "high", "x"))

    seq = [flip(at["y"], ds) for ds in (0, 1)]
    x_low = [lines.start(x_hbm.at[seq[ds]], x.at[2 + ds], near["low"]) for ds in (0, 1)]
    e_low = lines.start(extra_hbm, extra.at[pl.ds(2, 2)], near["low"])
    units = (
        Weight(env, wq, wqkv, True, 0, q_width),
        Weight(env, wk, wqkv, True, q_width, head),
        Weight(env, wv, wqkv, True, q_width + head, head),
    )
    scale = Gains(env, gain_hbm, gain_all, True, 0, 0)
    for unit in (scale, *units):
        unit.exchange()
    x_core = [lines.start(x_hbm.at[seq[ds]], x.at[4 + ds], near["core"]) for ds in (0, 1)]
    e_core = lines.start(extra_hbm, extra.at[pl.ds(4, 2)], near["core"])
    x_own = [moves.start(x_hbm.at[seq[ds]], x.at[ds]) for ds in (0, 1)]
    e_own = moves.start(extra_hbm, extra.at[pl.ds(0, 2)])
    for unit in (scale, *units):
        unit.ready()
    in_qkv = Weight(env, None, wqkv, True, 0, wqkv.shape[1])
    for dc in (0, 1):
        scale.send_z(dc)
        scale.send_x(dc)
        in_qkv.send_z(dc)
        in_qkv.send_x(dc)
    w_out = Weight(env, wo, w_o, False, 0, q_width)
    w_gate = Weight(env, wg, wgu, True, 0, hidden)
    w_up = Weight(env, wu, wgu, True, hidden, hidden)
    w_down = Weight(env, wd, w_d, False, 0, hidden)
    w_out.exchange()
    w_gate.exchange()
    arrive(x_low)
    e_low.wait_recv()
    x_far = [lines.start(x.at[2 + ds], x.at[6 + ds], near["core"]) for ds in (0, 1)]
    e_far = lines.start(extra.at[pl.ds(2, 2)], extra.at[pl.ds(6, 2)], near["core"])
    w_up.exchange()
    w_down.exchange()
    for dc in (0, 1):
        scale.pass_x(dc)
        in_qkv.pass_x(dc)
    w_out.ready()
    for dc in (0, 1):
        w_out.send_z(dc)
        w_out.send_x(dc)
    w_gate.ready()
    w_gate.send_z(0)
    scale.complete()
    gains[...] = jnp.zeros_like(gains)
    ranks = gain_all.shape[0]
    small = gain_all[0, 2:4, :]
    for n in range(ranks):
        gains[0:2, n * block : (n + 1) * block] = gain_all[n, 0:2, :]
        if n:
            small = small + gain_all[n, 2:4, :]
    gains[2:4, 0:head] = small

    finish(x_own)
    arrive(x_core + x_far)
    e_own.wait()
    e_core.wait_recv()
    e_far.wait_recv()
    h[...] = x[0].astype(f32)

    @pl.loop(0, 8)
    def _(n):
        wide = x[n].astype(f32)
        span = pl.ds(pl.multiple_of(n * part, part), part)
        a[span, :] = (wide * root_scale(wide) * gains[0:1, :]).astype(bf16)

    in_qkv.complete()
    moves.save(wqkv, wqkv_out)
    gain_q = gains[2:3, 0:head]
    gain_k = gains[3:4, 0:head]

    @pl.loop(0, 4)
    def _(m):
        big = pl.ds(pl.multiple_of(m * rows, rows), rows)
        product = nn(a[big, :], wqkv[...])
        raw[big, :] = product[:, : q_width + head]
        for half in (0, 1):
            n = 2 * m + half
            span = pl.ds(pl.multiple_of(n * part, part), part)
            cos, sin = tables(extra, n)
            piece = product[half * part : (half + 1) * part]
            for j in range(q_width // head):
                u = piece[:, j * head : (j + 1) * head]
                q[span, pl.ds(j * head, head)] = turn(u * root_scale(u) * gain_q, cos, sin).astype(bf16)
            u = piece[:, q_width : q_width + head]
            kv[span, pl.ds(0, head)] = turn(u * root_scale(u) * gain_k, cos, sin).astype(bf16)
            kv[span, pl.ds(head, head)] = piece[:, q_width + head :].astype(bf16)

    kv_far = lines.start(kv, kvp, near["high"])
    for source, target in ((a, a_out), (raw, raw_out), (q, q_out), (kv, kv_out), (extra, extra_out), (gains, gains_out)):
        moves.save(source, target)
    for dc in (0, 1):
        w_out.pass_x(dc)
    for dc in (0, 1):
        w_gate.send_x(dc)
    kv_far.wait_recv()
    w_gate.send_z(1)
    c_own = [moves.start(c_hbm.at[seq[ds]], c.at[ds]) for ds in (0, 1)]
    c_core = [lines.start(c_hbm.at[seq[ds]], c.at[4 + ds], near["core"]) for ds in (0, 1)]
    c_low = [lines.start(c_hbm.at[seq[ds]], c.at[2 + ds], near["low"]) for ds in (0, 1)]
    moves.save(kvp, kvp_out)
    scaling = head ** (-0.5)

    @pl.loop(0, 2)
    def _(n):
        @pl.loop(0, 2)
        def _(m):
            base = pl.multiple_of(n * (4 * part) + m * part, part)
            keys = jnp.concatenate([pair_rows(kv, base, part, (0, head)), pair_rows(kvp, base, part, (0, head))], axis=0)
            values = jnp.concatenate(
                [pair_rows(kv, base, part, (head, 2 * head)), pair_rows(kvp, base, part, (head, 2 * head))], axis=0
            )
            allowed = allowed_pairs(at, n, m, part, q_width // head, extra)
            scores = jnp.where(allowed, nt(stack_heads(q, base, part, head), keys) * scaling, -jnp.inf)
            peak = jnp.max(scores, axis=-1, keepdims=True)
            weights = jnp.exp(scores - peak)
            total = jnp.sum(weights, axis=-1, keepdims=True)
            mixed = nn(weights.astype(bf16), values) / total
            unstack(o, base, part, head, mixed)
            unstack(lse, base, part, head, jnp.broadcast_to(peak + jnp.log(total), mixed.shape))

    moves.save(o, o_out)
    moves.save(lse, lse_out)
    w_out.complete()
    moves.save(w_o, wo_out)
    out = x
    lines.settle(x_far)

    def project(first):
        @pl.loop(0, 4)
        def _(m):
            n = first + m
            span = pl.ds(pl.multiple_of(n * part, part), part)
            out[n] = nn(o[span, :], w_o[...]).astype(bf16)

    project(4)
    sent = {k: lines.start(out.at[4 + k], from_core.at[k], near["core"]) for k in (3, 1, 2, 0)}
    project(0)

    def pump_gate():
        for dc in (0, 1):
            w_gate.pass_x(dc)
        w_up.ready()
        for dc in (0, 1):
            w_up.send_z(dc)
            w_up.send_x(dc)
        arrive(c_low)
        return [lines.start(c.at[2 + ds], c.at[6 + ds], near["core"]) for ds in (0, 1)]

    sums, c_far = sum_lines(near, lines, out, sent, from_core, kept, second, from_z, from_y, last, pump_gate)
    h[...] = h[...] + sums
    moves.save(h, h_out)
    wide = h[...]
    b_all[0] = (wide * root_scale(wide) * gains[1:2, :]).astype(bf16)

    def pump_up():
        for dc in (0, 1):
            w_up.pass_x(dc)
        w_down.ready()
        for dc in (0, 1):
            w_down.send_z(dc)
            w_down.send_x(dc)

    spread_lines(near, lines, b_all, pump_up)
    moves.save(b_all, b_out)

    w_gate.complete()

    w_up.complete()
    moves.save(wgu, wgu_out)

    @pl.loop(0, 4)
    def _(m):
        span = pl.ds(pl.multiple_of(m * rows, rows), rows)
        b = pair(b_all, m)
        g = nn(b, wgu[:, 0:hidden])
        u = nn(b, wgu[:, hidden : 2 * hidden])
        gu[span, pl.ds(0, hidden)] = g.astype(bf16)
        gu[span, pl.ds(hidden, hidden)] = u.astype(bf16)
        z[span, :] = (g * jax.nn.sigmoid(g) * u).astype(bf16)

    moves.save(z, z_out)
    moves.save(gu, gu_out)
    finish(c_own)
    arrive(c_core + c_far)
    moves.save(c, c_out)
    for dc in (0, 1):
        w_down.pass_x(dc)
    w_down.complete()
    moves.save(w_d, wd_out)
    lines.close()
    moves.close()


def pair(ref, m):
    return jnp.concatenate([ref[2 * m], ref[2 * m + 1]], axis=0)


def sum_lines(near, lines, part, first, from_core, kept, second, from_z, from_y, last, pump):
    half = part.shape[2] // 2
    a, b = pl.ds(0, half), pl.ds(half, half)

    def total(k):
        first[k].wait_recv()
        return part[k].astype(f32) + from_core[k].astype(f32)

    kept[2] = total(3).astype(bf16)
    z1 = lines.start(kept.at[2, :, a], from_z.at[1], near["low"])
    y1 = lines.start(kept.at[2, :, b], from_y.at[1], near["across"])
    kept[0] = total(1).astype(bf16)
    y0 = lines.start(kept.at[0, :, b], from_y.at[0], near["across"])
    kept[1] = total(2).astype(bf16)
    z0 = lines.start(kept.at[1, :, a], from_z.at[0], near["low"])
    z1.wait_recv()
    second[0] = (kept[0, :, a].astype(f32) + from_z[1].astype(f32)).astype(bf16)
    y2 = lines.start(second.at[0], last.at[0], near["across"])
    y1.wait_recv()
    second[1] = (kept[1, :, b].astype(f32) + from_y[1].astype(f32)).astype(bf16)
    z2 = lines.start(second.at[1], last.at[1], near["low"])
    extra = pump()
    mine = total(0)
    arrive((z0, y0, y2, z2))
    left = mine[:, :half] + from_z[0].astype(f32) + last[0].astype(f32)
    right = mine[:, half:] + from_y[0].astype(f32) + last[1].astype(f32)
    return jnp.concatenate([left, right], axis=1), extra


def spread_lines(near, lines, out, pump):
    half = out.shape[2] // 2
    a, b = pl.ds(0, half), pl.ds(half, half)
    ya = lines.start(out.at[0, :, a], out.at[1, :, a], near["across"])
    zb = lines.start(out.at[0, :, b], out.at[2, :, b], near["low"])
    yb = lines.start(out.at[0, :, b], out.at[1, :, b], near["across"])
    za = lines.start(out.at[0, :, a], out.at[2, :, a], near["low"])
    c0 = lines.start(out.at[0], out.at[4], near["core"])
    ya.wait_recv()
    zc = lines.start(out.at[1, :, a], out.at[3, :, a], near["low"])
    zb.wait_recv()
    yc = lines.start(out.at[2, :, b], out.at[3, :, b], near["across"])
    yb.wait_recv()
    c1 = lines.start(out.at[1], out.at[5], near["core"])
    za.wait_recv()
    c2 = lines.start(out.at[2], out.at[6], near["core"])
    zc.wait_recv()
    yc.wait_recv()
    c3 = lines.start(out.at[3], out.at[7], near["core"])
    pump()
    arrive((c0, c1, c2, c3))


VM = pl.BlockSpec(memory_space=pltpu.VMEM)
HB = pl.BlockSpec(memory_space=pl.ANY)


def shaped(shape, dtype):
    return jax.ShapeDtypeStruct(shape, dtype)


def local_call(kernel, outs, args, specs, scratch=()):
    return pl.pallas_call(
        kernel,
        out_shape=tuple(outs),
        in_specs=list(specs),
        out_specs=tuple(VM for _ in outs),
        scratch_shapes=list(scratch),
        compiler_params=pltpu.CompilerParams(vmem_limit_bytes=60 * 1024 * 1024),
    )(*args)


def group_call(kernel, number, outs, args, part, width, copies):
    half = width // 2
    return pl.pallas_call(
        kernel,
        out_shape=tuple(outs),
        in_specs=[VM for _ in args],
        out_specs=tuple(VM for _ in outs),
        scratch_shapes=[
            pltpu.VMEM((4, part, width), bf16),
            pltpu.VMEM((3, part, width), bf16),
            pltpu.VMEM((2, part, half), bf16),
            pltpu.VMEM((2, part, half), bf16),
            pltpu.VMEM((2, part, half), bf16),
            pltpu.VMEM((2, part, half), bf16),
            pltpu.SemaphoreType.DMA((copies,)),
            pltpu.SemaphoreType.DMA((copies,)),
        ],
        compiler_params=pltpu.CompilerParams(
            collective_id=number, has_side_effects=True, vmem_limit_bytes=60 * 1024 * 1024
        ),
    )(*args)


def split_device(
    block_input, doc_positions, out_cotangent, attn_gain, mlp_gain, query_gain, key_gain,
    w_query, w_key, w_value, w_out, w_gate, w_up, w_down,
):
    dp_count = lax.axis_size("dp")
    ctx_count = lax.axis_size("ctx")
    rank_count = dp_count * ctx_count
    ZL, ZH, C, X = 1, 2, ctx_count, 2 * ctx_count
    at = place()
    rank = at["dp"] * ctx_count + at["ctx"]
    upper = at["y"] == 1
    zl_on = at["zl"] == 1
    c_on = at["c"] == 1
    seqs, part, width = block_input.shape
    block = attn_gain.shape[0]
    head_piece = query_gain.shape[0]
    head = head_piece * rank_count
    masks = (0, ZL, C, C | ZL)

    def swap(value, mask):
        return lax.ppermute(value, ("dp", "ctx"), [(i, i ^ mask) for i in range(rank_count)])

    def swap_y(value):
        return lax.ppermute(value, "mp", [(0, 1), (1, 0)])

    own_p = jnp.where(upper, doc_positions[::-1], doc_positions).astype(f32)
    inverse = rope_base ** (-2.0 * jnp.arange(head // 2).astype(f32) / head)
    angles = own_p[:, :, None] * inverse
    extra = jnp.stack(
        [jnp.concatenate([jnp.cos(angles), jnp.sin(angles)], axis=2), jnp.broadcast_to(own_p[:, :, None], (seqs, part, head))],
        axis=1,
    )
    small = jnp.stack([query_gain, key_gain]).astype(f32)
    small = lax.dynamic_update_slice(jnp.zeros((2, head), f32), small, (0, rank * head_piece))
    own_gains = jnp.concatenate([jnp.stack([attn_gain, mlp_gain]).astype(f32), small, jnp.zeros((4, block), f32)])

    tokens = 4 * seqs * part
    q_width = w_query.shape[1] // 4
    hidden = w_gate.shape[1] // 4
    bound = functools.partial
    eighths = (8, part, width)
    half = (2, part, width // 2)
    shapes = {
        "a": ((tokens, width), bf16), "raw": ((tokens, q_width + head), f32), "q": ((tokens, q_width), bf16),
        "kv": ((tokens, 2 * head), bf16), "kvp": ((tokens, 2 * head), bf16), "o": ((tokens, q_width), bf16),
        "lse": ((tokens, q_width), f32), "h": ((part, width), f32), "b": (eighths, bf16), "z": ((tokens, hidden), bf16),
        "gu": ((tokens, 2 * hidden), bf16), "c": (eighths, bf16), "extra": ((8, 2, part, head), f32), "gains": ((8, width), f32),
        "wqkv": ((width, q_width + 2 * head), bf16), "wo": ((q_width, width), bf16),
        "wgu": ((width, 2 * hidden), bf16), "wd": ((hidden, width), bf16),
    }
    room = {name: pltpu.VMEM(*spec) for name, spec in shapes.items()}
    kept = pl.pallas_call(
        bound(forward_kernel, ctx_count, block, head),
        out_shape=[shaped(*spec) for spec in shapes.values()],
        in_specs=[HB] * 11,
        out_specs=[HB] * len(shapes),
        scratch_shapes=[
            pltpu.VMEM(eighths, bf16), room["extra"], pltpu.VMEM((rank_count, 8, block), f32),
            room["wqkv"], room["wo"], room["wgu"], room["wd"], room["a"], room["raw"], room["q"], room["kv"], room["kvp"],
            room["o"], room["lse"], pltpu.VMEM((4, part, width), bf16), pltpu.VMEM((3, part, width), bf16),
            pltpu.VMEM(half, bf16), pltpu.VMEM(half, bf16), pltpu.VMEM(half, bf16), pltpu.VMEM(half, bf16),
            room["h"], room["b"], room["z"], room["gu"], room["c"], room["gains"],
            pltpu.SemaphoreType.DMA((160,)), pltpu.SemaphoreType.DMA((160,)), pltpu.SemaphoreType.DMA((64,)),
        ],
        compiler_params=pltpu.CompilerParams(collective_id=0, has_side_effects=True, vmem_limit_bytes=63 * 1024 * 1024),
    )(block_input, out_cotangent, extra, own_gains, w_query, w_key, w_value, w_out, w_gate, w_up, w_down)
    kept = dict(zip(shapes, kept))
    q, kv, kvp, o, lse, h, z, gu, raw, a = (kept[k] for k in ("q", "kv", "kvp", "o", "lse", "h", "z", "gu", "raw", "a"))
    b_all = kept["b"].reshape(tokens, width)
    cs = [kept["c"][2 * n : 2 * n + 2].reshape(2 * part, width) for n in range(4)]
    x_mine = jnp.where(upper, block_input[1], block_input[0])
    c_mine = cs[0][:part]
    gains = kept["gains"]
    gain_attn, gain_mlp = gains[0:1], gains[1:2]

    def plus(*values):
        total = values[0].astype(f32)
        for value in values[1:]:
            total = total + value.astype(f32)
        return total.astype(bf16)

    def home(quarters, axis):
        far = swap(quarters[3], X)
        near = swap(quarters[2], X)
        over_z = swap(plus(quarters[1], far), ZH)
        piece = plus(quarters[0], near, over_z)
        sent = []
        for dc in (0, 1):
            lo, hi = jnp.split(piece[dc], 2, axis=axis)
            sent += [jnp.where(zl_on, hi, lo), jnp.where(zl_on, lo, hi)]
        got = [sent[0]] + [swap(sent[k], masks[k]) for k in (1, 2, 3)]
        got = [
            jnp.where(zl_on, got[1], got[0]), jnp.where(zl_on, got[0], got[1]),
            jnp.where(zl_on, got[3], got[2]), jnp.where(zl_on, got[2], got[3]),
        ]
        return [jnp.where(c_on, got[k ^ 2], got[k]) for k in range(4)]

    quarter = [shaped((2, hidden, 2 * block), bf16)] * 4
    grads_down = local_call(bound(grad_cols_kernel, ctx_count, block), quarter, (z, *cs), [VM] * 5)
    dgu, part_b = local_call(
        bound(gate_back_kernel, ctx_count, block),
        [shaped((tokens, 2 * hidden), bf16), shaped((tokens, width), bf16)],
        (*cs, gu, kept["wd"], kept["wgu"]),
        [VM] * 7,
    )
    quarter = [shaped((2, 2 * block, 2 * hidden), bf16)] * 4
    grads_gate = local_call(bound(grad_rows_kernel, ctx_count, block), quarter, (b_all, dgu), [VM] * 2)
    dh, dh_all, mlp_gain_part = group_call(
        sum_spread_back_kernel, 1,
        [shaped((part, width), f32), shaped(eighths, bf16), shaped((1, width), f32)],
        (part_b.reshape(eighths), h, c_mine, gain_mlp), part, width, 20,
    )
    dh_all = dh_all.reshape(tokens, width)
    dq, dkv, dkvp = local_call(
        bound(attend_back_kernel, ctx_count, block, part, head),
        [shaped((tokens, q_width), f32), shaped((tokens, 2 * head), f32), shaped((tokens, 2 * head), bf16)],
        (dh_all, o, q, kv, kvp, lse, kept["extra"], kept["wo"]),
        [VM] * 8,
        [pltpu.VMEM((tokens, q_width), bf16)],
    )
    got_kv = swap(dkvp, ZH)
    quarter = [shaped((2, q_width, 2 * block), bf16)] * 4
    grads_out = local_call(bound(grad_wide_kernel, ctx_count, block), quarter, (o, dh_all), [VM] * 2)
    (part_d,) = local_call(
        bound(down_kernel, ctx_count, block), [shaped((tokens, width), bf16)],
        (z, kept["wd"]), [VM] * 2,
    )
    (out_mine,) = group_call(
        sum_out_kernel, 2, [shaped((part, width), bf16)], (part_d.reshape(eighths), h), part, width, 10,
    )
    dqkv, part_a, gq_part, gk_part = local_call(
        bound(qkv_back_kernel, ctx_count, block),
        [
            shaped((tokens, q_width + 2 * head), bf16),
            shaped((tokens, width), bf16),
            shaped((1, head), f32),
            shaped((1, head), f32),
        ],
        (dq, dkv, got_kv, raw, kept["extra"], gains, kept["wqkv"]),
        [VM] * 7,
    )
    quarter = [shaped((2, 2 * block, q_width + 2 * head), bf16)] * 4
    grads_qkv = local_call(bound(grad_rows_kernel, ctx_count, block), quarter, (a, dqkv), [VM] * 2)
    in_mine, attn_gain_part = group_call(
        sum_in_kernel, 3, [shaped((part, width), bf16), shaped((1, width), f32)],
        (part_a.reshape(eighths), dh, x_mine, gain_attn), part, width, 10,
    )

    def both(mine):
        other = swap_y(mine)
        return jnp.stack([jnp.where(upper, other, mine), jnp.where(upper, mine, other)])

    block_output = both(out_mine)
    input_grad = both(in_mine).astype(f32)
    home_down = home(grads_down, 1)
    home_gate = home(grads_gate, 0)
    home_out = home(grads_out, 1)
    home_qkv = home(grads_qkv, 0)

    totals = jnp.concatenate(
        [
            attn_gain_part.reshape(rank_count, block),
            mlp_gain_part.reshape(rank_count, block),
            gq_part.reshape(rank_count, head_piece),
            gk_part.reshape(rank_count, head_piece),
        ],
        axis=1,
    )
    totals = jnp.take(totals, jnp.arange(rank_count) ^ rank, axis=0)
    for mask in (X, C, ZH, ZL):
        many = totals.shape[0] // 2
        totals = totals[:many] + swap(totals[many:], mask)
    totals = (totals + swap_y(totals))[0]

    def side(blocks, low, high):
        return jnp.concatenate([t[:, low:high] for t in blocks], axis=1).astype(f32)

    return (
        block_output,
        input_grad,
        totals[:block],
        totals[block : 2 * block],
        totals[2 * block : 2 * block + head_piece],
        totals[2 * block + head_piece :],
        side(home_qkv, 0, q_width),
        side(home_qkv, q_width, q_width + head),
        side(home_qkv, q_width + head, q_width + 2 * head),
        jnp.concatenate(home_out, axis=0).astype(f32),
        side(home_gate, 0, hidden),
        side(home_gate, hidden, 2 * hidden),
        jnp.concatenate(home_down, axis=0).astype(f32),
    )


def rms_scale(value_rows):
    return lax.rsqrt(jnp.mean(value_rows * value_rows, axis=-1, keepdims=True) + eps_norm)


def rope_tables(places, head_size):
    half_size = head_size // 2
    inverse = rope_base ** (-2.0 * jnp.arange(half_size).astype(jnp.float32) / head_size)
    angles = places.astype(jnp.float32)[:, None] * inverse[None, :]
    angles = jnp.concatenate([angles, angles], axis=-1)
    return (jnp.cos(angles), jnp.sin(angles))


def rotate(values, cosine, sine):
    half_size = values.shape[-1] // 2
    turned = jnp.concatenate([-values[..., half_size:], values[..., :half_size]], axis=-1)
    return values * cosine[:, None, :] + turned * sine[:, None, :]


def rotate_back(grads, cosine, sine):
    half_size = grads.shape[-1] // 2
    weighted = grads * sine[:, None, :]
    return grads * cosine[:, None, :] + jnp.concatenate(
        [weighted[..., half_size:], -weighted[..., :half_size]], axis=-1
    )


def block_mask(query_index, lowest, key_index):
    return (key_index[None, :] <= query_index[:, None]) & (key_index[None, :] >= lowest[:, None])


def dot_nt(left, right):
    return lax.dot_general(
        left, right, (((1,), (1,)), ((), ())), preferred_element_type=jnp.float32
    )


def dot_tn(left, right):
    return lax.dot_general(
        left, right, (((0,), (0,)), ((), ())), preferred_element_type=jnp.float32
    )


def micro_pass(inputs_seq, places, cotangent, shards, totals):
    float_type = jnp.float32
    half_type = jnp.bfloat16
    fetched = (
        lax.all_gather(shards[0], ("dp", "ctx"), axis=0, tiled=True),
        lax.all_gather(shards[1], ("dp", "ctx"), axis=0, tiled=True),
        lax.all_gather(shards[2], ("dp", "ctx"), axis=0, tiled=True),
        lax.all_gather(shards[3], ("dp", "ctx"), axis=0, tiled=True),
        lax.all_gather(shards[4], ("dp", "ctx"), axis=0, tiled=True),
        lax.all_gather(shards[5], ("dp", "ctx"), axis=0, tiled=True),
        lax.all_gather(shards[6], ("dp", "ctx"), axis=0, tiled=True),
        lax.all_gather(shards[7], ("dp", "ctx"), axis=1, tiled=True),
        lax.all_gather(shards[8], ("dp", "ctx"), axis=0, tiled=True),
        lax.all_gather(shards[9], ("dp", "ctx"), axis=0, tiled=True),
        lax.all_gather(shards[10], ("dp", "ctx"), axis=1, tiled=True),
    )
    gain_attn = fetched[0].astype(float_type)
    gain_mlp = fetched[1].astype(float_type)
    gain_query = fetched[2].astype(float_type)
    gain_key = fetched[3].astype(float_type)
    query_proj, key_proj, value_proj, out_proj, gate_proj, up_proj, down_proj = fetched[4:]
    head_size = gain_query.shape[0]
    head_count = query_proj.shape[1] // head_size
    kv_count = key_proj.shape[1] // head_size
    group_size = head_count // kv_count
    token_count = inputs_seq.shape[0]
    ctx_count = lax.axis_size("ctx")
    ctx_rank = lax.axis_index("ctx")
    scaling = head_size ** (-0.5)
    query_index = ctx_rank * token_count + jnp.arange(token_count, dtype=jnp.int32)
    lowest = query_index - places
    last_query = ctx_rank * token_count + token_count - 1
    residual_in = inputs_seq.astype(float_type)
    scale_attn = rms_scale(residual_in)
    normed_attn = residual_in * scale_attn
    attn_input = (normed_attn * gain_attn).astype(half_type)
    query_raw = jnp.dot(attn_input, query_proj, preferred_element_type=float_type).reshape(
        token_count, head_count, head_size
    )
    key_raw = jnp.dot(attn_input, key_proj, preferred_element_type=float_type).reshape(
        token_count, kv_count, head_size
    )
    value_rows = jnp.dot(attn_input, value_proj, preferred_element_type=float_type).astype(
        half_type
    )
    query_scale = rms_scale(query_raw)
    query_normed = query_raw * query_scale
    key_scale = rms_scale(key_raw)
    key_normed = key_raw * key_scale
    cosine, sine = rope_tables(places, head_size)
    query_rot = rotate(query_normed * gain_query, cosine, sine).astype(half_type)
    key_rot = (
        rotate(key_normed * gain_key, cosine, sine)
        .astype(half_type)
        .reshape(token_count, kv_count * head_size)
    )
    query_group = query_rot.reshape(token_count, kv_count, group_size, head_size)
    initial = (
        jnp.full((kv_count, group_size, token_count), -1e30, float_type),
        jnp.zeros((kv_count, group_size, token_count), float_type),
        jnp.zeros((token_count, kv_count, group_size, head_size), float_type),
    )
    pieces = (
        lax.all_gather(key_rot, "ctx", axis=0, tiled=True),
        lax.all_gather(value_rows, "ctx", axis=0, tiled=True),
    )
    row_count = pieces[0].shape[0]
    key_piece = pieces[0].reshape(row_count, kv_count, head_size)
    value_piece = pieces[1].reshape(row_count, kv_count, head_size)

    def fold_attend(state):
        peak, total, running = state
        scores = (
            jnp.einsum("qkgd,jkd->kgqj", query_group, key_piece, preferred_element_type=float_type)
            * scaling
        )
        allowed = block_mask(query_index, lowest, jnp.arange(row_count, dtype=jnp.int32))
        new_peak = jnp.maximum(peak, jnp.max(jnp.where(allowed, scores, -jnp.inf), axis=-1))
        weights = jnp.where(allowed, jnp.exp(scores - new_peak[..., None]), 0.0)
        total = jnp.sum(weights, axis=-1)
        running = jnp.einsum(
            "kgqj,jkd->qkgd",
            weights.astype(half_type),
            value_piece,
            preferred_element_type=float_type,
        )
        return (new_peak, total, running)

    peak, total, running = lax.cond(
        jnp.int32(0) <= last_query, fold_attend, lambda state: state, initial
    )
    attn_rows = (
        (running / jnp.transpose(total, (2, 0, 1))[..., None])
        .astype(half_type)
        .reshape(token_count, head_count * head_size)
    )
    log_total = peak + jnp.log(total)
    attn_out = lax.psum(
        jnp.dot(attn_rows, out_proj, preferred_element_type=float_type).astype(jnp.bfloat16), "mp"
    ).astype(jnp.float32)
    middle = residual_in + attn_out
    scale_mlp = rms_scale(middle)
    normed_mlp = middle * scale_mlp
    mlp_input = (normed_mlp * gain_mlp).astype(half_type)
    gate_rows = jnp.dot(mlp_input, gate_proj, preferred_element_type=float_type)
    up_rows = jnp.dot(mlp_input, up_proj, preferred_element_type=float_type)
    sigmoid_gate = jax.nn.sigmoid(gate_rows)
    hidden_rows = (gate_rows * sigmoid_gate * up_rows).astype(half_type)
    mlp_out = lax.psum(
        jnp.dot(hidden_rows, down_proj, preferred_element_type=float_type).astype(jnp.bfloat16),
        "mp",
    ).astype(jnp.float32)
    block_output = (middle + mlp_out).astype(half_type)
    refetched = (
        lax.all_gather(shards[0], ("dp", "ctx"), axis=0, tiled=True),
        lax.all_gather(shards[1], ("dp", "ctx"), axis=0, tiled=True),
        lax.all_gather(shards[2], ("dp", "ctx"), axis=0, tiled=True),
        lax.all_gather(shards[3], ("dp", "ctx"), axis=0, tiled=True),
        lax.all_gather(shards[4], ("dp", "ctx"), axis=0, tiled=True),
        lax.all_gather(shards[5], ("dp", "ctx"), axis=0, tiled=True),
        lax.all_gather(shards[6], ("dp", "ctx"), axis=0, tiled=True),
        lax.all_gather(shards[7], ("dp", "ctx"), axis=1, tiled=True),
        lax.all_gather(shards[8], ("dp", "ctx"), axis=0, tiled=True),
        lax.all_gather(shards[9], ("dp", "ctx"), axis=0, tiled=True),
        lax.all_gather(shards[10], ("dp", "ctx"), axis=1, tiled=True),
    )
    gain_attn = refetched[0].astype(float_type)
    gain_mlp = refetched[1].astype(float_type)
    gain_query = refetched[2].astype(float_type)
    gain_key = refetched[3].astype(float_type)
    query_proj, key_proj, value_proj, out_proj, gate_proj, up_proj, down_proj = refetched[4:]
    down_grad = dot_tn(hidden_rows, cotangent)
    hidden_grad = dot_nt(cotangent, down_proj)
    gate_grad = (
        hidden_grad * up_rows * sigmoid_gate * (1.0 + gate_rows * (1.0 - sigmoid_gate))
    ).astype(half_type)
    up_grad = (hidden_grad * gate_rows * sigmoid_gate).astype(half_type)
    gate_proj_grad = dot_tn(mlp_input, gate_grad)
    up_proj_grad = dot_tn(mlp_input, up_grad)
    mlp_in_grad = lax.psum(
        (dot_nt(gate_grad, gate_proj) + dot_nt(up_grad, up_proj)).astype(jnp.bfloat16), "mp"
    ).astype(jnp.float32)
    mlp_gain_grad = jnp.sum(mlp_in_grad * normed_mlp, axis=0)
    normed_grad = mlp_in_grad * gain_mlp
    middle_grad = cotangent.astype(float_type) + scale_mlp * (
        normed_grad - normed_mlp * jnp.mean(normed_grad * normed_mlp, axis=-1, keepdims=True)
    )
    middle_half = middle_grad.astype(half_type)
    out_proj_grad = dot_tn(attn_rows, middle_half)
    attn_grad = dot_nt(middle_half, out_proj).astype(half_type)
    grad_group = attn_grad.reshape(token_count, kv_count, group_size, head_size)
    attn_group = attn_rows.reshape(token_count, kv_count, group_size, head_size)
    row_dot = jnp.einsum(
        "qkgd,qkgd->kgq", grad_group, attn_group, preferred_element_type=float_type
    )
    key_back, value_back = (
        lax.all_gather(key_rot, "ctx", axis=0, tiled=True),
        lax.all_gather(value_rows, "ctx", axis=0, tiled=True),
    )

    def back_block(query_sum, block_id):
        start = block_id * token_count
        key_piece = lax.dynamic_slice_in_dim(key_back, start, token_count, 0).reshape(
            token_count, kv_count, head_size
        )
        value_piece = lax.dynamic_slice_in_dim(value_back, start, token_count, 0).reshape(
            token_count, kv_count, head_size
        )

        def back_attend(running):
            scores = (
                jnp.einsum(
                    "qkgd,jkd->kgqj", query_group, key_piece, preferred_element_type=float_type
                )
                * scaling
            )
            allowed = block_mask(
                query_index, lowest, start + jnp.arange(token_count, dtype=jnp.int32)
            )
            probs = jnp.where(allowed, jnp.exp(scores - log_total[..., None]), 0.0)
            value_part = jnp.einsum(
                "kgqj,qkgd->jkd",
                probs.astype(half_type),
                grad_group,
                preferred_element_type=float_type,
            )
            prob_grad = jnp.einsum(
                "qkgd,jkd->kgqj", grad_group, value_piece, preferred_element_type=float_type
            )
            score_half = (probs * (prob_grad - row_dot[..., None])).astype(half_type)
            query_part = (
                jnp.einsum(
                    "kgqj,jkd->qkgd", score_half, key_piece, preferred_element_type=float_type
                )
                * scaling
            )
            key_part = (
                jnp.einsum(
                    "kgqj,qkgd->jkd", score_half, query_group, preferred_element_type=float_type
                )
                * scaling
            )
            return (
                running + query_part,
                jnp.concatenate(
                    [
                        key_part.reshape(token_count, kv_count * head_size),
                        value_part.reshape(token_count, kv_count * head_size),
                    ],
                    axis=-1,
                ),
            )

        def passing(running):
            return (running, jnp.zeros((token_count, 2 * kv_count * head_size), float_type))

        return lax.cond(start <= last_query, back_attend, passing, query_sum)

    query_grad, kv_terms = lax.scan(
        back_block,
        jnp.zeros((token_count, kv_count, group_size, head_size), float_type),
        jnp.arange(ctx_count, dtype=jnp.int32),
    )
    kv_grad = lax.psum_scatter(
        kv_terms.reshape(ctx_count * token_count, 2 * kv_count * head_size).astype(jnp.bfloat16),
        "ctx",
        scatter_dimension=0,
        tiled=True,
    ).astype(jnp.float32)
    key_rot_grad = kv_grad[:, : kv_count * head_size].reshape(token_count, kv_count, head_size)
    value_half = kv_grad[:, kv_count * head_size :].astype(half_type)
    query_back = rotate_back(query_grad.reshape(token_count, head_count, head_size), cosine, sine)
    key_grad_back = rotate_back(key_rot_grad, cosine, sine)
    query_gain_part = jnp.sum(query_back * query_normed, axis=(0, 1))
    key_gain_part = jnp.sum(key_grad_back * key_normed, axis=(0, 1))
    query_ngrad = query_back * gain_query
    key_ngrad = key_grad_back * gain_key
    query_half = (
        (
            query_scale
            * (
                query_ngrad
                - query_normed * jnp.mean(query_ngrad * query_normed, axis=-1, keepdims=True)
            )
        )
        .reshape(token_count, head_count * head_size)
        .astype(half_type)
    )
    key_half = (
        (
            key_scale
            * (key_ngrad - key_normed * jnp.mean(key_ngrad * key_normed, axis=-1, keepdims=True))
        )
        .reshape(token_count, kv_count * head_size)
        .astype(half_type)
    )
    query_proj_grad = dot_tn(attn_input, query_half)
    key_proj_grad = dot_tn(attn_input, key_half)
    value_proj_grad = dot_tn(attn_input, value_half)
    attn_in_grad, query_gain_sum, key_gain_sum = (
        lax.psum(
            (
                dot_nt(query_half, query_proj)
                + dot_nt(key_half, key_proj)
                + dot_nt(value_half, value_proj)
            ).astype(jnp.bfloat16),
            "mp",
        ).astype(jnp.float32),
        lax.psum(query_gain_part.astype(jnp.bfloat16), "mp").astype(jnp.float32),
        lax.psum(key_gain_part.astype(jnp.bfloat16), "mp").astype(jnp.float32),
    )
    attn_gain_grad = jnp.sum(attn_in_grad * normed_attn, axis=0)
    normed_in_grad = attn_in_grad * gain_attn
    input_grad = middle_grad + scale_attn * (
        normed_in_grad
        - normed_attn * jnp.mean(normed_in_grad * normed_attn, axis=-1, keepdims=True)
    )
    addition = (
        attn_gain_grad,
        mlp_gain_grad,
        query_gain_sum,
        key_gain_sum,
        query_proj_grad,
        key_proj_grad,
        value_proj_grad,
        out_proj_grad,
        gate_proj_grad,
        up_proj_grad,
        down_grad,
    )
    totals = tuple((earlier + later for earlier, later in zip(totals, addition)))
    return (block_output, input_grad, totals)


def on_device(
    block_input,
    doc_positions,
    out_cotangent,
    attn_gain,
    mlp_gain,
    query_gain,
    key_gain,
    w_query,
    w_key,
    w_value,
    w_out,
    w_gate,
    w_up,
    w_down,
):
    shards = (
        attn_gain,
        mlp_gain,
        query_gain,
        key_gain,
        w_query,
        w_key,
        w_value,
        w_out,
        w_gate,
        w_up,
        w_down,
    )
    head_size = query_gain.shape[0] * lax.axis_size(("dp", "ctx"))
    model_width = block_input.shape[2]
    query_width = w_query.shape[1]
    kv_width = w_key.shape[1]
    hidden_width = w_gate.shape[1]
    totals = (
        jnp.zeros((model_width,), jnp.float32),
        jnp.zeros((model_width,), jnp.float32),
        jnp.zeros((head_size,), jnp.float32),
        jnp.zeros((head_size,), jnp.float32),
        jnp.zeros((model_width, query_width), jnp.float32),
        jnp.zeros((model_width, kv_width), jnp.float32),
        jnp.zeros((model_width, kv_width), jnp.float32),
        jnp.zeros((query_width, model_width), jnp.float32),
        jnp.zeros((model_width, hidden_width), jnp.float32),
        jnp.zeros((model_width, hidden_width), jnp.float32),
        jnp.zeros((hidden_width, model_width), jnp.float32),
    )
    output_list = []
    grad_list = []
    for micro in range(block_input.shape[0]):
        output_rows, input_rows, totals = micro_pass(
            block_input[micro], doc_positions[micro], out_cotangent[micro], shards, totals
        )
        output_list.append(output_rows)
        grad_list.append(input_rows)
    owned = (
        lax.psum_scatter(totals[0], ("dp", "ctx"), scatter_dimension=0, tiled=True),
        lax.psum_scatter(totals[1], ("dp", "ctx"), scatter_dimension=0, tiled=True),
        lax.psum_scatter(totals[2], ("dp", "ctx"), scatter_dimension=0, tiled=True),
        lax.psum_scatter(totals[3], ("dp", "ctx"), scatter_dimension=0, tiled=True),
        lax.psum_scatter(totals[4], ("dp", "ctx"), scatter_dimension=0, tiled=True),
        lax.psum_scatter(totals[5], ("dp", "ctx"), scatter_dimension=0, tiled=True),
        lax.psum_scatter(totals[6], ("dp", "ctx"), scatter_dimension=0, tiled=True),
        lax.psum_scatter(totals[7], ("dp", "ctx"), scatter_dimension=1, tiled=True),
        lax.psum_scatter(totals[8], ("dp", "ctx"), scatter_dimension=0, tiled=True),
        lax.psum_scatter(totals[9], ("dp", "ctx"), scatter_dimension=0, tiled=True),
        lax.psum_scatter(totals[10], ("dp", "ctx"), scatter_dimension=1, tiled=True),
    )
    return (
        jnp.stack(output_list),
        jnp.stack(grad_list),
        owned[0],
        owned[1],
        owned[2],
        owned[3],
        owned[4],
        owned[5],
        owned[6],
        owned[7],
        owned[8],
        owned[9],
        owned[10],
    )


def choose(mesh, arrays):
    dp, ctx, mp = mesh.shape["dp"], mesh.shape["ctx"], mesh.shape["mp"]
    width = arrays[0].shape[2]
    paired = dp == 4 and ctx == 4 and mp == 2
    return split_device if paired and width % (dp * ctx * 128) == 0 else on_device


def solution(mesh):
    in_specs = (
        P("dp", "ctx", None),
        P("dp", "ctx"),
        P("dp", "ctx", None),
        P(("dp", "ctx")),
        P(("dp", "ctx")),
        P(("dp", "ctx")),
        P(("dp", "ctx")),
        P(("dp", "ctx"), "mp"),
        P(("dp", "ctx"), "mp"),
        P(("dp", "ctx"), "mp"),
        P("mp", ("dp", "ctx")),
        P(("dp", "ctx"), "mp"),
        P(("dp", "ctx"), "mp"),
        P("mp", ("dp", "ctx")),
    )
    out_specs = (
        P("dp", "ctx", None),
        P("dp", "ctx", None),
        P(("dp", "ctx")),
        P(("dp", "ctx")),
        P(("dp", "ctx")),
        P(("dp", "ctx")),
        P(("dp", "ctx"), "mp"),
        P(("dp", "ctx"), "mp"),
        P(("dp", "ctx"), "mp"),
        P("mp", ("dp", "ctx")),
        P(("dp", "ctx"), "mp"),
        P(("dp", "ctx"), "mp"),
        P("mp", ("dp", "ctx")),
    )

    def run(*arrays):
        return jax.shard_map(
            choose(mesh, arrays), mesh=mesh, in_specs=in_specs, out_specs=out_specs, check_vma=False
        )(*arrays)

    return run
```

```python
import functools

import jax
import jax.numpy as jnp
from jax import lax
from jax.experimental import pallas as pl
from jax.experimental.pallas import tpu as pltpu
from jax.sharding import PartitionSpec as P

eps_norm = 1e-06
rope_base = 1000000.0
MESH = pl.DeviceIdType.MESH
f32 = jnp.float32
bf16 = jnp.bfloat16
DP, CTX, MP = "dp", "ctx", "mp"
CORE, LOW, ACROSS, DIAG, HIGH, ACROSS_X = range(6)
PIECES = ((0, 0), (0, 1), (1, 0), (1, 1))


def flip(value, bit):
    return 1 - value if bit else value


def place():
    dp = lax.axis_index(DP)
    ctx = lax.axis_index(CTX)
    return {
        DP: dp,
        CTX: ctx,
        "y": lax.axis_index(MP),
        "x": dp // 2,
        "c": dp % 2,
        "zh": ctx // 2,
        "zl": ctx % 2,
    }


def run_start(at, dx, dzh, dc, ctx_count, block):
    start = ((flip(at["x"], dx) * 2 + flip(at["c"], dc)) * ctx_count + flip(at["zh"], dzh) * 2) * block
    return pl.multiple_of(start, 2 * block)


def finish(copies):
    for copy in copies:
        copy.wait()


def nn(left, right):
    return lax.dot_general(left, right, (((1,), (0,)), ((), ())), preferred_element_type=f32)


def nt(left, right):
    return lax.dot_general(left, right, (((1,), (1,)), ((), ())), preferred_element_type=f32)


def tn(left, right):
    return lax.dot_general(left, right, (((0,), (0,)), ((), ())), preferred_element_type=f32)


def root_scale(values):
    return lax.rsqrt(jnp.mean(values * values, axis=-1, keepdims=True) + eps_norm)


def turn(values, cosine, sine):
    return values * cosine + pltpu.roll(values, values.shape[-1] // 2, 1) * sine


def turn_back(values, cosine, sine):
    return values * cosine + pltpu.roll(values * sine, values.shape[-1] // 2, 1)


def pair_rows(ref, base, part, span):
    far = base + 2 * part
    return jnp.concatenate(
        [ref[pl.ds(base, part), :][:, span[0] : span[1]], ref[pl.ds(far, part), :][:, span[0] : span[1]]], axis=0
    )


def allowed_pairs(at, n, m, part, heads, extra):
    def fold(index, size, times):
        for k in range(times - 1, 0, -1):
            index = jnp.where(index >= k * size, index - k * size, index)
        return index

    row = lax.broadcasted_iota(jnp.int32, (heads * 2 * part, 4 * part), 0)
    col = lax.broadcasted_iota(jnp.int32, (heads * 2 * part, 4 * part), 1)
    near = at["zl"] * part
    far = (1 - at["zl"]) * part
    row = fold(row, 2 * part, heads)
    query = jnp.where(row < part, row + near, row - part + far) + at["zh"] * 2 * part
    inner = fold(col, 2 * part, 2)
    key = jnp.where(inner < part, inner + near, inner - part + far)
    key = key + jnp.where(col < 2 * part, at["zh"], 1 - at["zh"]) * (2 * part)
    query, key = query.astype(f32), key.astype(f32)
    spot = jnp.concatenate([extra[n * 4 + m, 1], extra[n * 4 + 2 + m, 1]] * heads, axis=0)[:, :1]
    return (key <= query) & (key >= query - spot)


def stack_heads(ref, base, part, head):
    heads = ref.shape[1] // head
    return jnp.concatenate([pair_rows(ref, base, part, (h * head, (h + 1) * head)) for h in range(heads)], axis=0)


def unstack(ref, base, part, head, values):
    heads = ref.shape[1] // head
    for h in range(heads):
        top = 2 * part * h
        ref[pl.ds(base, part), pl.ds(h * head, head)] = values[top : top + part].astype(ref.dtype)
        ref[pl.ds(base + 2 * part, part), pl.ds(h * head, head)] = values[top + part : top + 2 * part].astype(ref.dtype)


def partners(at):
    return (
        {DP: at[DP] + 1 - 2 * at["c"]},
        {CTX: at[CTX] + 1 - 2 * at["zl"]},
        {MP: 1 - at["y"]},
    )


class Lines:
    def __init__(self, send, recv):
        self.send, self.recv, self.used, self.open = send, recv, 0, []

    def start(self, source, target, device):
        copy = pltpu.make_async_remote_copy(
            src_ref=source,
            dst_ref=target,
            send_sem=self.send.at[self.used],
            recv_sem=self.recv.at[self.used],
            device_id=device,
            device_id_type=MESH,
        )
        copy.start()
        self.used += 1
        self.open.append(copy)
        return copy

    def close(self):
        self.settle(list(self.open))

    def settle(self, copies):
        for copy in copies:
            copy.wait_send()
        self.open = [copy for copy in self.open if all(copy is not done for done in copies)]


class Moves:
    def __init__(self, sems):
        self.sems, self.used, self.open = sems, 0, []

    def start(self, source, target):
        copy = pltpu.make_async_copy(source, target, self.sems.at[self.used])
        copy.start()
        self.used += 1
        return copy

    def save(self, source, target):
        self.open.append(self.start(source, target))

    def close(self):
        finish(self.open)


def arrive(copies):
    for copy in copies:
        copy.wait_recv()


def neighbours(at):
    core, low, across = partners(at)
    return {
        CORE: core,
        LOW: low,
        ACROSS: across,
        DIAG: {**core, **low},
        HIGH: {CTX: at[CTX] + 2 - 4 * at["zh"]},
        ACROSS_X: {DP: at[DP] + 2 - 4 * at["x"]},
    }


def meet_all(near, names):
    barrier = pltpu.get_barrier_semaphore()
    for name in names:
        pl.semaphore_signal(barrier, inc=1, device_id=near[name], device_id_type=MESH)
    pl.semaphore_wait(barrier, len(names))


class Env:
    def __init__(self, at, near, lines, moves, ctx_count, block):
        self.at, self.near, self.lines, self.moves = at, near, lines, moves
        self.ctx_count, self.block = ctx_count, block


class Weight:
    def __init__(self, env, shard, target, by_rows, low, size):
        self.env, self.shard, self.target, self.by_rows, self.low, self.size = env, shard, target, by_rows, low, size
        self.over_z, self.own_x, self.far_x = [None, None], [None, None], [None, None]

    def mine(self):
        at, ctx_count, block = self.env.at, self.env.ctx_count, self.env.block
        spot = pl.ds(pl.multiple_of((at[DP] * ctx_count + at[CTX]) * block, block), block)
        return self.target.at[spot, pl.ds(self.low, self.size)] if self.by_rows else self.target.at[:, spot]

    def run(self, dx, dzh, dc):
        spot = pl.ds(run_start(self.env.at, dx, dzh, dc, self.env.ctx_count, self.env.block), 2 * self.env.block)
        return self.target.at[spot, pl.ds(self.low, self.size)] if self.by_rows else self.target.at[:, spot]

    def cut(self, dc, dzl):
        at = self.env.at
        start = pl.multiple_of((flip(at["c"], dc) * 2 + flip(at["zl"], dzl)) * self.size, 128)
        return self.shard.at[:, pl.ds(start, self.size)] if self.by_rows else self.shard.at[pl.ds(start, self.size), :]

    def exchange(self):
        near, lines = self.env.near, self.env.lines
        self.local = self.env.moves.start(self.cut(0, 0), self.mine())
        self.got = [
            lines.start(self.cut(dc, dzl), self.mine(), near[name])
            for dc, dzl, name in ((0, 1, LOW), (1, 0, CORE), (1, 1, DIAG))
        ]

    def ready(self):
        self.local.wait()
        arrive(self.got)

    def send_z(self, dc):
        self.over_z[dc] = self.env.lines.start(self.run(0, 0, dc), self.run(0, 0, dc), self.env.near[HIGH])

    def send_x(self, dc):
        self.own_x[dc] = self.env.lines.start(self.run(0, 0, dc), self.run(0, 0, dc), self.env.near[ACROSS_X])

    def pass_x(self, dc):
        self.over_z[dc].wait_recv()
        self.far_x[dc] = self.env.lines.start(self.run(0, 1, dc), self.run(0, 1, dc), self.env.near[ACROSS_X])

    def complete(self):
        arrive(self.own_x + self.far_x)


class Gains(Weight):
    def mine(self):
        return self.target.at[self.env.at[DP] * self.env.ctx_count + self.env.at[CTX]]

    def run(self, dx, dzh, dc):
        at = self.env.at
        return self.target.at[
            pl.ds((flip(at["x"], dx) * 2 + flip(at["c"], dc)) * self.env.ctx_count + flip(at["zh"], dzh) * 2, 2)
        ]

    def cut(self, dc, dzl):
        return self.shard


def tables(extra, n):
    packed = extra[n, 0]
    turned = pltpu.roll(packed, packed.shape[1] // 2, 1)
    first = lax.broadcasted_iota(jnp.int32, packed.shape, 1) < packed.shape[1] // 2
    return jnp.where(first, packed, turned), jnp.where(first, -turned, packed)


def forward_kernel(
    ctx_count, block, head,
    x_hbm, c_hbm, extra_hbm, gain_hbm, wq, wk, wv, wo, wg, wu, wd,
    a_out, raw_out, q_out, kv_out, kvp_out, o_out, lse_out, h_out, b_out, z_out, gu_out, c_out, extra_out, gains_out,
    wqkv_out, wo_out, wgu_out, wd_out,
    x, extra, gain_all, wqkv, w_o, wgu, w_d, a, raw, q, kv, kvp, o, lse, from_core, kept, second_a, second_b, from_z, from_y, last_a, last_b,
    h, b_all, z, gu, c, gains, send, recv, local,
):
    at = place()
    near = neighbours(at)
    lines, moves = Lines(send, recv), Moves(local)
    env = Env(at, near, lines, moves, ctx_count, block)
    part, width = x.shape[1], x.shape[2]
    q_width = q.shape[1]
    hidden = z.shape[1]
    rows = 2 * part
    meet_all(near, (CORE, LOW, ACROSS, DIAG, HIGH, ACROSS_X))

    seq = [flip(at["y"], ds) for ds in (0, 1)]
    x_low = lines.start(x_hbm.at[seq[0]], x.at[2], near[LOW])
    e_low = lines.start(extra_hbm.at[0], extra.at[2], near[LOW])
    units = (
        Weight(env, wq, wqkv, True, 0, q_width),
        Weight(env, wk, wqkv, True, q_width, head),
        Weight(env, wv, wqkv, True, q_width + head, head),
    )
    scale = Gains(env, gain_hbm, gain_all, True, 0, 0)
    for unit in (scale, *units):
        unit.exchange()
    x_core = [lines.start(x_hbm.at[seq[ds]], x.at[4 + ds], near[CORE]) for ds in (0, 1)]
    e_core = lines.start(extra_hbm, extra.at[pl.ds(4, 2)], near[CORE])
    x_own = [moves.start(x_hbm.at[seq[ds]], x.at[ds]) for ds in (0, 1)]
    e_own = moves.start(extra_hbm, extra.at[pl.ds(0, 2)])
    for unit in (scale, *units):
        unit.ready()
    in_qkv = Weight(env, None, wqkv, True, 0, wqkv.shape[1])
    for dc in (0, 1):
        scale.send_z(dc)
        scale.send_x(dc)
        in_qkv.send_z(dc)
        in_qkv.send_x(dc)
    w_out = Weight(env, wo, w_o, False, 0, q_width)
    w_gate = Weight(env, wg, wgu, True, 0, hidden)
    w_up = Weight(env, wu, wgu, True, hidden, hidden)
    w_down = Weight(env, wd, w_d, False, 0, hidden)
    w_out.exchange()
    w_gate.exchange()
    x_far, x_across = share(near, lines, x, x_low)
    e_far, e_across = share(near, lines, extra, e_low)
    w_up.exchange()
    w_down.exchange()
    x_far.append(pass_on(near, lines, x, x_across))
    e_far.append(pass_on(near, lines, extra, e_across))
    for dc in (0, 1):
        scale.pass_x(dc)
        in_qkv.pass_x(dc)
    w_out.ready()
    for dc in (0, 1):
        w_out.send_z(dc)
        w_out.send_x(dc)
    w_gate.ready()
    w_gate.send_z(0)
    scale.complete()
    gains[...] = jnp.zeros_like(gains)
    ranks = gain_all.shape[0]
    small = gain_all[0, 2:4, :]
    for n in range(ranks):
        gains[0:2, n * block : (n + 1) * block] = gain_all[n, 0:2, :]
        if n:
            small = small + gain_all[n, 2:4, :]
    gains[2:4, 0:head] = small

    finish(x_own)
    arrive(x_core + x_far)
    e_own.wait()
    arrive([e_core, *e_far])
    h[...] = x[0].astype(f32)

    @pl.loop(0, 8)
    def _(n):
        wide = x[n].astype(f32)
        span = pl.ds(pl.multiple_of(n * part, part), part)
        a[span, :] = (wide * root_scale(wide) * gains[0:1, :]).astype(bf16)

    in_qkv.complete()
    moves.save(wqkv, wqkv_out)
    gain_q = gains[2:3, 0:head]
    gain_k = gains[3:4, 0:head]

    @pl.loop(0, 4)
    def _(m):
        big = pl.ds(pl.multiple_of(m * rows, rows), rows)
        product = nn(a[big, :], wqkv[...])
        raw[big, :] = product[:, : q_width + head]
        for half in (0, 1):
            n = 2 * m + half
            span = pl.ds(pl.multiple_of(n * part, part), part)
            cos, sin = tables(extra, n)
            piece = product[half * part : (half + 1) * part]
            for j in range(q_width // head):
                u = piece[:, j * head : (j + 1) * head]
                q[span, pl.ds(j * head, head)] = turn(u * root_scale(u) * gain_q, cos, sin).astype(bf16)
            u = piece[:, q_width : q_width + head]
            kv[span, pl.ds(0, head)] = turn(u * root_scale(u) * gain_k, cos, sin).astype(bf16)
            kv[span, pl.ds(head, head)] = piece[:, q_width + head :].astype(bf16)

    kv_far = lines.start(kv, kvp, near[HIGH])
    for source, target in ((a, a_out), (raw, raw_out), (q, q_out), (kv, kv_out), (extra, extra_out), (gains, gains_out)):
        moves.save(source, target)
    for dc in (0, 1):
        w_out.pass_x(dc)
    for dc in (0, 1):
        w_gate.send_x(dc)
    kv_far.wait_recv()
    w_gate.send_z(1)
    c_own = [moves.start(c_hbm.at[seq[ds]], c.at[ds]) for ds in (0, 1)]
    c_core = [lines.start(c_hbm.at[seq[ds]], c.at[4 + ds], near[CORE]) for ds in (0, 1)]
    c_low = lines.start(c_hbm.at[seq[0]], c.at[2], near[LOW])
    w_up.ready()
    for dc in (0, 1):
        w_up.send_z(dc)
        w_up.send_x(dc)
    moves.save(kvp, kvp_out)
    scaling = head ** (-0.5)

    @pl.loop(0, 2)
    def _(n):
        @pl.loop(0, 2)
        def _(m):
            base = pl.multiple_of(n * (4 * part) + m * part, part)
            keys = jnp.concatenate([pair_rows(kv, base, part, (0, head)), pair_rows(kvp, base, part, (0, head))], axis=0)
            values = jnp.concatenate(
                [pair_rows(kv, base, part, (head, 2 * head)), pair_rows(kvp, base, part, (head, 2 * head))], axis=0
            )
            allowed = allowed_pairs(at, n, m, part, q_width // head, extra)
            scores = jnp.where(allowed, nt(stack_heads(q, base, part, head), keys) * scaling, -jnp.inf)
            peak = jnp.max(scores, axis=-1, keepdims=True)
            weights = jnp.exp(scores - peak)
            total = jnp.sum(weights, axis=-1, keepdims=True)
            mixed = nn(weights.astype(bf16), values) / total
            unstack(o, base, part, head, mixed)
            unstack(lse, base, part, head, jnp.broadcast_to(peak + jnp.log(total), mixed.shape))

    moves.save(o, o_out)
    moves.save(lse, lse_out)
    w_out.complete()
    moves.save(w_o, wo_out)
    out = x
    lines.settle([*x_far, x_across])

    def project(first):
        @pl.loop(0, 4)
        def _(m):
            n = first + m
            span = pl.ds(pl.multiple_of(n * part, part), part)
            out[n] = nn(o[span, :], w_o[...]).astype(bf16)

    project(4)
    sent = {k: lines.start(out.at[4 + k], from_core.at[k], near[CORE]) for k in (3, 1, 2, 0)}
    project(0)

    def pump_gate():
        for dc in (0, 1):
            w_gate.pass_x(dc)
        w_down.ready()
        for dc in (0, 1):
            w_down.send_z(dc)
            w_down.send_x(dc)
        return share(near, lines, c, c_low)

    sums, (c_far, c_across) = sum_lines(near, lines, out, sent, from_core, kept, second_a, second_b, from_z, from_y, last_a, last_b, pump_gate)
    h[...] = h[...] + sums
    moves.save(h, h_out)
    wide = h[...]
    b_all[0] = (wide * root_scale(wide) * gains[1:2, :]).astype(bf16)

    def pump_up():
        for dc in (0, 1):
            w_up.pass_x(dc)
        c_far.append(pass_on(near, lines, c, c_across))

    spread_lines(near, lines, b_all, from_z.shape[2], pump_up)
    moves.save(b_all, b_out)

    w_gate.complete()

    w_up.complete()
    moves.save(wgu, wgu_out)

    @pl.loop(0, 4)
    def _(m):
        span = pl.ds(pl.multiple_of(m * rows, rows), rows)
        b = pair(b_all, m)
        g = nn(b, wgu[:, 0:hidden])
        u = nn(b, wgu[:, hidden : 2 * hidden])
        gu[span, pl.ds(0, hidden)] = g.astype(bf16)
        gu[span, pl.ds(hidden, hidden)] = u.astype(bf16)
        z[span, :] = (g * jax.nn.sigmoid(g) * u).astype(bf16)

    moves.save(z, z_out)
    moves.save(gu, gu_out)
    finish(c_own)
    arrive(c_core + c_far)
    moves.save(c, c_out)
    for dc in (0, 1):
        w_down.pass_x(dc)
    w_down.complete()
    moves.save(w_d, wd_out)
    lines.close()
    moves.close()


def share(near, lines, ref, low):
    low.wait_recv()
    across = lines.start(ref.at[2], ref.at[3], near[ACROSS])
    return [lines.start(ref.at[2], ref.at[6], near[CORE])], across


def pass_on(near, lines, ref, across):
    across.wait_recv()
    return lines.start(ref.at[3], ref.at[7], near[CORE])


def pair(ref, m):
    return jnp.concatenate([ref[2 * m], ref[2 * m + 1]], axis=0)


def sum_lines(near, lines, part, first, from_core, kept, second_a, second_b, from_z, from_y, last_a, last_b, pump):
    width, cut = part.shape[2], from_z.shape[2]
    a, b = pl.ds(0, cut), pl.ds(cut, width - cut)

    def total(k):
        first[k].wait_recv()
        return part[k].astype(f32) + from_core[k].astype(f32)

    kept[2] = total(3).astype(bf16)
    y1 = lines.start(kept.at[2, :, b], from_y.at[1], near[ACROSS])
    z1 = lines.start(kept.at[2, :, a], from_z.at[1], near[LOW])
    kept[0] = total(1).astype(bf16)
    y0 = lines.start(kept.at[0, :, b], from_y.at[0], near[ACROSS])
    kept[1] = total(2).astype(bf16)
    z0 = lines.start(kept.at[1, :, a], from_z.at[0], near[LOW])
    y1.wait_recv()
    second_b[...] = (kept[1, :, b].astype(f32) + from_y[1].astype(f32)).astype(bf16)
    z2 = lines.start(second_b, last_b, near[LOW])
    z1.wait_recv()
    second_a[...] = (kept[0, :, a].astype(f32) + from_z[1].astype(f32)).astype(bf16)
    y2 = lines.start(second_a, last_a, near[ACROSS])
    extra = pump()
    mine = total(0)
    arrive((z0, y0, y2, z2))
    lines.settle([*first.values(), z1, y1, y0, z0, y2, z2])
    left = mine[:, :cut] + from_z[0].astype(f32) + last_a[...].astype(f32)
    right = mine[:, cut:] + from_y[0].astype(f32) + last_b[...].astype(f32)
    return jnp.concatenate([left, right], axis=1), extra


def spread_lines(near, lines, out, cut, pump):
    width = out.shape[2]
    a, b = pl.ds(0, cut), pl.ds(cut, width - cut)
    zb = lines.start(out.at[0, :, b], out.at[2, :, b], near[LOW])
    ya = lines.start(out.at[0, :, a], out.at[1, :, a], near[ACROSS])
    yb = lines.start(out.at[0, :, b], out.at[1, :, b], near[ACROSS])
    za = lines.start(out.at[0, :, a], out.at[2, :, a], near[LOW])
    c0 = lines.start(out.at[0], out.at[4], near[CORE])
    ya.wait_recv()
    zc = lines.start(out.at[1, :, a], out.at[3, :, a], near[LOW])
    zb.wait_recv()
    yc = lines.start(out.at[2, :, b], out.at[3, :, b], near[ACROSS])
    yb.wait_recv()
    c1 = lines.start(out.at[1], out.at[5], near[CORE])
    za.wait_recv()
    c2 = lines.start(out.at[2], out.at[6], near[CORE])
    zc.wait_recv()
    yc.wait_recv()
    c3 = lines.start(out.at[3], out.at[7], near[CORE])
    pump()
    arrive((c0, c1, c2, c3))
    return [ya, zb, yb, za, c0, zc, yc, c1, c2, c3]


class Grad:
    def __init__(self, env, work, by_rows, over_x, over_z, outs):
        self.env, self.work, self.by_rows, self.outs = env, work, by_rows, outs
        self.from_x, self.from_z = over_x, over_z
        self.x, self.z, self.last, self.local = {}, {}, [], []

    def index(self, dx, dzh, dc):
        spot = pl.ds(run_start(self.env.at, dx, dzh, dc, self.env.ctx_count, self.env.block), 2 * self.env.block)
        return (spot, slice(None)) if self.by_rows else (slice(None), spot)

    def send_x(self, dzh, dc):
        self.x[dzh, dc] = self.env.lines.start(
            self.work.at[self.index(1, dzh, dc)], self.from_x.at[2 * dzh + dc], self.env.near[ACROSS_X]
        )

    def pass_z(self, dc):
        self.x[1, dc].wait_recv()
        spot = self.index(0, 1, dc)
        self.work[spot] = (self.work[spot].astype(f32) + self.from_x[2 + dc].astype(f32)).astype(bf16)
        self.z[dc] = self.env.lines.start(self.work.at[spot], self.from_z.at[dc], self.env.near[HIGH])

    def deliver(self, dc):
        at, block = self.env.at, self.env.block
        self.x[0, dc].wait_recv()
        self.z[dc].wait_recv()
        spot = self.index(0, 0, dc)
        self.work[spot] = (
            self.work[spot].astype(f32) + self.from_x[dc].astype(f32) + self.from_z[dc].astype(f32)
        ).astype(bf16)
        slot = at["c"] * 2 + at["zl"]
        for dzl, name in ((1, (LOW, DIAG)[dc]), (0, (None, CORE)[dc])):
            start = run_start(at, 0, 0, dc, self.env.ctx_count, block) + flip(at["zl"], dzl) * block
            mine = pl.ds(pl.multiple_of(start, block), block)
            for out, low, size in self.outs:
                there = pl.ds(pl.multiple_of(slot * size, 128), size)
                if self.by_rows:
                    source, target = self.work.at[mine, pl.ds(low, size)], out.at[:, there]
                else:
                    source, target = self.work.at[:, mine], out.at[there, :]
                if name is None:
                    self.local.append(self.env.moves.start(source, target))
                else:
                    self.last.append(self.env.lines.start(source, target, self.env.near[name]))

    def finish(self):
        arrive(self.last)
        finish(self.local)


def eighths_of(unit, dx, make):
    @pl.loop(0, 2)
    def _(dzh):
        @pl.loop(0, 2)
        def _(dc):
            at, count = unit.env.at, unit.env.ctx_count
            near_zh = at["zh"] + dzh - 2 * at["zh"] * dzh
            near_c = at["c"] + dc - 2 * at["c"] * dc
            start = ((flip(at["x"], dx) * 2 + near_c) * count + near_zh * 2) * unit.env.block
            spot = pl.ds(pl.multiple_of(start, 2 * unit.env.block), 2 * unit.env.block)
            value = make(spot).astype(bf16)
            if unit.by_rows:
                unit.work[spot, :] = value
            else:
                unit.work[:, spot] = value


def columns(ref, run):
    block = ref[:, :, run]
    return block.reshape(block.shape[0] * block.shape[1], block.shape[2])


def backward_kernel(
    ctx_count, block, head,
    x_hbm, a_hbm, raw_hbm, q_hbm, kv_hbm, kvp_hbm, o_hbm, lse_hbm, h_hbm, b_hbm, z_hbm, gu_hbm, c_hbm, extra_hbm, gains_hbm,
    wqkv_hbm, wo_hbm, wgu_hbm, wd_hbm,
    out_hbm, in_hbm, g_query, g_key, g_value, g_out, g_gate, g_up, g_down, small_out,
    c, wd, z, gu, wgu, b, q, kv, kvp, o, lse, raw, extra, gains, wqkv, wo, h, dh, x_mine, dq, dkv, dkvp, got, do, dqkv,
    work_d, work_o, work_q, rx_d, rz_d, rx_g, rz_g, rx_o, rz_o, rx_q, rz_q,
    from_core, kept, second_a, second_b, from_z, from_y, last_a, last_b, own_out, own_in, sums, small, rx_s, rz_s, ry_s,
    send, recv, local, ready, done,
):
    at = place()
    near = neighbours(at)
    lines, moves = Lines(send, recv), Moves(local)
    env = Env(at, near, lines, moves, ctx_count, block)
    part, width = c.shape[1], c.shape[2]
    q_width = q.shape[1]
    hidden = z.shape[1]
    rows = 2 * part
    scaling = head ** (-0.5)
    fetch = moves.start
    get_z, get_c, get_d, get_gu = fetch(z_hbm, z), fetch(c_hbm, c), fetch(wd_hbm, wd), fetch(gu_hbm, gu)
    get_w, get_b = fetch(wgu_hbm, wgu), fetch(b_hbm, b)
    get_more = [fetch(*p) for p in ((h_hbm, h), (gains_hbm, gains), (wo_hbm, wo), (o_hbm, o))]
    get_rest = [
        fetch(*p)
        for p in ((q_hbm, q), (kv_hbm, kv), (kvp_hbm, kvp), (lse_hbm, lse), (raw_hbm, raw), (extra_hbm, extra), (wqkv_hbm, wqkv))
    ]
    get_x = fetch(x_hbm.at[at["y"]], x_mine)
    meet_all(near, (CORE, LOW, ACROSS, DIAG, HIGH, ACROSS_X))
    down = Grad(env, work_d, False, rx_d, rz_d, ((g_down, 0, hidden),))
    gate = Grad(env, wgu, True, rx_g, rz_g, ((g_gate, 0, hidden), (g_up, hidden, hidden)))
    outward = Grad(env, work_o, False, rx_o, rz_o, ((g_out, 0, q_width),))
    inward = Grad(env, work_q, True, rx_q, rz_q, ((g_query, 0, q_width), (g_key, q_width, head), (g_value, q_width + head, head)))

    get_z.wait()
    get_c.wait()
    eighths_of(down, 1, lambda run: tn(z[...], columns(c, run)))
    for dc in (0, 1):
        down.send_x(1, dc)
    eighths_of(down, 0, lambda run: tn(z[...], columns(c, run)))
    get_d.wait()
    get_gu.wait()
    dh[...] = c[0].astype(f32)

    @pl.loop(0, 4)
    def _(m):
        span = pl.ds(pl.multiple_of(m * rows, rows), rows)
        dz = nt(pair(c, m), wd[...])
        g = gu[span, pl.ds(0, hidden)].astype(f32)
        u = gu[span, pl.ds(hidden, hidden)].astype(f32)
        s = jax.nn.sigmoid(g)
        gu[span, pl.ds(0, hidden)] = (dz * u * s * (1.0 + g * (1.0 - s))).astype(bf16)
        gu[span, pl.ds(hidden, hidden)] = (dz * g * s).astype(bf16)

    get_w.wait()

    def spill(first, source, weight, back):
        @pl.loop(0, 2)
        def _(m):
            n = first // 2 + m
            span = pl.ds(pl.multiple_of(n * rows, rows), rows)
            product = (nt if back else nn)(source[span, :], weight[...]).astype(bf16)
            c[2 * n] = product[:part]
            c[2 * n + 1] = product[part:]

    def to_core():
        return {k: lines.start(c.at[4 + k], from_core.at[k], near[CORE]) for k in (3, 1, 2, 0)}

    spill(4, gu, wgu, True)
    sent = to_core()
    spill(0, gu, wgu, True)
    for dc in (0, 1):
        down.pass_z(dc)
    get_b.wait()
    eighths_of(gate, 1, lambda run: tn(columns(b, run), gu[...]))
    for dc in (0, 1):
        gate.send_x(1, dc)
    eighths_of(gate, 0, lambda run: tn(columns(b, run), gu[...]))
    for device in (CORE, LOW, ACROSS):
        pl.semaphore_signal(ready, inc=1, device_id=near[device], device_id_type=MESH)
    finish(get_more)

    def pump_down():
        for dc in (0, 1):
            down.send_x(0, dc)
        for dc in (0, 1):
            gate.send_x(0, dc)

    db, _ = sum_lines(near, lines, c, sent, from_core, kept, second_a, second_b, from_z, from_y, last_a, last_b, pump_down)
    wide = h[...]
    r = root_scale(wide)
    n_m = wide * r
    sums[1:2, :] = jnp.sum(db * n_m, axis=0, keepdims=True)
    t = db * gains[1:2, :]
    middle = dh[...] + r * (t - n_m * jnp.mean(t * n_m, axis=-1, keepdims=True))
    dh[...] = middle
    pl.semaphore_wait(ready, 3)
    b[0] = middle.astype(bf16)
    spread = spread_lines(near, lines, b, from_z.shape[2], lambda: None)
    gate.pass_z(0)

    @pl.loop(0, 4)
    def _(m):
        span = pl.ds(pl.multiple_of(m * rows, rows), rows)
        do[span, :] = nt(pair(b, m), wo[...]).astype(bf16)

    eighths_of(outward, 1, lambda run: tn(o[...], columns(b, run)))
    for dzh, dc in ((1, 0), (1, 1), (0, 0), (0, 1)):
        outward.send_x(dzh, dc)
    eighths_of(outward, 0, lambda run: tn(o[...], columns(b, run)))
    lines.settle(spread)
    get_a = fetch(a_hbm, b)
    finish(get_rest)

    @pl.loop(0, 2)
    def _(n):
        @pl.loop(0, 2)
        def _(m):
            base = pl.multiple_of(n * (4 * part) + m * part, part)
            query = stack_heads(q, base, part, head)
            mixed = stack_heads(o, base, part, head)
            grad = stack_heads(do, base, part, head)
            level = stack_heads(lse, base, part, head)[:, :1]
            keys = jnp.concatenate([pair_rows(kv, base, part, (0, head)), pair_rows(kvp, base, part, (0, head))], axis=0)
            values = jnp.concatenate(
                [pair_rows(kv, base, part, (head, 2 * head)), pair_rows(kvp, base, part, (head, 2 * head))], axis=0
            )
            allowed = allowed_pairs(at, n, m, part, q_width // head, extra)
            probs = jnp.where(allowed, jnp.exp(jnp.where(allowed, nt(query, keys) * scaling - level, 0.0)), 0.0)
            dv = tn(probs.astype(bf16), grad)
            row_dot = jnp.sum(grad.astype(f32) * mixed.astype(f32), axis=-1, keepdims=True)
            ds = (probs * (nt(grad, values) - row_dot)).astype(bf16)
            unstack(dq, base, part, head, nn(ds, keys) * scaling)
            dk = tn(ds, query) * scaling
            for ref, top in ((dkv, 0), (dkvp, 2 * part)):
                for i in (0, 1):
                    spot = pl.ds(base + i * 2 * part, part)
                    low = top + i * part
                    ref[spot, pl.ds(0, head)] = dk[low : low + part].astype(ref.dtype)
                    ref[spot, pl.ds(head, head)] = dv[low : low + part].astype(ref.dtype)

    kv_far = lines.start(dkvp, got, near[HIGH])

    spill(4, z, wd, False)
    sent = to_core()
    spill(0, z, wd, False)
    total, _ = sum_lines(near, lines, c, sent, from_core, kept, second_a, second_b, from_z, from_y, last_a, last_b, lambda: gate.pass_z(1))
    for device in (CORE, LOW, ACROSS):
        pl.semaphore_signal(done, inc=1, device_id=near[device], device_id_type=MESH)
    own_out[...] = (h[...] + total).astype(bf16)
    out_far = lines.start(own_out, out_hbm.at[at["y"]], near[ACROSS])
    moves.save(own_out, out_hbm.at[at["y"]])
    for dc in (0, 1):
        outward.pass_z(dc)

    kv_far.wait_recv()
    gain_q = gains[2:3, 0:head]
    gain_k = gains[3:4, 0:head]
    small_q = jnp.zeros((1, head), f32)

    def through(u, w, gain, cos, sin):
        scale = root_scale(u)
        n = u * scale
        e = turn_back(w, cos, sin)
        f = e * gain
        grad = (scale * (f - n * jnp.mean(f * n, axis=-1, keepdims=True))).astype(bf16)
        return grad, jnp.sum(e * n, axis=0, keepdims=True)

    sums[2:4, 0:head] = jnp.zeros((2, head), f32)

    @pl.loop(0, 8)
    def _(n):
        span = pl.ds(pl.multiple_of(n * part, part), part)
        cos, sin = tables(extra, n)
        for j in range(q_width // head):
            cols = pl.ds(j * head, head)
            dqkv[span, cols], add = through(raw[span, cols], dq[span, cols], gain_q, cos, sin)
            sums[2:3, 0:head] += add
        dk = dkv[span, pl.ds(0, head)] + got[span, pl.ds(0, head)].astype(f32)
        dv = dkv[span, pl.ds(head, head)] + got[span, pl.ds(head, head)].astype(f32)
        cols = pl.ds(q_width, head)
        dqkv[span, cols], add = through(raw[span, cols], dk, gain_k, cos, sin)
        sums[3:4, 0:head] += add
        dqkv[span, pl.ds(q_width + head, head)] = dv.astype(bf16)

    spill(4, dqkv, wqkv, True)
    pl.semaphore_wait(done, 3)
    sent = to_core()
    get_a.wait()
    eighths_of(inward, 1, lambda run: tn(columns(b, run), dqkv[...]))
    for dzh, dc in ((1, 0), (1, 1), (0, 0), (0, 1)):
        inward.send_x(dzh, dc)
    spill(0, dqkv, wqkv, True)
    eighths_of(inward, 0, lambda run: tn(columns(b, run), dqkv[...]))
    get_x.wait()

    def pump_in():
        for dc in (0, 1):
            inward.pass_z(dc)
        for dc in (0, 1):
            down.deliver(dc)

    da, _ = sum_lines(near, lines, c, sent, from_core, kept, second_a, second_b, from_z, from_y, last_a, last_b, pump_in)
    wide = x_mine[...].astype(f32)
    r = root_scale(wide)
    n_a = wide * r
    sums[0:1, :] = jnp.sum(da * n_a, axis=0, keepdims=True)
    f = da * gains[0:1, :]
    own_in[...] = (dh[...] + r * (f - n_a * jnp.mean(f * n_a, axis=-1, keepdims=True))).astype(bf16)
    in_far = lines.start(own_in, in_hbm.at[at["y"]], near[ACROSS])
    moves.save(own_in, in_hbm.at[at["y"]])

    ranks = small.shape[0]
    for n in range(ranks):
        small[n, 0:2, :] = sums[0:2, n * block : (n + 1) * block]
        small[n, 2:4, :] = sums[2:4, 0:head]
        small[n, 4:8, :] = jnp.zeros((4, block), f32)

    def few(dx, dzh, dc):
        return pl.ds((flip(at["x"], dx) * 2 + flip(at["c"], dc)) * ctx_count + flip(at["zh"], dzh) * 2, 2)

    over_x = {k: lines.start(small.at[few(1, *k)], rx_s.at[2 * k[0] + k[1]], near[ACROSS_X]) for k in ((1, 0), (1, 1), (0, 0), (0, 1))}
    over_z = []
    for dc in (0, 1):
        over_x[1, dc].wait_recv()
        small[few(0, 1, dc)] += rx_s[2 + dc]
        over_z.append(lines.start(small.at[few(0, 1, dc)], rz_s.at[dc], near[HIGH]))
    for dc in (0, 1):
        gate.deliver(dc)
    for dc in (0, 1):
        over_x[0, dc].wait_recv()
        over_z[dc].wait_recv()
        small[few(0, 0, dc)] += rx_s[dc] + rz_s[dc]
    base = few(0, 0, 0).start
    side = few(0, 0, 1).start
    spread = [
        lines.start(small.at[base + 1 - at["zl"]], ry_s.at[0], near[LOW]),
        lines.start(small.at[side + at["zl"]], ry_s.at[1], near[CORE]),
        lines.start(small.at[side + 1 - at["zl"]], ry_s.at[2], near[DIAG]),
    ]
    for dc in (0, 1):
        outward.deliver(dc)
    arrive(spread)
    ry_s[3] = small[base + at["zl"]] + ry_s[0] + ry_s[1] + ry_s[2]
    across = lines.start(ry_s.at[3], ry_s.at[4], near[ACROSS])
    for dc in (0, 1):
        inward.deliver(dc)
    across.wait_recv()
    small_out[...] = ry_s[3] + ry_s[4]
    for unit in (down, gate, outward, inward):
        unit.finish()
    arrive((out_far, in_far))
    lines.close()
    moves.close()


VM = pl.BlockSpec(memory_space=pltpu.VMEM)
HB = pl.BlockSpec(memory_space=pl.ANY)


def shaped(shape, dtype):
    return jax.ShapeDtypeStruct(shape, dtype)


def split_device(
    block_input, doc_positions, out_cotangent, attn_gain, mlp_gain, query_gain, key_gain,
    w_query, w_key, w_value, w_out, w_gate, w_up, w_down,
):
    dp_count = lax.axis_size(DP)
    ctx_count = lax.axis_size(CTX)
    rank_count = dp_count * ctx_count
    at = place()
    rank = at[DP] * ctx_count + at[CTX]
    upper = at["y"] == 1
    seqs, part, width = block_input.shape
    block = attn_gain.shape[0]
    head_piece = query_gain.shape[0]
    head = head_piece * rank_count
    own_p = jnp.where(upper, doc_positions[::-1], doc_positions).astype(f32)
    inverse = rope_base ** (-2.0 * jnp.arange(head // 2).astype(f32) / head)
    angles = own_p[:, :, None] * inverse
    extra = jnp.stack(
        [jnp.concatenate([jnp.cos(angles), jnp.sin(angles)], axis=2), jnp.broadcast_to(own_p[:, :, None], (seqs, part, head))],
        axis=1,
    )
    small = jnp.stack([query_gain, key_gain]).astype(f32)
    small = lax.dynamic_update_slice(jnp.zeros((2, head), f32), small, (0, rank * head_piece))
    own_gains = jnp.concatenate([jnp.stack([attn_gain, mlp_gain]).astype(f32), small, jnp.zeros((4, block), f32)])

    tokens = 4 * seqs * part
    q_width = w_query.shape[1] // 4
    hidden = w_gate.shape[1] // 4
    bound = functools.partial
    eighths = (8, part, width)
    cut = width // 4
    sum_room = [
        pltpu.VMEM((4, part, width), bf16), pltpu.VMEM((3, part, width), bf16),
        pltpu.VMEM((part, cut), bf16), pltpu.VMEM((part, width - cut), bf16),
        pltpu.VMEM((2, part, cut), bf16), pltpu.VMEM((2, part, width - cut), bf16),
        pltpu.VMEM((part, cut), bf16), pltpu.VMEM((part, width - cut), bf16),
    ]
    shapes = {
        "a": ((tokens, width), bf16), "raw": ((tokens, q_width + head), f32), "q": ((tokens, q_width), bf16),
        "kv": ((tokens, 2 * head), bf16), "kvp": ((tokens, 2 * head), bf16), "o": ((tokens, q_width), bf16),
        "lse": ((tokens, q_width), f32), "h": ((part, width), f32), "b": (eighths, bf16), "z": ((tokens, hidden), bf16),
        "gu": ((tokens, 2 * hidden), bf16), "c": (eighths, bf16), "extra": ((8, 2, part, head), f32), "gains": ((8, width), f32),
        "wqkv": ((width, q_width + 2 * head), bf16), "wo": ((q_width, width), bf16),
        "wgu": ((width, 2 * hidden), bf16), "wd": ((hidden, width), bf16),
    }
    room = {name: pltpu.VMEM(*spec) for name, spec in shapes.items()}
    kept = pl.pallas_call(
        bound(forward_kernel, ctx_count, block, head),
        out_shape=[shaped(*spec) for spec in shapes.values()],
        in_specs=[HB] * 11,
        out_specs=[HB] * len(shapes),
        scratch_shapes=[
            pltpu.VMEM(eighths, bf16), room["extra"], pltpu.VMEM((rank_count, 8, block), f32),
            room["wqkv"], room["wo"], room["wgu"], room["wd"], room["a"], room["raw"], room["q"], room["kv"], room["kvp"],
            room["o"], room["lse"], *sum_room,
            room["h"], room["b"], room["z"], room["gu"], room["c"], room["gains"],
            pltpu.SemaphoreType.DMA((160,)), pltpu.SemaphoreType.DMA((160,)), pltpu.SemaphoreType.DMA((64,)),
        ],
        compiler_params=pltpu.CompilerParams(collective_id=0, has_side_effects=True, vmem_limit_bytes=63 * 1024 * 1024),
    )(block_input, out_cotangent, extra, own_gains, w_query, w_key, w_value, w_out, w_gate, w_up, w_down)
    kept = dict(zip(shapes, kept))
    pair_shape = (seqs, part, width)
    names = (
        "a", "raw", "q", "kv", "kvp", "o", "lse", "h", "b", "z", "gu", "c", "extra", "gains", "wqkv", "wo", "wgu", "wd",
    )
    run = 2 * block
    vmem = pltpu.VMEM
    wide_q = q_width + 2 * head
    outs = pl.pallas_call(
        bound(backward_kernel, ctx_count, block, head),
        out_shape=[
            shaped(pair_shape, bf16), shaped(pair_shape, bf16),
            shaped(w_query.shape, bf16), shaped(w_key.shape, bf16), shaped(w_value.shape, bf16), shaped(w_out.shape, bf16),
            shaped(w_gate.shape, bf16), shaped(w_up.shape, bf16), shaped(w_down.shape, bf16), shaped((8, block), f32),
        ],
        in_specs=[HB] * (1 + len(names)),
        out_specs=[HB] * 9 + [VM],
        scratch_shapes=[
            *(room[k] for k in ("c", "wd", "z", "gu", "wgu", "b", "q", "kv", "kvp", "o", "lse", "raw", "extra", "gains", "wqkv", "wo", "h")),
            vmem((part, width), f32), vmem((part, width), bf16),
            vmem((tokens, q_width), f32), vmem((tokens, 2 * head), f32), vmem((tokens, 2 * head), bf16), vmem((tokens, 2 * head), bf16),
            vmem((tokens, q_width), bf16), vmem((tokens, wide_q), bf16),
            vmem((hidden, width), bf16), vmem((q_width, width), bf16), vmem((width, wide_q), bf16),
            vmem((4, hidden, run), bf16), vmem((2, hidden, run), bf16),
            vmem((4, run, 2 * hidden), bf16), vmem((2, run, 2 * hidden), bf16),
            vmem((4, q_width, run), bf16), vmem((2, q_width, run), bf16),
            vmem((4, run, wide_q), bf16), vmem((2, run, wide_q), bf16),
            *sum_room,
            vmem((part, width), bf16), vmem((part, width), bf16), vmem((8, width), f32),
            vmem((rank_count, 8, block), f32), vmem((4, 2, 8, block), f32), vmem((2, 2, 8, block), f32), vmem((5, 8, block), f32),
            pltpu.SemaphoreType.DMA((160,)), pltpu.SemaphoreType.DMA((160,)), pltpu.SemaphoreType.DMA((64,)),
            pltpu.SemaphoreType.REGULAR, pltpu.SemaphoreType.REGULAR,
        ],
        compiler_params=pltpu.CompilerParams(collective_id=1, has_side_effects=True, vmem_limit_bytes=67043328),
    )(block_input, kept["a"].reshape(eighths), *(kept[k] for k in names[1:]))
    small = outs[9]
    slots = small[2:4].reshape(2, rank_count, head_piece)
    slots = lax.dynamic_index_in_dim(slots, rank, 1, keepdims=False)
    return (
        outs[0], outs[1].astype(f32), small[0], small[1], slots[0], slots[1], *(grad.astype(f32) for grad in outs[2:9]),
    )


def rms_scale(value_rows):
    return lax.rsqrt(jnp.mean(value_rows * value_rows, axis=-1, keepdims=True) + eps_norm)


def rope_tables(places, head_size):
    half_size = head_size // 2
    inverse = rope_base ** (-2.0 * jnp.arange(half_size).astype(jnp.float32) / head_size)
    angles = places.astype(jnp.float32)[:, None] * inverse[None, :]
    angles = jnp.concatenate([angles, angles], axis=-1)
    return (jnp.cos(angles), jnp.sin(angles))


def rotate(values, cosine, sine):
    half_size = values.shape[-1] // 2
    turned = jnp.concatenate([-values[..., half_size:], values[..., :half_size]], axis=-1)
    return values * cosine[:, None, :] + turned * sine[:, None, :]


def rotate_back(grads, cosine, sine):
    half_size = grads.shape[-1] // 2
    weighted = grads * sine[:, None, :]
    return grads * cosine[:, None, :] + jnp.concatenate(
        [weighted[..., half_size:], -weighted[..., :half_size]], axis=-1
    )


def block_mask(query_index, lowest, key_index):
    return (key_index[None, :] <= query_index[:, None]) & (key_index[None, :] >= lowest[:, None])


def dot_nt(left, right):
    return lax.dot_general(
        left, right, (((1,), (1,)), ((), ())), preferred_element_type=jnp.float32
    )


def dot_tn(left, right):
    return lax.dot_general(
        left, right, (((0,), (0,)), ((), ())), preferred_element_type=jnp.float32
    )


def micro_pass(inputs_seq, places, cotangent, shards, totals):
    float_type = jnp.float32
    half_type = jnp.bfloat16
    fetched = (
        lax.all_gather(shards[0], (DP, CTX), axis=0, tiled=True),
        lax.all_gather(shards[1], (DP, CTX), axis=0, tiled=True),
        lax.all_gather(shards[2], (DP, CTX), axis=0, tiled=True),
        lax.all_gather(shards[3], (DP, CTX), axis=0, tiled=True),
        lax.all_gather(shards[4], (DP, CTX), axis=0, tiled=True),
        lax.all_gather(shards[5], (DP, CTX), axis=0, tiled=True),
        lax.all_gather(shards[6], (DP, CTX), axis=0, tiled=True),
        lax.all_gather(shards[7], (DP, CTX), axis=1, tiled=True),
        lax.all_gather(shards[8], (DP, CTX), axis=0, tiled=True),
        lax.all_gather(shards[9], (DP, CTX), axis=0, tiled=True),
        lax.all_gather(shards[10], (DP, CTX), axis=1, tiled=True),
    )
    gain_attn = fetched[0].astype(float_type)
    gain_mlp = fetched[1].astype(float_type)
    gain_query = fetched[2].astype(float_type)
    gain_key = fetched[3].astype(float_type)
    query_proj, key_proj, value_proj, out_proj, gate_proj, up_proj, down_proj = fetched[4:]
    head_size = gain_query.shape[0]
    head_count = query_proj.shape[1] // head_size
    kv_count = key_proj.shape[1] // head_size
    group_size = head_count // kv_count
    token_count = inputs_seq.shape[0]
    ctx_count = lax.axis_size(CTX)
    ctx_rank = lax.axis_index(CTX)
    scaling = head_size ** (-0.5)
    query_index = ctx_rank * token_count + jnp.arange(token_count, dtype=jnp.int32)
    lowest = query_index - places
    last_query = ctx_rank * token_count + token_count - 1
    residual_in = inputs_seq.astype(float_type)
    scale_attn = rms_scale(residual_in)
    normed_attn = residual_in * scale_attn
    attn_input = (normed_attn * gain_attn).astype(half_type)
    query_raw = jnp.dot(attn_input, query_proj, preferred_element_type=float_type).reshape(
        token_count, head_count, head_size
    )
    key_raw = jnp.dot(attn_input, key_proj, preferred_element_type=float_type).reshape(
        token_count, kv_count, head_size
    )
    value_rows = jnp.dot(attn_input, value_proj, preferred_element_type=float_type).astype(
        half_type
    )
    query_scale = rms_scale(query_raw)
    query_normed = query_raw * query_scale
    key_scale = rms_scale(key_raw)
    key_normed = key_raw * key_scale
    cosine, sine = rope_tables(places, head_size)
    query_rot = rotate(query_normed * gain_query, cosine, sine).astype(half_type)
    key_rot = (
        rotate(key_normed * gain_key, cosine, sine)
        .astype(half_type)
        .reshape(token_count, kv_count * head_size)
    )
    query_group = query_rot.reshape(token_count, kv_count, group_size, head_size)
    initial = (
        jnp.full((kv_count, group_size, token_count), -1e30, float_type),
        jnp.zeros((kv_count, group_size, token_count), float_type),
        jnp.zeros((token_count, kv_count, group_size, head_size), float_type),
    )
    pieces = (
        lax.all_gather(key_rot, CTX, axis=0, tiled=True),
        lax.all_gather(value_rows, CTX, axis=0, tiled=True),
    )
    row_count = pieces[0].shape[0]
    key_piece = pieces[0].reshape(row_count, kv_count, head_size)
    value_piece = pieces[1].reshape(row_count, kv_count, head_size)

    def fold_attend(state):
        peak, total, running = state
        scores = (
            jnp.einsum("qkgd,jkd->kgqj", query_group, key_piece, preferred_element_type=float_type)
            * scaling
        )
        allowed = block_mask(query_index, lowest, jnp.arange(row_count, dtype=jnp.int32))
        new_peak = jnp.maximum(peak, jnp.max(jnp.where(allowed, scores, -jnp.inf), axis=-1))
        weights = jnp.where(allowed, jnp.exp(scores - new_peak[..., None]), 0.0)
        total = jnp.sum(weights, axis=-1)
        running = jnp.einsum(
            "kgqj,jkd->qkgd",
            weights.astype(half_type),
            value_piece,
            preferred_element_type=float_type,
        )
        return (new_peak, total, running)

    peak, total, running = lax.cond(
        jnp.int32(0) <= last_query, fold_attend, lambda state: state, initial
    )
    attn_rows = (
        (running / jnp.transpose(total, (2, 0, 1))[..., None])
        .astype(half_type)
        .reshape(token_count, head_count * head_size)
    )
    log_total = peak + jnp.log(total)
    attn_out = lax.psum(
        jnp.dot(attn_rows, out_proj, preferred_element_type=float_type).astype(jnp.bfloat16), MP
    ).astype(jnp.float32)
    middle = residual_in + attn_out
    scale_mlp = rms_scale(middle)
    normed_mlp = middle * scale_mlp
    mlp_input = (normed_mlp * gain_mlp).astype(half_type)
    gate_rows = jnp.dot(mlp_input, gate_proj, preferred_element_type=float_type)
    up_rows = jnp.dot(mlp_input, up_proj, preferred_element_type=float_type)
    sigmoid_gate = jax.nn.sigmoid(gate_rows)
    hidden_rows = (gate_rows * sigmoid_gate * up_rows).astype(half_type)
    mlp_out = lax.psum(
        jnp.dot(hidden_rows, down_proj, preferred_element_type=float_type).astype(jnp.bfloat16),
        MP,
    ).astype(jnp.float32)
    block_output = (middle + mlp_out).astype(half_type)
    refetched = (
        lax.all_gather(shards[0], (DP, CTX), axis=0, tiled=True),
        lax.all_gather(shards[1], (DP, CTX), axis=0, tiled=True),
        lax.all_gather(shards[2], (DP, CTX), axis=0, tiled=True),
        lax.all_gather(shards[3], (DP, CTX), axis=0, tiled=True),
        lax.all_gather(shards[4], (DP, CTX), axis=0, tiled=True),
        lax.all_gather(shards[5], (DP, CTX), axis=0, tiled=True),
        lax.all_gather(shards[6], (DP, CTX), axis=0, tiled=True),
        lax.all_gather(shards[7], (DP, CTX), axis=1, tiled=True),
        lax.all_gather(shards[8], (DP, CTX), axis=0, tiled=True),
        lax.all_gather(shards[9], (DP, CTX), axis=0, tiled=True),
        lax.all_gather(shards[10], (DP, CTX), axis=1, tiled=True),
    )
    gain_attn = refetched[0].astype(float_type)
    gain_mlp = refetched[1].astype(float_type)
    gain_query = refetched[2].astype(float_type)
    gain_key = refetched[3].astype(float_type)
    query_proj, key_proj, value_proj, out_proj, gate_proj, up_proj, down_proj = refetched[4:]
    down_grad = dot_tn(hidden_rows, cotangent)
    hidden_grad = dot_nt(cotangent, down_proj)
    gate_grad = (
        hidden_grad * up_rows * sigmoid_gate * (1.0 + gate_rows * (1.0 - sigmoid_gate))
    ).astype(half_type)
    up_grad = (hidden_grad * gate_rows * sigmoid_gate).astype(half_type)
    gate_proj_grad = dot_tn(mlp_input, gate_grad)
    up_proj_grad = dot_tn(mlp_input, up_grad)
    mlp_in_grad = lax.psum(
        (dot_nt(gate_grad, gate_proj) + dot_nt(up_grad, up_proj)).astype(jnp.bfloat16), MP
    ).astype(jnp.float32)
    mlp_gain_grad = jnp.sum(mlp_in_grad * normed_mlp, axis=0)
    normed_grad = mlp_in_grad * gain_mlp
    middle_grad = cotangent.astype(float_type) + scale_mlp * (
        normed_grad - normed_mlp * jnp.mean(normed_grad * normed_mlp, axis=-1, keepdims=True)
    )
    middle_half = middle_grad.astype(half_type)
    out_proj_grad = dot_tn(attn_rows, middle_half)
    attn_grad = dot_nt(middle_half, out_proj).astype(half_type)
    grad_group = attn_grad.reshape(token_count, kv_count, group_size, head_size)
    attn_group = attn_rows.reshape(token_count, kv_count, group_size, head_size)
    row_dot = jnp.einsum(
        "qkgd,qkgd->kgq", grad_group, attn_group, preferred_element_type=float_type
    )
    key_back, value_back = (
        lax.all_gather(key_rot, CTX, axis=0, tiled=True),
        lax.all_gather(value_rows, CTX, axis=0, tiled=True),
    )

    def back_block(query_sum, block_id):
        start = block_id * token_count
        key_piece = lax.dynamic_slice_in_dim(key_back, start, token_count, 0).reshape(
            token_count, kv_count, head_size
        )
        value_piece = lax.dynamic_slice_in_dim(value_back, start, token_count, 0).reshape(
            token_count, kv_count, head_size
        )

        def back_attend(running):
            scores = (
                jnp.einsum(
                    "qkgd,jkd->kgqj", query_group, key_piece, preferred_element_type=float_type
                )
                * scaling
            )
            allowed = block_mask(
                query_index, lowest, start + jnp.arange(token_count, dtype=jnp.int32)
            )
            probs = jnp.where(allowed, jnp.exp(scores - log_total[..., None]), 0.0)
            value_part = jnp.einsum(
                "kgqj,qkgd->jkd",
                probs.astype(half_type),
                grad_group,
                preferred_element_type=float_type,
            )
            prob_grad = jnp.einsum(
                "qkgd,jkd->kgqj", grad_group, value_piece, preferred_element_type=float_type
            )
            score_half = (probs * (prob_grad - row_dot[..., None])).astype(half_type)
            query_part = (
                jnp.einsum(
                    "kgqj,jkd->qkgd", score_half, key_piece, preferred_element_type=float_type
                )
                * scaling
            )
            key_part = (
                jnp.einsum(
                    "kgqj,qkgd->jkd", score_half, query_group, preferred_element_type=float_type
                )
                * scaling
            )
            return (
                running + query_part,
                jnp.concatenate(
                    [
                        key_part.reshape(token_count, kv_count * head_size),
                        value_part.reshape(token_count, kv_count * head_size),
                    ],
                    axis=-1,
                ),
            )

        def passing(running):
            return (running, jnp.zeros((token_count, 2 * kv_count * head_size), float_type))

        return lax.cond(start <= last_query, back_attend, passing, query_sum)

    query_grad, kv_terms = lax.scan(
        back_block,
        jnp.zeros((token_count, kv_count, group_size, head_size), float_type),
        jnp.arange(ctx_count, dtype=jnp.int32),
    )
    kv_grad = lax.psum_scatter(
        kv_terms.reshape(ctx_count * token_count, 2 * kv_count * head_size).astype(jnp.bfloat16),
        CTX,
        scatter_dimension=0,
        tiled=True,
    ).astype(jnp.float32)
    key_rot_grad = kv_grad[:, : kv_count * head_size].reshape(token_count, kv_count, head_size)
    value_half = kv_grad[:, kv_count * head_size :].astype(half_type)
    query_back = rotate_back(query_grad.reshape(token_count, head_count, head_size), cosine, sine)
    key_grad_back = rotate_back(key_rot_grad, cosine, sine)
    query_gain_part = jnp.sum(query_back * query_normed, axis=(0, 1))
    key_gain_part = jnp.sum(key_grad_back * key_normed, axis=(0, 1))
    query_ngrad = query_back * gain_query
    key_ngrad = key_grad_back * gain_key
    query_half = (
        (
            query_scale
            * (
                query_ngrad
                - query_normed * jnp.mean(query_ngrad * query_normed, axis=-1, keepdims=True)
            )
        )
        .reshape(token_count, head_count * head_size)
        .astype(half_type)
    )
    key_half = (
        (
            key_scale
            * (key_ngrad - key_normed * jnp.mean(key_ngrad * key_normed, axis=-1, keepdims=True))
        )
        .reshape(token_count, kv_count * head_size)
        .astype(half_type)
    )
    query_proj_grad = dot_tn(attn_input, query_half)
    key_proj_grad = dot_tn(attn_input, key_half)
    value_proj_grad = dot_tn(attn_input, value_half)
    attn_in_grad, query_gain_sum, key_gain_sum = (
        lax.psum(
            (
                dot_nt(query_half, query_proj)
                + dot_nt(key_half, key_proj)
                + dot_nt(value_half, value_proj)
            ).astype(jnp.bfloat16),
            MP,
        ).astype(jnp.float32),
        lax.psum(query_gain_part.astype(jnp.bfloat16), MP).astype(jnp.float32),
        lax.psum(key_gain_part.astype(jnp.bfloat16), MP).astype(jnp.float32),
    )
    attn_gain_grad = jnp.sum(attn_in_grad * normed_attn, axis=0)
    normed_in_grad = attn_in_grad * gain_attn
    input_grad = middle_grad + scale_attn * (
        normed_in_grad
        - normed_attn * jnp.mean(normed_in_grad * normed_attn, axis=-1, keepdims=True)
    )
    addition = (
        attn_gain_grad,
        mlp_gain_grad,
        query_gain_sum,
        key_gain_sum,
        query_proj_grad,
        key_proj_grad,
        value_proj_grad,
        out_proj_grad,
        gate_proj_grad,
        up_proj_grad,
        down_grad,
    )
    totals = tuple((earlier + later for earlier, later in zip(totals, addition)))
    return (block_output, input_grad, totals)


def on_device(
    block_input,
    doc_positions,
    out_cotangent,
    attn_gain,
    mlp_gain,
    query_gain,
    key_gain,
    w_query,
    w_key,
    w_value,
    w_out,
    w_gate,
    w_up,
    w_down,
):
    shards = (
        attn_gain,
        mlp_gain,
        query_gain,
        key_gain,
        w_query,
        w_key,
        w_value,
        w_out,
        w_gate,
        w_up,
        w_down,
    )
    head_size = query_gain.shape[0] * lax.axis_size((DP, CTX))
    model_width = block_input.shape[2]
    query_width = w_query.shape[1]
    kv_width = w_key.shape[1]
    hidden_width = w_gate.shape[1]
    totals = (
        jnp.zeros((model_width,), jnp.float32),
        jnp.zeros((model_width,), jnp.float32),
        jnp.zeros((head_size,), jnp.float32),
        jnp.zeros((head_size,), jnp.float32),
        jnp.zeros((model_width, query_width), jnp.float32),
        jnp.zeros((model_width, kv_width), jnp.float32),
        jnp.zeros((model_width, kv_width), jnp.float32),
        jnp.zeros((query_width, model_width), jnp.float32),
        jnp.zeros((model_width, hidden_width), jnp.float32),
        jnp.zeros((model_width, hidden_width), jnp.float32),
        jnp.zeros((hidden_width, model_width), jnp.float32),
    )
    output_list = []
    grad_list = []
    for micro in range(block_input.shape[0]):
        output_rows, input_rows, totals = micro_pass(
            block_input[micro], doc_positions[micro], out_cotangent[micro], shards, totals
        )
        output_list.append(output_rows)
        grad_list.append(input_rows)
    owned = (
        lax.psum_scatter(totals[0], (DP, CTX), scatter_dimension=0, tiled=True),
        lax.psum_scatter(totals[1], (DP, CTX), scatter_dimension=0, tiled=True),
        lax.psum_scatter(totals[2], (DP, CTX), scatter_dimension=0, tiled=True),
        lax.psum_scatter(totals[3], (DP, CTX), scatter_dimension=0, tiled=True),
        lax.psum_scatter(totals[4], (DP, CTX), scatter_dimension=0, tiled=True),
        lax.psum_scatter(totals[5], (DP, CTX), scatter_dimension=0, tiled=True),
        lax.psum_scatter(totals[6], (DP, CTX), scatter_dimension=0, tiled=True),
        lax.psum_scatter(totals[7], (DP, CTX), scatter_dimension=1, tiled=True),
        lax.psum_scatter(totals[8], (DP, CTX), scatter_dimension=0, tiled=True),
        lax.psum_scatter(totals[9], (DP, CTX), scatter_dimension=0, tiled=True),
        lax.psum_scatter(totals[10], (DP, CTX), scatter_dimension=1, tiled=True),
    )
    return (
        jnp.stack(output_list),
        jnp.stack(grad_list),
        owned[0],
        owned[1],
        owned[2],
        owned[3],
        owned[4],
        owned[5],
        owned[6],
        owned[7],
        owned[8],
        owned[9],
        owned[10],
    )


def choose(mesh, arrays):
    dp, ctx, mp = mesh.shape[DP], mesh.shape[CTX], mesh.shape[MP]
    width = arrays[0].shape[2]
    paired = dp == 4 and ctx == 4 and mp == 2
    return split_device if paired and width % (dp * ctx * 128) == 0 else on_device


def solution(mesh):
    in_specs = (
        P(DP, CTX, None),
        P(DP, CTX),
        P(DP, CTX, None),
        P((DP, CTX)),
        P((DP, CTX)),
        P((DP, CTX)),
        P((DP, CTX)),
        P((DP, CTX), MP),
        P((DP, CTX), MP),
        P((DP, CTX), MP),
        P(MP, (DP, CTX)),
        P((DP, CTX), MP),
        P((DP, CTX), MP),
        P(MP, (DP, CTX)),
    )
    out_specs = (
        P(DP, CTX, None),
        P(DP, CTX, None),
        P((DP, CTX)),
        P((DP, CTX)),
        P((DP, CTX)),
        P((DP, CTX)),
        P((DP, CTX), MP),
        P((DP, CTX), MP),
        P((DP, CTX), MP),
        P(MP, (DP, CTX)),
        P((DP, CTX), MP),
        P((DP, CTX), MP),
        P(MP, (DP, CTX)),
    )

    def run(*arrays):
        return jax.shard_map(
            choose(mesh, arrays), mesh=mesh, in_specs=in_specs, out_specs=out_specs, check_vma=False
        )(*arrays)

    return run
```

```python
import functools

import jax
import jax.numpy as jnp
from jax import lax
from jax.experimental import pallas as pl
from jax.experimental.pallas import tpu as pltpu
from jax.sharding import PartitionSpec as P

eps_norm = 1e-06
rope_base = 1000000.0
MESH = pl.DeviceIdType.MESH
f32 = jnp.float32
bf16 = jnp.bfloat16
DP, CTX, MP = "dp", "ctx", "mp"
CORE, LOW, ACROSS, DIAG, HIGH, ACROSS_X = range(6)
PIECES = ((0, 0), (0, 1), (1, 0), (1, 1))


def flip(value, bit):
    return 1 - value if bit else value


def place():
    dp = lax.axis_index(DP)
    ctx = lax.axis_index(CTX)
    return {
        DP: dp,
        CTX: ctx,
        "y": lax.axis_index(MP),
        "x": dp // 2,
        "c": dp % 2,
        "zh": ctx // 2,
        "zl": ctx % 2,
    }


def run_start(at, dx, dzh, dc, ctx_count, block):
    start = ((flip(at["x"], dx) * 2 + flip(at["c"], dc)) * ctx_count + flip(at["zh"], dzh) * 2) * block
    return pl.multiple_of(start, 2 * block)


def finish(copies):
    for copy in copies:
        copy.wait()


def nn(left, right):
    return lax.dot_general(left, right, (((1,), (0,)), ((), ())), preferred_element_type=f32)


def nt(left, right):
    return lax.dot_general(left, right, (((1,), (1,)), ((), ())), preferred_element_type=f32)


def tn(left, right):
    return lax.dot_general(left, right, (((0,), (0,)), ((), ())), preferred_element_type=f32)


def root_scale(values):
    return lax.rsqrt(jnp.mean(values * values, axis=-1, keepdims=True) + eps_norm)


def turn(values, cosine, sine):
    return values * cosine + pltpu.roll(values, values.shape[-1] // 2, 1) * sine


def turn_back(values, cosine, sine):
    return values * cosine + pltpu.roll(values * sine, values.shape[-1] // 2, 1)


def pair_rows(ref, base, part, span):
    far = base + 2 * part
    return jnp.concatenate(
        [ref[pl.ds(base, part), :][:, span[0] : span[1]], ref[pl.ds(far, part), :][:, span[0] : span[1]]], axis=0
    )


def allowed_pairs(at, n, m, part, heads, extra):
    def fold(index, size, times):
        for k in range(times - 1, 0, -1):
            index = jnp.where(index >= k * size, index - k * size, index)
        return index

    row = lax.broadcasted_iota(jnp.int32, (heads * 2 * part, 4 * part), 0)
    col = lax.broadcasted_iota(jnp.int32, (heads * 2 * part, 4 * part), 1)
    near = at["zl"] * part
    far = (1 - at["zl"]) * part
    row = fold(row, 2 * part, heads)
    query = jnp.where(row < part, row + near, row - part + far) + at["zh"] * 2 * part
    inner = fold(col, 2 * part, 2)
    key = jnp.where(inner < part, inner + near, inner - part + far)
    key = key + jnp.where(col < 2 * part, at["zh"], 1 - at["zh"]) * (2 * part)
    query, key = query.astype(f32), key.astype(f32)
    spot = jnp.concatenate([extra[n * 4 + m, 1], extra[n * 4 + 2 + m, 1]] * heads, axis=0)[:, :1]
    return (key <= query) & (key >= query - spot)


def stack_heads(ref, base, part, head):
    heads = ref.shape[1] // head
    return jnp.concatenate([pair_rows(ref, base, part, (h * head, (h + 1) * head)) for h in range(heads)], axis=0)


def unstack(ref, base, part, head, values):
    heads = ref.shape[1] // head
    for h in range(heads):
        top = 2 * part * h
        ref[pl.ds(base, part), pl.ds(h * head, head)] = values[top : top + part].astype(ref.dtype)
        ref[pl.ds(base + 2 * part, part), pl.ds(h * head, head)] = values[top + part : top + 2 * part].astype(ref.dtype)


def partners(at):
    return (
        {DP: at[DP] + 1 - 2 * at["c"]},
        {CTX: at[CTX] + 1 - 2 * at["zl"]},
        {MP: 1 - at["y"]},
    )


class Lines:
    def __init__(self, send, recv):
        self.send, self.recv, self.used, self.open = send, recv, 0, []

    def start(self, source, target, device):
        copy = pltpu.make_async_remote_copy(
            src_ref=source,
            dst_ref=target,
            send_sem=self.send.at[self.used],
            recv_sem=self.recv.at[self.used],
            device_id=device,
            device_id_type=MESH,
        )
        copy.start()
        self.used += 1
        self.open.append(copy)
        return copy

    def close(self):
        self.settle(list(self.open))

    def settle(self, copies):
        for copy in copies:
            copy.wait_send()
        self.open = [copy for copy in self.open if all(copy is not done for done in copies)]


class Moves:
    def __init__(self, sems):
        self.sems, self.used, self.open = sems, 0, []

    def start(self, source, target):
        copy = pltpu.make_async_copy(source, target, self.sems.at[self.used])
        copy.start()
        self.used += 1
        return copy

    def save(self, source, target):
        self.open.append(self.start(source, target))

    def close(self):
        finish(self.open)


def arrive(copies):
    for copy in copies:
        copy.wait_recv()


def neighbours(at):
    core, low, across = partners(at)
    return {
        CORE: core,
        LOW: low,
        ACROSS: across,
        DIAG: {**core, **low},
        HIGH: {CTX: at[CTX] + 2 - 4 * at["zh"]},
        ACROSS_X: {DP: at[DP] + 2 - 4 * at["x"]},
    }


def meet_all(near, names):
    barrier = pltpu.get_barrier_semaphore()
    for name in names:
        pl.semaphore_signal(barrier, inc=1, device_id=near[name], device_id_type=MESH)
    pl.semaphore_wait(barrier, len(names))


class Env:
    def __init__(self, at, near, lines, moves, ctx_count, block):
        self.at, self.near, self.lines, self.moves = at, near, lines, moves
        self.ctx_count, self.block = ctx_count, block


class Weight:
    def __init__(self, env, shard, target, by_rows, low, size):
        self.env, self.shard, self.target, self.by_rows, self.low, self.size = env, shard, target, by_rows, low, size
        self.over_z, self.own_x, self.far_x = [None, None], [None, None], [None, None]

    def mine(self):
        at, ctx_count, block = self.env.at, self.env.ctx_count, self.env.block
        spot = pl.ds(pl.multiple_of((at[DP] * ctx_count + at[CTX]) * block, block), block)
        return self.target.at[spot, pl.ds(self.low, self.size)] if self.by_rows else self.target.at[:, spot]

    def run(self, dx, dzh, dc):
        spot = pl.ds(run_start(self.env.at, dx, dzh, dc, self.env.ctx_count, self.env.block), 2 * self.env.block)
        return self.target.at[spot, pl.ds(self.low, self.size)] if self.by_rows else self.target.at[:, spot]

    def cut(self, dc, dzl):
        at = self.env.at
        start = pl.multiple_of((flip(at["c"], dc) * 2 + flip(at["zl"], dzl)) * self.size, 128)
        return self.shard.at[:, pl.ds(start, self.size)] if self.by_rows else self.shard.at[pl.ds(start, self.size), :]

    def exchange(self):
        near, lines = self.env.near, self.env.lines
        self.local = self.env.moves.start(self.cut(0, 0), self.mine())
        self.got = [
            lines.start(self.cut(dc, dzl), self.mine(), near[name])
            for dc, dzl, name in ((0, 1, LOW), (1, 0, CORE), (1, 1, DIAG))
        ]

    def ready(self):
        self.local.wait()
        arrive(self.got)

    def send_z(self, dc):
        self.over_z[dc] = self.env.lines.start(self.run(0, 0, dc), self.run(0, 0, dc), self.env.near[HIGH])

    def send_x(self, dc):
        self.own_x[dc] = self.env.lines.start(self.run(0, 0, dc), self.run(0, 0, dc), self.env.near[ACROSS_X])

    def pass_x(self, dc):
        self.over_z[dc].wait_recv()
        self.far_x[dc] = self.env.lines.start(self.run(0, 1, dc), self.run(0, 1, dc), self.env.near[ACROSS_X])

    def complete(self):
        arrive(self.own_x + self.far_x)


class Gains(Weight):
    def mine(self):
        return self.target.at[self.env.at[DP] * self.env.ctx_count + self.env.at[CTX]]

    def run(self, dx, dzh, dc):
        at = self.env.at
        return self.target.at[
            pl.ds((flip(at["x"], dx) * 2 + flip(at["c"], dc)) * self.env.ctx_count + flip(at["zh"], dzh) * 2, 2)
        ]

    def cut(self, dc, dzl):
        return self.shard


def tables(extra, n):
    packed = extra[n, 0]
    turned = pltpu.roll(packed, packed.shape[1] // 2, 1)
    first = lax.broadcasted_iota(jnp.int32, packed.shape, 1) < packed.shape[1] // 2
    return jnp.where(first, packed, turned), jnp.where(first, -turned, packed)


def forward_kernel(
    ctx_count, block, head,
    x_hbm, c_hbm, extra_hbm, gain_hbm, wq, wk, wv, wo, wg, wu, wd,
    a_out, raw_out, q_out, kv_out, kvp_out, o_out, lse_out, h_out, b_out, z_out, gu_out, c_out, extra_out, gains_out,
    wqkv_out, wo_out, wgu_out, wd_out, work_d_out,
    x, extra, gain_all, wqkv, w_o, wgu, w_d, a, raw, q, kv, kvp, o, lse, from_core, kept, second_a, second_b, from_z, from_y, last_a, last_b,
    h, b_all, z, gu, c, gains, work_d, send, recv, local,
):
    at = place()
    near = neighbours(at)
    lines, moves = Lines(send, recv), Moves(local)
    env = Env(at, near, lines, moves, ctx_count, block)
    part, width = x.shape[1], x.shape[2]
    q_width = q.shape[1]
    hidden = z.shape[1]
    rows = 2 * part
    meet_all(near, (CORE, LOW, ACROSS, DIAG, HIGH, ACROSS_X))

    seq = [flip(at["y"], ds) for ds in (0, 1)]
    units = (
        Weight(env, wq, wqkv, True, 0, q_width),
        Weight(env, wk, wqkv, True, q_width, head),
        Weight(env, wv, wqkv, True, q_width + head, head),
    )
    scale = Gains(env, gain_hbm, gain_all, True, 0, 0)
    w_out = Weight(env, wo, w_o, False, 0, q_width)
    w_gate = Weight(env, wg, wgu, True, 0, hidden)
    w_up = Weight(env, wu, wgu, True, hidden, hidden)
    w_down = Weight(env, wd, w_d, False, 0, hidden)
    for unit in (scale, *units, w_out):
        unit.exchange()
    x_low = lines.start(x_hbm.at[seq[0]], x.at[2], near[LOW])
    e_low = lines.start(extra_hbm.at[0], extra.at[2], near[LOW])
    w_gate.exchange()
    x_core = [lines.start(x_hbm.at[seq[ds]], x.at[4 + ds], near[CORE]) for ds in (0, 1)]
    e_core = lines.start(extra_hbm, extra.at[pl.ds(4, 2)], near[CORE])
    x_own = [moves.start(x_hbm.at[seq[ds]], x.at[ds]) for ds in (0, 1)]
    e_own = moves.start(extra_hbm, extra.at[pl.ds(0, 2)])
    for unit in (scale, *units):
        unit.ready()
    in_qkv = Weight(env, None, wqkv, True, 0, wqkv.shape[1])
    for dc in (0, 1):
        scale.send_z(dc)
        scale.send_x(dc)
        in_qkv.send_z(dc)
        in_qkv.send_x(dc)
    w_out.ready()
    for dc in (0, 1):
        w_out.send_z(dc)
        w_out.send_x(dc)
    x_far, x_across = share(near, lines, x, x_low)
    e_far, e_across = share(near, lines, extra, e_low)
    w_up.exchange()
    w_down.exchange()
    x_far.append(pass_on(near, lines, x, x_across))
    e_far.append(pass_on(near, lines, extra, e_across))
    for dc in (0, 1):
        scale.pass_x(dc)
        in_qkv.pass_x(dc)
    w_gate.ready()
    w_gate.send_z(0)
    scale.complete()
    gains[...] = jnp.zeros_like(gains)
    ranks = gain_all.shape[0]
    small = gain_all[0, 2:4, :]
    for n in range(ranks):
        gains[0:2, n * block : (n + 1) * block] = gain_all[n, 0:2, :]
        if n:
            small = small + gain_all[n, 2:4, :]
    gains[2:4, 0:head] = small

    finish(x_own)
    arrive(x_core + x_far)
    e_own.wait()
    arrive([e_core, *e_far])
    h[...] = x[0].astype(f32)

    @pl.loop(0, 8)
    def _(n):
        wide = x[n].astype(f32)
        span = pl.ds(pl.multiple_of(n * part, part), part)
        a[span, :] = (wide * root_scale(wide) * gains[0:1, :]).astype(bf16)

    in_qkv.complete()
    moves.save(wqkv, wqkv_out)
    gain_q = gains[2:3, 0:head]
    gain_k = gains[3:4, 0:head]

    @pl.loop(0, 4)
    def _(m):
        big = pl.ds(pl.multiple_of(m * rows, rows), rows)
        product = nn(a[big, :], wqkv[...])
        raw[big, :] = product[:, : q_width + head]
        for half in (0, 1):
            n = 2 * m + half
            span = pl.ds(pl.multiple_of(n * part, part), part)
            cos, sin = tables(extra, n)
            piece = product[half * part : (half + 1) * part]
            for j in range(q_width // head):
                u = piece[:, j * head : (j + 1) * head]
                q[span, pl.ds(j * head, head)] = turn(u * root_scale(u) * gain_q, cos, sin).astype(bf16)
            u = piece[:, q_width : q_width + head]
            kv[span, pl.ds(0, head)] = turn(u * root_scale(u) * gain_k, cos, sin).astype(bf16)
            kv[span, pl.ds(head, head)] = piece[:, q_width + head :].astype(bf16)

    kv_far = lines.start(kv, kvp, near[HIGH])
    for source, target in ((a, a_out), (raw, raw_out), (q, q_out), (kv, kv_out), (extra, extra_out), (gains, gains_out)):
        moves.save(source, target)
    for dc in (0, 1):
        w_out.pass_x(dc)
    for dc in (0, 1):
        w_gate.send_x(dc)
    kv_far.wait_recv()
    w_gate.send_z(1)
    c_own = [moves.start(c_hbm.at[seq[ds]], c.at[ds]) for ds in (0, 1)]
    c_core = [lines.start(c_hbm.at[seq[ds]], c.at[4 + ds], near[CORE]) for ds in (0, 1)]
    c_low = lines.start(c_hbm.at[seq[0]], c.at[2], near[LOW])
    w_up.ready()
    for dc in (0, 1):
        w_up.send_x(dc)
    moves.save(kvp, kvp_out)
    scaling = head ** (-0.5)

    @pl.loop(0, 2)
    def _(n):
        @pl.loop(0, 2)
        def _(m):
            base = pl.multiple_of(n * (4 * part) + m * part, part)
            keys = jnp.concatenate([pair_rows(kv, base, part, (0, head)), pair_rows(kvp, base, part, (0, head))], axis=0)
            values = jnp.concatenate(
                [pair_rows(kv, base, part, (head, 2 * head)), pair_rows(kvp, base, part, (head, 2 * head))], axis=0
            )
            allowed = allowed_pairs(at, n, m, part, q_width // head, extra)
            scores = jnp.where(allowed, nt(stack_heads(q, base, part, head), keys) * scaling, -jnp.inf)
            peak = jnp.max(scores, axis=-1, keepdims=True)
            weights = jnp.exp(scores - peak)
            total = jnp.sum(weights, axis=-1, keepdims=True)
            mixed = nn(weights.astype(bf16), values) / total
            unstack(o, base, part, head, mixed)
            unstack(lse, base, part, head, jnp.broadcast_to(peak + jnp.log(total), mixed.shape))

    moves.save(o, o_out)
    moves.save(lse, lse_out)
    w_out.complete()
    moves.save(w_o, wo_out)
    out = x
    lines.settle([*x_far, x_across])

    def project(first):
        @pl.loop(0, 4)
        def _(m):
            n = first + m
            span = pl.ds(pl.multiple_of(n * part, part), part)
            out[n] = nn(o[span, :], w_o[...]).astype(bf16)

    project(4)
    sent = {k: lines.start(out.at[4 + k], from_core.at[k], near[CORE]) for k in (3, 1, 2, 0)}
    project(0)

    def pump_gate():
        w_up.send_z(1)
        for dc in (0, 1):
            w_gate.pass_x(dc)
        w_down.ready()
        for dc in (0, 1):
            w_down.send_x(dc)
        return share(near, lines, c, c_low)

    sums, (c_far, c_across) = sum_lines(near, lines, out, sent, (from_core, kept, second_a, second_b, from_z, from_y, last_a, last_b), lambda: w_up.send_z(0), pump_gate)
    h[...] = h[...] + sums
    moves.save(h, h_out)
    wide = h[...]
    b_all[0] = (wide * root_scale(wide) * gains[1:2, :]).astype(bf16)

    def pump_up():
        for dc in (0, 1):
            w_down.send_z(dc)
        for dc in (0, 1):
            w_up.pass_x(dc)
        c_far.append(pass_on(near, lines, c, c_across))

    spread_lines(near, lines, b_all, from_z.shape[2], pump_up)
    moves.save(b_all, b_out)

    w_gate.complete()

    w_up.complete()
    moves.save(wgu, wgu_out)

    @pl.loop(0, 4)
    def _(m):
        span = pl.ds(pl.multiple_of(m * rows, rows), rows)
        b = pair(b_all, m)
        g = nn(b, wgu[:, 0:hidden])
        u = nn(b, wgu[:, hidden : 2 * hidden])
        gu[span, pl.ds(0, hidden)] = g.astype(bf16)
        gu[span, pl.ds(hidden, hidden)] = u.astype(bf16)
        z[span, :] = (g * jax.nn.sigmoid(g) * u).astype(bf16)

    moves.save(z, z_out)
    moves.save(gu, gu_out)
    finish(c_own)
    arrive(c_core + c_far)
    moves.save(c, c_out)
    down = Grad(env, work_d, False, None, None, ())
    w_down.pass_x(0)
    eighths_of(down, 1, lambda run: tn(z[...], columns(c, run)))
    w_down.pass_x(1)
    eighths_of(down, 0, lambda run: tn(z[...], columns(c, run)))
    moves.save(work_d, work_d_out)
    w_down.complete()
    moves.save(w_d, wd_out)
    lines.close()
    moves.close()


def share(near, lines, ref, low):
    low.wait_recv()
    across = lines.start(ref.at[2], ref.at[3], near[ACROSS])
    return [lines.start(ref.at[2], ref.at[6], near[CORE])], across


def pass_on(near, lines, ref, across):
    across.wait_recv()
    return lines.start(ref.at[3], ref.at[7], near[CORE])


def pair(ref, m):
    return jnp.concatenate([ref[2 * m], ref[2 * m + 1]], axis=0)


class Sum:
    def __init__(self, near, lines, part, first, rooms):
        self.near, self.lines, self.part, self.first = near, lines, part, first
        self.from_core, self.kept, self.second_a, self.second_b, self.from_z, self.from_y, self.last_a, self.last_b = rooms
        width, self.cut = part.shape[2], self.from_z.shape[2]
        self.a, self.b = pl.ds(0, self.cut), pl.ds(self.cut, width - self.cut)

    def total(self, k):
        self.first[k].wait_recv()
        return self.part[k].astype(f32) + self.from_core[k].astype(f32)

    def begin(self):
        lines, near, kept = self.lines, self.near, self.kept
        kept[2] = self.total(3).astype(bf16)
        self.y1 = lines.start(kept.at[2, :, self.b], self.from_y.at[1], near[ACROSS])
        self.z1 = lines.start(kept.at[2, :, self.a], self.from_z.at[1], near[LOW])
        kept[0] = self.total(1).astype(bf16)
        self.y0 = lines.start(kept.at[0, :, self.b], self.from_y.at[0], near[ACROSS])
        kept[1] = self.total(2).astype(bf16)
        self.z0 = lines.start(kept.at[1, :, self.a], self.from_z.at[0], near[LOW])

    def middle(self):
        lines, near, kept = self.lines, self.near, self.kept
        self.y1.wait_recv()
        self.second_b[...] = (kept[1, :, self.b].astype(f32) + self.from_y[1].astype(f32)).astype(bf16)
        self.z2 = lines.start(self.second_b, self.last_b, near[LOW])
        self.z1.wait_recv()
        self.second_a[...] = (kept[0, :, self.a].astype(f32) + self.from_z[1].astype(f32)).astype(bf16)
        self.y2 = lines.start(self.second_a, self.last_a, near[ACROSS])

    def end(self):
        arrive((self.z0, self.y0, self.y2, self.z2))
        self.lines.settle([self.z1, self.y1, self.y0, self.z0, self.y2, self.z2])
        left = self.from_z[0].astype(f32) + self.last_a[...].astype(f32)
        right = self.from_y[0].astype(f32) + self.last_b[...].astype(f32)
        return jnp.concatenate([left, right], axis=1)


def sum_lines(near, lines, part, first, rooms, early, pump):
    parts = Sum(near, lines, part, first, rooms)
    parts.begin()
    early()
    parts.middle()
    extra = pump()
    mine = parts.total(0)
    lines.settle(list(first.values()))
    return mine + parts.end(), extra


def spread_lines(near, lines, out, cut, pump):
    width = out.shape[2]
    a, b = pl.ds(0, cut), pl.ds(cut, width - cut)
    zb = lines.start(out.at[0, :, b], out.at[2, :, b], near[LOW])
    ya = lines.start(out.at[0, :, a], out.at[1, :, a], near[ACROSS])
    yb = lines.start(out.at[0, :, b], out.at[1, :, b], near[ACROSS])
    za = lines.start(out.at[0, :, a], out.at[2, :, a], near[LOW])
    c0 = lines.start(out.at[0], out.at[4], near[CORE])
    ya.wait_recv()
    zc = lines.start(out.at[1, :, a], out.at[3, :, a], near[LOW])
    zb.wait_recv()
    yc = lines.start(out.at[2, :, b], out.at[3, :, b], near[ACROSS])
    yb.wait_recv()
    c1 = lines.start(out.at[1], out.at[5], near[CORE])
    za.wait_recv()
    c2 = lines.start(out.at[2], out.at[6], near[CORE])
    zc.wait_recv()
    yc.wait_recv()
    c3 = lines.start(out.at[3], out.at[7], near[CORE])
    pump()
    arrive((c0, c1, c2, c3))
    return [ya, zb, yb, za, c0, zc, yc, c1, c2, c3]


class Grad:
    def __init__(self, env, work, by_rows, over_x, over_z, outs, span=slice(None)):
        self.env, self.work, self.by_rows, self.outs, self.span = env, work, by_rows, outs, span
        self.from_x, self.from_z = over_x, over_z
        self.x, self.z, self.last, self.local = {}, {}, [], []

    def index(self, dx, dzh, dc):
        spot = pl.ds(run_start(self.env.at, dx, dzh, dc, self.env.ctx_count, self.env.block), 2 * self.env.block)
        return (spot, self.span) if self.by_rows else (self.span, spot)

    def send_x(self, dzh, dc):
        self.x[dzh, dc] = self.env.lines.start(
            self.work.at[self.index(1, dzh, dc)], self.from_x.at[2 * dzh + dc], self.env.near[ACROSS_X]
        )

    def pass_z(self, dc):
        self.x[1, dc].wait_recv()
        spot = self.index(0, 1, dc)
        self.work[spot] = (self.work[spot].astype(f32) + self.from_x[2 + dc].astype(f32)).astype(bf16)
        self.z[dc] = self.env.lines.start(self.work.at[spot], self.from_z.at[dc], self.env.near[HIGH])

    def deliver(self, dc):
        at, block = self.env.at, self.env.block
        self.x[0, dc].wait_recv()
        self.z[dc].wait_recv()
        spot = self.index(0, 0, dc)
        self.work[spot] = (
            self.work[spot].astype(f32) + self.from_x[dc].astype(f32) + self.from_z[dc].astype(f32)
        ).astype(bf16)
        slot = at["c"] * 2 + at["zl"]
        for dzl, name in ((1, (LOW, DIAG)[dc]), (0, (None, CORE)[dc])):
            start = run_start(at, 0, 0, dc, self.env.ctx_count, block) + flip(at["zl"], dzl) * block
            mine = pl.ds(pl.multiple_of(start, block), block)
            for out, low, size in self.outs:
                there = pl.ds(pl.multiple_of(slot * size, 128), size)
                if self.by_rows:
                    source, target = self.work.at[mine, pl.ds(low, size)], out.at[:, there]
                else:
                    source, target = self.work.at[:, mine], out.at[there, :]
                if name is None:
                    self.local.append(self.env.moves.start(source, target))
                else:
                    self.last.append(self.env.lines.start(source, target, self.env.near[name]))

    def finish(self):
        arrive(self.last)
        finish(self.local)


def eighths_of(unit, dx, make):
    @pl.loop(0, 2)
    def _(dzh):
        @pl.loop(0, 2)
        def _(dc):
            at, count = unit.env.at, unit.env.ctx_count
            near_zh = at["zh"] + dzh - 2 * at["zh"] * dzh
            near_c = at["c"] + dc - 2 * at["c"] * dc
            start = ((flip(at["x"], dx) * 2 + near_c) * count + near_zh * 2) * unit.env.block
            spot = pl.ds(pl.multiple_of(start, 2 * unit.env.block), 2 * unit.env.block)
            value = make(spot).astype(bf16)
            if unit.by_rows:
                unit.work[spot, :] = value
            else:
                unit.work[:, spot] = value


def columns(ref, run):
    block = ref[:, :, run]
    return block.reshape(block.shape[0] * block.shape[1], block.shape[2])


def backward_kernel(
    ctx_count, block, head,
    x_hbm, a_hbm, raw_hbm, q_hbm, kv_hbm, kvp_hbm, o_hbm, lse_hbm, h_hbm, b_hbm, z_hbm, gu_hbm, c_hbm, extra_hbm, gains_hbm,
    wqkv_hbm, wo_hbm, wgu_hbm, wd_hbm, work_hbm,
    out_hbm, in_hbm, g_query, g_key, g_value, g_out, g_gate, g_up, g_down, small_out,
    c, wd, z, gu, wgu, b, q, kv, kvp, o, lse, raw, extra, gains, wqkv, wo, h, dh, x_mine, dq, dkv, dkvp, got, do, dqkv,
    work_d, work_o, work_q, rx_d, rz_d, rx_g, rz_g, rx_u, rz_u, rx_o, rz_o, rx_q, rz_q,
    from_core, kept, second_a, second_b, from_z, from_y, last_a, last_b, own_out, own_in, sums, small, rx_s, rz_s, ry_s,
    send, recv, local, ready, done, free,
):
    at = place()
    near = neighbours(at)
    lines, moves = Lines(send, recv), Moves(local)
    env = Env(at, near, lines, moves, ctx_count, block)
    part, width = c.shape[1], c.shape[2]
    q_width = q.shape[1]
    hidden = z.shape[1]
    rows = 2 * part
    scaling = head ** (-0.5)
    fetch = moves.start
    get_work = fetch(work_hbm, work_d)
    get_c, get_d, get_gu = fetch(c_hbm, c), fetch(wd_hbm, wd), fetch(gu_hbm, gu)
    get_w, get_b, get_z = fetch(wgu_hbm, wgu), fetch(b_hbm, b), fetch(z_hbm, z)
    get_more = [fetch(*p) for p in ((h_hbm, h), (gains_hbm, gains), (wo_hbm, wo), (o_hbm, o))]
    get_rest = [
        fetch(*p)
        for p in ((q_hbm, q), (kv_hbm, kv), (kvp_hbm, kvp), (lse_hbm, lse), (raw_hbm, raw), (extra_hbm, extra), (wqkv_hbm, wqkv))
    ]
    get_x = fetch(x_hbm.at[at["y"]], x_mine)
    meet_all(near, (CORE, LOW, ACROSS, DIAG, HIGH, ACROSS_X))
    down = Grad(env, work_d, False, rx_d, rz_d, ((g_down, 0, hidden),))
    gate = Grad(env, wgu, True, rx_g, rz_g, ((g_gate, 0, hidden),), pl.ds(0, hidden))
    up = Grad(env, wgu, True, rx_u, rz_u, ((g_up, hidden, hidden),), pl.ds(hidden, hidden))
    outward = Grad(env, work_o, False, rx_o, rz_o, ((g_out, 0, q_width),))
    inward = Grad(env, work_q, True, rx_q, rz_q, ((g_query, 0, q_width), (g_key, q_width, head), (g_value, q_width + head, head)))

    get_work.wait()
    for dc in (0, 1):
        down.send_x(1, dc)
    get_c.wait()
    get_d.wait()
    get_gu.wait()
    dh[...] = c[0].astype(f32)

    @pl.loop(0, 4)
    def _(m):
        span = pl.ds(pl.multiple_of(m * rows, rows), rows)
        dz = nt(pair(c, m), wd[...])
        g = gu[span, pl.ds(0, hidden)].astype(f32)
        u = gu[span, pl.ds(hidden, hidden)].astype(f32)
        s = jax.nn.sigmoid(g)
        gu[span, pl.ds(0, hidden)] = (dz * u * s * (1.0 + g * (1.0 - s))).astype(bf16)
        gu[span, pl.ds(hidden, hidden)] = (dz * g * s).astype(bf16)

    get_w.wait()

    def spill(first, source, weight, back):
        @pl.loop(0, 2)
        def _(m):
            n = first // 2 + m
            span = pl.ds(pl.multiple_of(n * rows, rows), rows)
            product = (nt if back else nn)(source[span, :], weight[...]).astype(bf16)
            c[2 * n] = product[:part]
            c[2 * n + 1] = product[part:]

    def to_core():
        return {k: lines.start(c.at[4 + k], from_core.at[k], near[CORE]) for k in (3, 1, 2, 0)}

    spill(4, gu, wgu, True)
    sent = to_core()
    spill(0, gu, wgu, True)
    get_b.wait()
    both = Grad(env, wgu, True, None, None, ())
    eighths_of(both, 1, lambda run: tn(columns(b, run), gu[...]))
    for unit in (gate, up):
        for dc in (0, 1):
            unit.send_x(1, dc)
    finish(get_more)
    rooms = (from_core, kept, second_a, second_b, from_z, from_y, last_a, last_b)

    def tell(flag):
        for name in (CORE, LOW, ACROSS):
            pl.semaphore_signal(flag, inc=1, device_id=near[name], device_id_type=MESH)

    def pump_gate():
        for dc in (0, 1):
            down.send_x(0, dc)
        for unit in (gate, up):
            for dc in (0, 1):
                unit.send_x(0, dc)
        eighths_of(both, 0, lambda run: tn(columns(b, run), gu[...]))
        tell(ready)
        down.pass_z(1)

    db, _ = sum_lines(near, lines, c, sent, rooms, lambda: down.pass_z(0), pump_gate)
    wide = h[...]
    r = root_scale(wide)
    n_m = wide * r
    sums[1:2, :] = jnp.sum(db * n_m, axis=0, keepdims=True)
    t = db * gains[1:2, :]
    middle = dh[...] + r * (t - n_m * jnp.mean(t * n_m, axis=-1, keepdims=True))
    dh[...] = middle
    pl.semaphore_wait(ready, 3)
    b[0] = middle.astype(bf16)

    def pump_spread():
        gate.pass_z(0)
        up.pass_z(0)

    spread = spread_lines(near, lines, b, from_z.shape[2], pump_spread)

    @pl.loop(0, 4)
    def _(m):
        span = pl.ds(pl.multiple_of(m * rows, rows), rows)
        do[span, :] = nt(pair(b, m), wo[...]).astype(bf16)

    finish(get_rest)

    @pl.loop(0, 2)
    def _(n):
        @pl.loop(0, 2)
        def _(m):
            base = pl.multiple_of(n * (4 * part) + m * part, part)
            query = stack_heads(q, base, part, head)
            mixed = stack_heads(o, base, part, head)
            grad = stack_heads(do, base, part, head)
            level = stack_heads(lse, base, part, head)[:, :1]
            keys = jnp.concatenate([pair_rows(kv, base, part, (0, head)), pair_rows(kvp, base, part, (0, head))], axis=0)
            values = jnp.concatenate(
                [pair_rows(kv, base, part, (head, 2 * head)), pair_rows(kvp, base, part, (head, 2 * head))], axis=0
            )
            allowed = allowed_pairs(at, n, m, part, q_width // head, extra)
            probs = jnp.where(allowed, jnp.exp(jnp.where(allowed, nt(query, keys) * scaling - level, 0.0)), 0.0)
            dv = tn(probs.astype(bf16), grad)
            row_dot = jnp.sum(grad.astype(f32) * mixed.astype(f32), axis=-1, keepdims=True)
            ds = (probs * (nt(grad, values) - row_dot)).astype(bf16)
            unstack(dq, base, part, head, nn(ds, keys) * scaling)
            dk = tn(ds, query) * scaling
            for ref, top in ((dkv, 0), (dkvp, 2 * part)):
                for i in (0, 1):
                    spot = pl.ds(base + i * 2 * part, part)
                    low = top + i * part
                    ref[spot, pl.ds(0, head)] = dk[low : low + part].astype(ref.dtype)
                    ref[spot, pl.ds(head, head)] = dv[low : low + part].astype(ref.dtype)

    kv_far = lines.start(dkvp, got, near[HIGH])
    get_z.wait()
    gate.pass_z(1)
    eighths_of(outward, 1, lambda run: tn(o[...], columns(b, run)))
    for dzh, dc in ((1, 0), (1, 1), (0, 0), (0, 1)):
        outward.send_x(dzh, dc)
    eighths_of(outward, 0, lambda run: tn(o[...], columns(b, run)))
    lines.settle(spread)
    get_a = fetch(a_hbm, b)

    spill(4, z, wd, False)
    sent = to_core()
    spill(0, z, wd, False)
    outer = Sum(near, lines, c, sent, rooms)
    outer.begin()
    up.pass_z(1)
    h[...] = h[...] + outer.total(0)
    lines.settle(list(sent.values()))
    tell(done)
    outer.middle()

    kv_far.wait_recv()
    gain_q = gains[2:3, 0:head]
    gain_k = gains[3:4, 0:head]

    def through(u, w, gain, cos, sin):
        scale = root_scale(u)
        n = u * scale
        e = turn_back(w, cos, sin)
        f = e * gain
        grad = (scale * (f - n * jnp.mean(f * n, axis=-1, keepdims=True))).astype(bf16)
        return grad, jnp.sum(e * n, axis=0, keepdims=True)

    sums[2:4, 0:head] = jnp.zeros((2, head), f32)

    @pl.loop(0, 8)
    def _(n):
        span = pl.ds(pl.multiple_of(n * part, part), part)
        cos, sin = tables(extra, n)
        for j in range(q_width // head):
            cols = pl.ds(j * head, head)
            dqkv[span, cols], add = through(raw[span, cols], dq[span, cols], gain_q, cos, sin)
            sums[2:3, 0:head] += add
        dk = dkv[span, pl.ds(0, head)] + got[span, pl.ds(0, head)].astype(f32)
        dv = dkv[span, pl.ds(head, head)] + got[span, pl.ds(head, head)].astype(f32)
        cols = pl.ds(q_width, head)
        dqkv[span, cols], add = through(raw[span, cols], dk, gain_k, cos, sin)
        sums[3:4, 0:head] += add
        dqkv[span, pl.ds(q_width + head, head)] = dv.astype(bf16)

    spill(4, dqkv, wqkv, True)
    pl.semaphore_wait(done, 3)
    sent = to_core()
    get_a.wait()
    eighths_of(inward, 1, lambda run: tn(columns(b, run), dqkv[...]))
    for dzh, dc in ((1, 0), (1, 1), (0, 0), (0, 1)):
        inward.send_x(dzh, dc)
    spill(0, dqkv, wqkv, True)
    own_out[...] = (h[...] + outer.end()).astype(bf16)
    tell(free)
    out_far = lines.start(own_out, out_hbm.at[at["y"]], near[ACROSS])
    moves.save(own_out, out_hbm.at[at["y"]])
    for dc in (0, 1):
        outward.pass_z(dc)
    get_x.wait()

    def pump_in():
        eighths_of(inward, 0, lambda run: tn(columns(b, run), dqkv[...]))
        for dc in (0, 1):
            inward.pass_z(dc)
        for dc in (0, 1):
            down.deliver(dc)

    pl.semaphore_wait(free, 3)
    da, _ = sum_lines(near, lines, c, sent, rooms, lambda: None, pump_in)
    wide = x_mine[...].astype(f32)
    r = root_scale(wide)
    n_a = wide * r
    sums[0:1, :] = jnp.sum(da * n_a, axis=0, keepdims=True)
    f = da * gains[0:1, :]
    own_in[...] = (dh[...] + r * (f - n_a * jnp.mean(f * n_a, axis=-1, keepdims=True))).astype(bf16)
    in_far = lines.start(own_in, in_hbm.at[at["y"]], near[ACROSS])
    moves.save(own_in, in_hbm.at[at["y"]])

    ranks = small.shape[0]
    for n in range(ranks):
        small[n, 0:2, :] = sums[0:2, n * block : (n + 1) * block]
        small[n, 2:4, :] = sums[2:4, 0:head]
        small[n, 4:8, :] = jnp.zeros((4, block), f32)

    def few(dx, dzh, dc):
        return pl.ds((flip(at["x"], dx) * 2 + flip(at["c"], dc)) * ctx_count + flip(at["zh"], dzh) * 2, 2)

    over_x = {k: lines.start(small.at[few(1, *k)], rx_s.at[2 * k[0] + k[1]], near[ACROSS_X]) for k in ((1, 0), (1, 1), (0, 0), (0, 1))}
    over_z = []
    for dc in (0, 1):
        over_x[1, dc].wait_recv()
        small[few(0, 1, dc)] += rx_s[2 + dc]
        over_z.append(lines.start(small.at[few(0, 1, dc)], rz_s.at[dc], near[HIGH]))
    for unit in (gate, up):
        for dc in (0, 1):
            unit.deliver(dc)
    for dc in (0, 1):
        over_x[0, dc].wait_recv()
        over_z[dc].wait_recv()
        small[few(0, 0, dc)] += rx_s[dc] + rz_s[dc]
    base = few(0, 0, 0).start
    side = few(0, 0, 1).start
    spread = [
        lines.start(small.at[base + 1 - at["zl"]], ry_s.at[0], near[LOW]),
        lines.start(small.at[side + at["zl"]], ry_s.at[1], near[CORE]),
        lines.start(small.at[side + 1 - at["zl"]], ry_s.at[2], near[DIAG]),
    ]
    for dc in (0, 1):
        outward.deliver(dc)
    arrive(spread)
    ry_s[3] = small[base + at["zl"]] + ry_s[0] + ry_s[1] + ry_s[2]
    across = lines.start(ry_s.at[3], ry_s.at[4], near[ACROSS])
    for dc in (0, 1):
        inward.deliver(dc)
    across.wait_recv()
    small_out[...] = ry_s[3] + ry_s[4]
    for unit in (down, gate, up, outward, inward):
        unit.finish()
    arrive((out_far, in_far))
    lines.close()
    moves.close()


def widen_kernel(count, *refs):
    source, target, narrow, wide = (refs[n * count : (n + 1) * count] for n in range(4))
    moves = Moves(refs[4 * count])
    begun = [moves.start(source[n], narrow[n]) for n in range(count)]
    for n in range(count):
        begun[n].wait()
        steps = 8
        rows = narrow[n].shape[0] // steps

        @pl.loop(0, steps)
        def _(m):
            span = pl.ds(pl.multiple_of(m * rows, rows), rows)
            wide[n][span, :] = narrow[n][span, :].astype(f32)

        moves.save(wide[n], target[n])
    moves.close()


VM = pl.BlockSpec(memory_space=pltpu.VMEM)
HB = pl.BlockSpec(memory_space=pl.ANY)


def shaped(shape, dtype):
    return jax.ShapeDtypeStruct(shape, dtype)


def split_device(
    block_input, doc_positions, out_cotangent, attn_gain, mlp_gain, query_gain, key_gain,
    w_query, w_key, w_value, w_out, w_gate, w_up, w_down,
):
    dp_count = lax.axis_size(DP)
    ctx_count = lax.axis_size(CTX)
    rank_count = dp_count * ctx_count
    at = place()
    rank = at[DP] * ctx_count + at[CTX]
    upper = at["y"] == 1
    seqs, part, width = block_input.shape
    block = attn_gain.shape[0]
    head_piece = query_gain.shape[0]
    head = head_piece * rank_count
    own_p = jnp.where(upper, doc_positions[::-1], doc_positions).astype(f32)
    inverse = rope_base ** (-2.0 * jnp.arange(head // 2).astype(f32) / head)
    angles = own_p[:, :, None] * inverse
    extra = jnp.stack(
        [jnp.concatenate([jnp.cos(angles), jnp.sin(angles)], axis=2), jnp.broadcast_to(own_p[:, :, None], (seqs, part, head))],
        axis=1,
    )
    small = jnp.stack([query_gain, key_gain]).astype(f32)
    small = lax.dynamic_update_slice(jnp.zeros((2, head), f32), small, (0, rank * head_piece))
    own_gains = jnp.concatenate([jnp.stack([attn_gain, mlp_gain]).astype(f32), small, jnp.zeros((4, block), f32)])

    tokens = 4 * seqs * part
    q_width = w_query.shape[1] // 4
    hidden = w_gate.shape[1] // 4
    bound = functools.partial
    eighths = (8, part, width)
    cut = width // 4
    sum_room = [
        pltpu.VMEM((4, part, width), bf16), pltpu.VMEM((3, part, width), bf16),
        pltpu.VMEM((part, cut), bf16), pltpu.VMEM((part, width - cut), bf16),
        pltpu.VMEM((2, part, cut), bf16), pltpu.VMEM((2, part, width - cut), bf16),
        pltpu.VMEM((part, cut), bf16), pltpu.VMEM((part, width - cut), bf16),
    ]
    shapes = {
        "a": ((tokens, width), bf16), "raw": ((tokens, q_width + head), f32), "q": ((tokens, q_width), bf16),
        "kv": ((tokens, 2 * head), bf16), "kvp": ((tokens, 2 * head), bf16), "o": ((tokens, q_width), bf16),
        "lse": ((tokens, q_width), f32), "h": ((part, width), f32), "b": (eighths, bf16), "z": ((tokens, hidden), bf16),
        "gu": ((tokens, 2 * hidden), bf16), "c": (eighths, bf16), "extra": ((8, 2, part, head), f32), "gains": ((8, width), f32),
        "wqkv": ((width, q_width + 2 * head), bf16), "wo": ((q_width, width), bf16),
        "wgu": ((width, 2 * hidden), bf16), "wd": ((hidden, width), bf16), "work": ((hidden, width), bf16),
    }
    room = {name: pltpu.VMEM(*spec) for name, spec in shapes.items()}
    kept = pl.pallas_call(
        bound(forward_kernel, ctx_count, block, head),
        out_shape=[shaped(*spec) for spec in shapes.values()],
        in_specs=[HB] * 11,
        out_specs=[HB] * len(shapes),
        scratch_shapes=[
            pltpu.VMEM(eighths, bf16), room["extra"], pltpu.VMEM((rank_count, 8, block), f32),
            room["wqkv"], room["wo"], room["wgu"], room["wd"], room["a"], room["raw"], room["q"], room["kv"], room["kvp"],
            room["o"], room["lse"], *sum_room,
            room["h"], room["b"], room["z"], room["gu"], room["c"], room["gains"], room["work"],
            pltpu.SemaphoreType.DMA((160,)), pltpu.SemaphoreType.DMA((160,)), pltpu.SemaphoreType.DMA((64,)),
        ],
        compiler_params=pltpu.CompilerParams(collective_id=0, has_side_effects=True, vmem_limit_bytes=63 * 1024 * 1024),
    )(block_input, out_cotangent, extra, own_gains, w_query, w_key, w_value, w_out, w_gate, w_up, w_down)
    kept = dict(zip(shapes, kept))
    pair_shape = (seqs, part, width)
    names = (
        "a", "raw", "q", "kv", "kvp", "o", "lse", "h", "b", "z", "gu", "c", "extra", "gains", "wqkv", "wo", "wgu", "wd", "work",
    )
    run = 2 * block
    vmem = pltpu.VMEM
    wide_q = q_width + 2 * head
    outs = pl.pallas_call(
        bound(backward_kernel, ctx_count, block, head),
        out_shape=[
            shaped(pair_shape, bf16), shaped(pair_shape, bf16),
            shaped(w_query.shape, bf16), shaped(w_key.shape, bf16), shaped(w_value.shape, bf16), shaped(w_out.shape, bf16),
            shaped(w_gate.shape, bf16), shaped(w_up.shape, bf16), shaped(w_down.shape, bf16), shaped((8, block), f32),
        ],
        in_specs=[HB] * (1 + len(names)),
        out_specs=[HB] * 9 + [VM],
        scratch_shapes=[
            *(room[k] for k in ("c", "wd", "z", "gu", "wgu", "b", "q", "kv", "kvp", "o", "lse", "raw", "extra", "gains", "wqkv", "wo", "h")),
            vmem((part, width), f32), vmem((part, width), bf16),
            vmem((tokens, q_width), f32), vmem((tokens, 2 * head), f32), vmem((tokens, 2 * head), bf16), vmem((tokens, 2 * head), bf16),
            vmem((tokens, q_width), bf16), vmem((tokens, wide_q), bf16),
            vmem((hidden, width), bf16), vmem((q_width, width), bf16), vmem((width, wide_q), bf16),
            vmem((4, hidden, run), bf16), vmem((2, hidden, run), bf16),
            vmem((4, run, hidden), bf16), vmem((2, run, hidden), bf16),
            vmem((4, run, hidden), bf16), vmem((2, run, hidden), bf16),
            vmem((4, q_width, run), bf16), vmem((2, q_width, run), bf16),
            vmem((4, run, wide_q), bf16), vmem((2, run, wide_q), bf16),
            *sum_room,
            vmem((part, width), bf16), vmem((part, width), bf16), vmem((8, width), f32),
            vmem((rank_count, 8, block), f32), vmem((4, 2, 8, block), f32), vmem((2, 2, 8, block), f32), vmem((5, 8, block), f32),
            pltpu.SemaphoreType.DMA((160,)), pltpu.SemaphoreType.DMA((160,)), pltpu.SemaphoreType.DMA((64,)),
            pltpu.SemaphoreType.REGULAR, pltpu.SemaphoreType.REGULAR, pltpu.SemaphoreType.REGULAR,
        ],
        compiler_params=pltpu.CompilerParams(collective_id=1, has_side_effects=True, vmem_limit_bytes=67043328),
    )(block_input, kept["a"].reshape(eighths), *(kept[k] for k in names[1:]))
    small = outs[9]
    slots = small[2:4].reshape(2, rank_count, head_piece)
    slots = lax.dynamic_index_in_dim(slots, rank, 1, keepdims=False)
    narrow = (outs[1].reshape(seqs * part, width), *outs[2:9])
    wide = pl.pallas_call(
        bound(widen_kernel, len(narrow)),
        out_shape=[shaped(array.shape, f32) for array in narrow],
        in_specs=[HB] * len(narrow),
        out_specs=[HB] * len(narrow),
        scratch_shapes=[
            *(vmem(array.shape, bf16) for array in narrow), *(vmem(array.shape, f32) for array in narrow),
            pltpu.SemaphoreType.DMA((2 * len(narrow),)),
        ],
        compiler_params=pltpu.CompilerParams(vmem_limit_bytes=48 * 1024 * 1024),
    )(*narrow)
    return (outs[0], wide[0].reshape(pair_shape), small[0], small[1], slots[0], slots[1], *wide[1:])


def rms_scale(value_rows):
    return lax.rsqrt(jnp.mean(value_rows * value_rows, axis=-1, keepdims=True) + eps_norm)


def rope_tables(places, head_size):
    half_size = head_size // 2
    inverse = rope_base ** (-2.0 * jnp.arange(half_size).astype(jnp.float32) / head_size)
    angles = places.astype(jnp.float32)[:, None] * inverse[None, :]
    angles = jnp.concatenate([angles, angles], axis=-1)
    return (jnp.cos(angles), jnp.sin(angles))


def rotate(values, cosine, sine):
    half_size = values.shape[-1] // 2
    turned = jnp.concatenate([-values[..., half_size:], values[..., :half_size]], axis=-1)
    return values * cosine[:, None, :] + turned * sine[:, None, :]


def rotate_back(grads, cosine, sine):
    half_size = grads.shape[-1] // 2
    weighted = grads * sine[:, None, :]
    return grads * cosine[:, None, :] + jnp.concatenate(
        [weighted[..., half_size:], -weighted[..., :half_size]], axis=-1
    )


def block_mask(query_index, lowest, key_index):
    return (key_index[None, :] <= query_index[:, None]) & (key_index[None, :] >= lowest[:, None])


def dot_nt(left, right):
    return lax.dot_general(
        left, right, (((1,), (1,)), ((), ())), preferred_element_type=jnp.float32
    )


def dot_tn(left, right):
    return lax.dot_general(
        left, right, (((0,), (0,)), ((), ())), preferred_element_type=jnp.float32
    )


def micro_pass(inputs_seq, places, cotangent, shards, totals):
    float_type = jnp.float32
    half_type = jnp.bfloat16
    fetched = (
        lax.all_gather(shards[0], (DP, CTX), axis=0, tiled=True),
        lax.all_gather(shards[1], (DP, CTX), axis=0, tiled=True),
        lax.all_gather(shards[2], (DP, CTX), axis=0, tiled=True),
        lax.all_gather(shards[3], (DP, CTX), axis=0, tiled=True),
        lax.all_gather(shards[4], (DP, CTX), axis=0, tiled=True),
        lax.all_gather(shards[5], (DP, CTX), axis=0, tiled=True),
        lax.all_gather(shards[6], (DP, CTX), axis=0, tiled=True),
        lax.all_gather(shards[7], (DP, CTX), axis=1, tiled=True),
        lax.all_gather(shards[8], (DP, CTX), axis=0, tiled=True),
        lax.all_gather(shards[9], (DP, CTX), axis=0, tiled=True),
        lax.all_gather(shards[10], (DP, CTX), axis=1, tiled=True),
    )
    gain_attn = fetched[0].astype(float_type)
    gain_mlp = fetched[1].astype(float_type)
    gain_query = fetched[2].astype(float_type)
    gain_key = fetched[3].astype(float_type)
    query_proj, key_proj, value_proj, out_proj, gate_proj, up_proj, down_proj = fetched[4:]
    head_size = gain_query.shape[0]
    head_count = query_proj.shape[1] // head_size
    kv_count = key_proj.shape[1] // head_size
    group_size = head_count // kv_count
    token_count = inputs_seq.shape[0]
    ctx_count = lax.axis_size(CTX)
    ctx_rank = lax.axis_index(CTX)
    scaling = head_size ** (-0.5)
    query_index = ctx_rank * token_count + jnp.arange(token_count, dtype=jnp.int32)
    lowest = query_index - places
    last_query = ctx_rank * token_count + token_count - 1
    residual_in = inputs_seq.astype(float_type)
    scale_attn = rms_scale(residual_in)
    normed_attn = residual_in * scale_attn
    attn_input = (normed_attn * gain_attn).astype(half_type)
    query_raw = jnp.dot(attn_input, query_proj, preferred_element_type=float_type).reshape(
        token_count, head_count, head_size
    )
    key_raw = jnp.dot(attn_input, key_proj, preferred_element_type=float_type).reshape(
        token_count, kv_count, head_size
    )
    value_rows = jnp.dot(attn_input, value_proj, preferred_element_type=float_type).astype(
        half_type
    )
    query_scale = rms_scale(query_raw)
    query_normed = query_raw * query_scale
    key_scale = rms_scale(key_raw)
    key_normed = key_raw * key_scale
    cosine, sine = rope_tables(places, head_size)
    query_rot = rotate(query_normed * gain_query, cosine, sine).astype(half_type)
    key_rot = (
        rotate(key_normed * gain_key, cosine, sine)
        .astype(half_type)
        .reshape(token_count, kv_count * head_size)
    )
    query_group = query_rot.reshape(token_count, kv_count, group_size, head_size)
    initial = (
        jnp.full((kv_count, group_size, token_count), -1e30, float_type),
        jnp.zeros((kv_count, group_size, token_count), float_type),
        jnp.zeros((token_count, kv_count, group_size, head_size), float_type),
    )
    pieces = (
        lax.all_gather(key_rot, CTX, axis=0, tiled=True),
        lax.all_gather(value_rows, CTX, axis=0, tiled=True),
    )
    row_count = pieces[0].shape[0]
    key_piece = pieces[0].reshape(row_count, kv_count, head_size)
    value_piece = pieces[1].reshape(row_count, kv_count, head_size)

    def fold_attend(state):
        peak, total, running = state
        scores = (
            jnp.einsum("qkgd,jkd->kgqj", query_group, key_piece, preferred_element_type=float_type)
            * scaling
        )
        allowed = block_mask(query_index, lowest, jnp.arange(row_count, dtype=jnp.int32))
        new_peak = jnp.maximum(peak, jnp.max(jnp.where(allowed, scores, -jnp.inf), axis=-1))
        weights = jnp.where(allowed, jnp.exp(scores - new_peak[..., None]), 0.0)
        total = jnp.sum(weights, axis=-1)
        running = jnp.einsum(
            "kgqj,jkd->qkgd",
            weights.astype(half_type),
            value_piece,
            preferred_element_type=float_type,
        )
        return (new_peak, total, running)

    peak, total, running = lax.cond(
        jnp.int32(0) <= last_query, fold_attend, lambda state: state, initial
    )
    attn_rows = (
        (running / jnp.transpose(total, (2, 0, 1))[..., None])
        .astype(half_type)
        .reshape(token_count, head_count * head_size)
    )
    log_total = peak + jnp.log(total)
    attn_out = lax.psum(
        jnp.dot(attn_rows, out_proj, preferred_element_type=float_type).astype(jnp.bfloat16), MP
    ).astype(jnp.float32)
    middle = residual_in + attn_out
    scale_mlp = rms_scale(middle)
    normed_mlp = middle * scale_mlp
    mlp_input = (normed_mlp * gain_mlp).astype(half_type)
    gate_rows = jnp.dot(mlp_input, gate_proj, preferred_element_type=float_type)
    up_rows = jnp.dot(mlp_input, up_proj, preferred_element_type=float_type)
    sigmoid_gate = jax.nn.sigmoid(gate_rows)
    hidden_rows = (gate_rows * sigmoid_gate * up_rows).astype(half_type)
    mlp_out = lax.psum(
        jnp.dot(hidden_rows, down_proj, preferred_element_type=float_type).astype(jnp.bfloat16),
        MP,
    ).astype(jnp.float32)
    block_output = (middle + mlp_out).astype(half_type)
    refetched = (
        lax.all_gather(shards[0], (DP, CTX), axis=0, tiled=True),
        lax.all_gather(shards[1], (DP, CTX), axis=0, tiled=True),
        lax.all_gather(shards[2], (DP, CTX), axis=0, tiled=True),
        lax.all_gather(shards[3], (DP, CTX), axis=0, tiled=True),
        lax.all_gather(shards[4], (DP, CTX), axis=0, tiled=True),
        lax.all_gather(shards[5], (DP, CTX), axis=0, tiled=True),
        lax.all_gather(shards[6], (DP, CTX), axis=0, tiled=True),
        lax.all_gather(shards[7], (DP, CTX), axis=1, tiled=True),
        lax.all_gather(shards[8], (DP, CTX), axis=0, tiled=True),
        lax.all_gather(shards[9], (DP, CTX), axis=0, tiled=True),
        lax.all_gather(shards[10], (DP, CTX), axis=1, tiled=True),
    )
    gain_attn = refetched[0].astype(float_type)
    gain_mlp = refetched[1].astype(float_type)
    gain_query = refetched[2].astype(float_type)
    gain_key = refetched[3].astype(float_type)
    query_proj, key_proj, value_proj, out_proj, gate_proj, up_proj, down_proj = refetched[4:]
    down_grad = dot_tn(hidden_rows, cotangent)
    hidden_grad = dot_nt(cotangent, down_proj)
    gate_grad = (
        hidden_grad * up_rows * sigmoid_gate * (1.0 + gate_rows * (1.0 - sigmoid_gate))
    ).astype(half_type)
    up_grad = (hidden_grad * gate_rows * sigmoid_gate).astype(half_type)
    gate_proj_grad = dot_tn(mlp_input, gate_grad)
    up_proj_grad = dot_tn(mlp_input, up_grad)
    mlp_in_grad = lax.psum(
        (dot_nt(gate_grad, gate_proj) + dot_nt(up_grad, up_proj)).astype(jnp.bfloat16), MP
    ).astype(jnp.float32)
    mlp_gain_grad = jnp.sum(mlp_in_grad * normed_mlp, axis=0)
    normed_grad = mlp_in_grad * gain_mlp
    middle_grad = cotangent.astype(float_type) + scale_mlp * (
        normed_grad - normed_mlp * jnp.mean(normed_grad * normed_mlp, axis=-1, keepdims=True)
    )
    middle_half = middle_grad.astype(half_type)
    out_proj_grad = dot_tn(attn_rows, middle_half)
    attn_grad = dot_nt(middle_half, out_proj).astype(half_type)
    grad_group = attn_grad.reshape(token_count, kv_count, group_size, head_size)
    attn_group = attn_rows.reshape(token_count, kv_count, group_size, head_size)
    row_dot = jnp.einsum(
        "qkgd,qkgd->kgq", grad_group, attn_group, preferred_element_type=float_type
    )
    key_back, value_back = (
        lax.all_gather(key_rot, CTX, axis=0, tiled=True),
        lax.all_gather(value_rows, CTX, axis=0, tiled=True),
    )

    def back_block(query_sum, block_id):
        start = block_id * token_count
        key_piece = lax.dynamic_slice_in_dim(key_back, start, token_count, 0).reshape(
            token_count, kv_count, head_size
        )
        value_piece = lax.dynamic_slice_in_dim(value_back, start, token_count, 0).reshape(
            token_count, kv_count, head_size
        )

        def back_attend(running):
            scores = (
                jnp.einsum(
                    "qkgd,jkd->kgqj", query_group, key_piece, preferred_element_type=float_type
                )
                * scaling
            )
            allowed = block_mask(
                query_index, lowest, start + jnp.arange(token_count, dtype=jnp.int32)
            )
            probs = jnp.where(allowed, jnp.exp(scores - log_total[..., None]), 0.0)
            value_part = jnp.einsum(
                "kgqj,qkgd->jkd",
                probs.astype(half_type),
                grad_group,
                preferred_element_type=float_type,
            )
            prob_grad = jnp.einsum(
                "qkgd,jkd->kgqj", grad_group, value_piece, preferred_element_type=float_type
            )
            score_half = (probs * (prob_grad - row_dot[..., None])).astype(half_type)
            query_part = (
                jnp.einsum(
                    "kgqj,jkd->qkgd", score_half, key_piece, preferred_element_type=float_type
                )
                * scaling
            )
            key_part = (
                jnp.einsum(
                    "kgqj,qkgd->jkd", score_half, query_group, preferred_element_type=float_type
                )
                * scaling
            )
            return (
                running + query_part,
                jnp.concatenate(
                    [
                        key_part.reshape(token_count, kv_count * head_size),
                        value_part.reshape(token_count, kv_count * head_size),
                    ],
                    axis=-1,
                ),
            )

        def passing(running):
            return (running, jnp.zeros((token_count, 2 * kv_count * head_size), float_type))

        return lax.cond(start <= last_query, back_attend, passing, query_sum)

    query_grad, kv_terms = lax.scan(
        back_block,
        jnp.zeros((token_count, kv_count, group_size, head_size), float_type),
        jnp.arange(ctx_count, dtype=jnp.int32),
    )
    kv_grad = lax.psum_scatter(
        kv_terms.reshape(ctx_count * token_count, 2 * kv_count * head_size).astype(jnp.bfloat16),
        CTX,
        scatter_dimension=0,
        tiled=True,
    ).astype(jnp.float32)
    key_rot_grad = kv_grad[:, : kv_count * head_size].reshape(token_count, kv_count, head_size)
    value_half = kv_grad[:, kv_count * head_size :].astype(half_type)
    query_back = rotate_back(query_grad.reshape(token_count, head_count, head_size), cosine, sine)
    key_grad_back = rotate_back(key_rot_grad, cosine, sine)
    query_gain_part = jnp.sum(query_back * query_normed, axis=(0, 1))
    key_gain_part = jnp.sum(key_grad_back * key_normed, axis=(0, 1))
    query_ngrad = query_back * gain_query
    key_ngrad = key_grad_back * gain_key
    query_half = (
        (
            query_scale
            * (
                query_ngrad
                - query_normed * jnp.mean(query_ngrad * query_normed, axis=-1, keepdims=True)
            )
        )
        .reshape(token_count, head_count * head_size)
        .astype(half_type)
    )
    key_half = (
        (
            key_scale
            * (key_ngrad - key_normed * jnp.mean(key_ngrad * key_normed, axis=-1, keepdims=True))
        )
        .reshape(token_count, kv_count * head_size)
        .astype(half_type)
    )
    query_proj_grad = dot_tn(attn_input, query_half)
    key_proj_grad = dot_tn(attn_input, key_half)
    value_proj_grad = dot_tn(attn_input, value_half)
    attn_in_grad, query_gain_sum, key_gain_sum = (
        lax.psum(
            (
                dot_nt(query_half, query_proj)
                + dot_nt(key_half, key_proj)
                + dot_nt(value_half, value_proj)
            ).astype(jnp.bfloat16),
            MP,
        ).astype(jnp.float32),
        lax.psum(query_gain_part.astype(jnp.bfloat16), MP).astype(jnp.float32),
        lax.psum(key_gain_part.astype(jnp.bfloat16), MP).astype(jnp.float32),
    )
    attn_gain_grad = jnp.sum(attn_in_grad * normed_attn, axis=0)
    normed_in_grad = attn_in_grad * gain_attn
    input_grad = middle_grad + scale_attn * (
        normed_in_grad
        - normed_attn * jnp.mean(normed_in_grad * normed_attn, axis=-1, keepdims=True)
    )
    addition = (
        attn_gain_grad,
        mlp_gain_grad,
        query_gain_sum,
        key_gain_sum,
        query_proj_grad,
        key_proj_grad,
        value_proj_grad,
        out_proj_grad,
        gate_proj_grad,
        up_proj_grad,
        down_grad,
    )
    totals = tuple((earlier + later for earlier, later in zip(totals, addition)))
    return (block_output, input_grad, totals)


def on_device(
    block_input,
    doc_positions,
    out_cotangent,
    attn_gain,
    mlp_gain,
    query_gain,
    key_gain,
    w_query,
    w_key,
    w_value,
    w_out,
    w_gate,
    w_up,
    w_down,
):
    shards = (
        attn_gain,
        mlp_gain,
        query_gain,
        key_gain,
        w_query,
        w_key,
        w_value,
        w_out,
        w_gate,
        w_up,
        w_down,
    )
    head_size = query_gain.shape[0] * lax.axis_size((DP, CTX))
    model_width = block_input.shape[2]
    query_width = w_query.shape[1]
    kv_width = w_key.shape[1]
    hidden_width = w_gate.shape[1]
    totals = (
        jnp.zeros((model_width,), jnp.float32),
        jnp.zeros((model_width,), jnp.float32),
        jnp.zeros((head_size,), jnp.float32),
        jnp.zeros((head_size,), jnp.float32),
        jnp.zeros((model_width, query_width), jnp.float32),
        jnp.zeros((model_width, kv_width), jnp.float32),
        jnp.zeros((model_width, kv_width), jnp.float32),
        jnp.zeros((query_width, model_width), jnp.float32),
        jnp.zeros((model_width, hidden_width), jnp.float32),
        jnp.zeros((model_width, hidden_width), jnp.float32),
        jnp.zeros((hidden_width, model_width), jnp.float32),
    )
    output_list = []
    grad_list = []
    for micro in range(block_input.shape[0]):
        output_rows, input_rows, totals = micro_pass(
            block_input[micro], doc_positions[micro], out_cotangent[micro], shards, totals
        )
        output_list.append(output_rows)
        grad_list.append(input_rows)
    owned = (
        lax.psum_scatter(totals[0], (DP, CTX), scatter_dimension=0, tiled=True),
        lax.psum_scatter(totals[1], (DP, CTX), scatter_dimension=0, tiled=True),
        lax.psum_scatter(totals[2], (DP, CTX), scatter_dimension=0, tiled=True),
        lax.psum_scatter(totals[3], (DP, CTX), scatter_dimension=0, tiled=True),
        lax.psum_scatter(totals[4], (DP, CTX), scatter_dimension=0, tiled=True),
        lax.psum_scatter(totals[5], (DP, CTX), scatter_dimension=0, tiled=True),
        lax.psum_scatter(totals[6], (DP, CTX), scatter_dimension=0, tiled=True),
        lax.psum_scatter(totals[7], (DP, CTX), scatter_dimension=1, tiled=True),
        lax.psum_scatter(totals[8], (DP, CTX), scatter_dimension=0, tiled=True),
        lax.psum_scatter(totals[9], (DP, CTX), scatter_dimension=0, tiled=True),
        lax.psum_scatter(totals[10], (DP, CTX), scatter_dimension=1, tiled=True),
    )
    return (
        jnp.stack(output_list),
        jnp.stack(grad_list),
        owned[0],
        owned[1],
        owned[2],
        owned[3],
        owned[4],
        owned[5],
        owned[6],
        owned[7],
        owned[8],
        owned[9],
        owned[10],
    )


def choose(mesh, arrays):
    dp, ctx, mp = mesh.shape[DP], mesh.shape[CTX], mesh.shape[MP]
    width = arrays[0].shape[2]
    paired = dp == 4 and ctx == 4 and mp == 2
    return split_device if paired and width % (dp * ctx * 128) == 0 else on_device


def solution(mesh):
    in_specs = (
        P(DP, CTX, None),
        P(DP, CTX),
        P(DP, CTX, None),
        P((DP, CTX)),
        P((DP, CTX)),
        P((DP, CTX)),
        P((DP, CTX)),
        P((DP, CTX), MP),
        P((DP, CTX), MP),
        P((DP, CTX), MP),
        P(MP, (DP, CTX)),
        P((DP, CTX), MP),
        P((DP, CTX), MP),
        P(MP, (DP, CTX)),
    )
    out_specs = (
        P(DP, CTX, None),
        P(DP, CTX, None),
        P((DP, CTX)),
        P((DP, CTX)),
        P((DP, CTX)),
        P((DP, CTX)),
        P((DP, CTX), MP),
        P((DP, CTX), MP),
        P((DP, CTX), MP),
        P(MP, (DP, CTX)),
        P((DP, CTX), MP),
        P((DP, CTX), MP),
        P(MP, (DP, CTX)),
    )

    def run(*arrays):
        return jax.shard_map(
            choose(mesh, arrays), mesh=mesh, in_specs=in_specs, out_specs=out_specs, check_vma=False
        )(*arrays)

    return run
```

```python
import functools

import jax
import jax.numpy as jnp
from jax import lax
from jax.experimental import pallas as pl
from jax.experimental.pallas import tpu as pltpu
from jax.sharding import PartitionSpec as P

eps_norm = 1e-06
rope_base = 1000000.0
MESH = pl.DeviceIdType.MESH
f32 = jnp.float32
bf16 = jnp.bfloat16
DP, CTX, MP = "dp", "ctx", "mp"
CORE, LOW, ACROSS, DIAG, HIGH, ACROSS_X = range(6)
PIECES = ((0, 0), (0, 1), (1, 0), (1, 1))


def flip(value, bit):
    return 1 - value if bit else value


def place():
    dp = lax.axis_index(DP)
    ctx = lax.axis_index(CTX)
    return {
        DP: dp,
        CTX: ctx,
        "y": lax.axis_index(MP),
        "x": dp // 2,
        "c": dp % 2,
        "zh": ctx // 2,
        "zl": ctx % 2,
    }


def run_start(at, dx, dzh, dc, ctx_count, block):
    start = ((flip(at["x"], dx) * 2 + flip(at["c"], dc)) * ctx_count + flip(at["zh"], dzh) * 2) * block
    return pl.multiple_of(start, 2 * block)


def finish(copies):
    for copy in copies:
        copy.wait()


def nn(left, right):
    return lax.dot_general(left, right, (((1,), (0,)), ((), ())), preferred_element_type=f32)


def nt(left, right):
    return lax.dot_general(left, right, (((1,), (1,)), ((), ())), preferred_element_type=f32)


def tn(left, right):
    return lax.dot_general(left, right, (((0,), (0,)), ((), ())), preferred_element_type=f32)


def root_scale(values):
    return lax.rsqrt(jnp.mean(values * values, axis=-1, keepdims=True) + eps_norm)


def turn(values, cosine, sine):
    return values * cosine + pltpu.roll(values, values.shape[-1] // 2, 1) * sine


def turn_back(values, cosine, sine):
    return values * cosine + pltpu.roll(values * sine, values.shape[-1] // 2, 1)


def pair_rows(ref, base, part, span):
    far = base + 2 * part
    return jnp.concatenate(
        [ref[pl.ds(base, part), :][:, span[0] : span[1]], ref[pl.ds(far, part), :][:, span[0] : span[1]]], axis=0
    )


def allowed_pairs(at, n, m, part, heads, extra):
    def fold(index, size, times):
        for k in range(times - 1, 0, -1):
            index = jnp.where(index >= k * size, index - k * size, index)
        return index

    row = lax.broadcasted_iota(jnp.int32, (heads * 2 * part, 4 * part), 0)
    col = lax.broadcasted_iota(jnp.int32, (heads * 2 * part, 4 * part), 1)
    near = at["zl"] * part
    far = (1 - at["zl"]) * part
    row = fold(row, 2 * part, heads)
    query = jnp.where(row < part, row + near, row - part + far) + at["zh"] * 2 * part
    inner = fold(col, 2 * part, 2)
    key = jnp.where(inner < part, inner + near, inner - part + far)
    key = key + jnp.where(col < 2 * part, at["zh"], 1 - at["zh"]) * (2 * part)
    query, key = query.astype(f32), key.astype(f32)
    spot = jnp.concatenate([extra[n * 4 + m, 1], extra[n * 4 + 2 + m, 1]] * heads, axis=0)[:, :1]
    return (key <= query) & (key >= query - spot)


def stack_heads(ref, base, part, head):
    heads = ref.shape[1] // head
    return jnp.concatenate([pair_rows(ref, base, part, (h * head, (h + 1) * head)) for h in range(heads)], axis=0)


def unstack(ref, base, part, head, values):
    heads = ref.shape[1] // head
    for h in range(heads):
        top = 2 * part * h
        ref[pl.ds(base, part), pl.ds(h * head, head)] = values[top : top + part].astype(ref.dtype)
        ref[pl.ds(base + 2 * part, part), pl.ds(h * head, head)] = values[top + part : top + 2 * part].astype(ref.dtype)


def partners(at):
    return (
        {DP: at[DP] + 1 - 2 * at["c"]},
        {CTX: at[CTX] + 1 - 2 * at["zl"]},
        {MP: 1 - at["y"]},
    )


class Lines:
    def __init__(self, send, recv):
        self.send, self.recv, self.used, self.open = send, recv, 0, []

    def start(self, source, target, device):
        copy = pltpu.make_async_remote_copy(
            src_ref=source,
            dst_ref=target,
            send_sem=self.send.at[self.used],
            recv_sem=self.recv.at[self.used],
            device_id=device,
            device_id_type=MESH,
        )
        copy.start()
        self.used += 1
        self.open.append(copy)
        return copy

    def close(self):
        self.settle(list(self.open))

    def settle(self, copies):
        for copy in copies:
            copy.wait_send()
        self.open = [copy for copy in self.open if all(copy is not done for done in copies)]


class Moves:
    def __init__(self, sems):
        self.sems, self.used, self.open = sems, 0, []

    def start(self, source, target):
        copy = pltpu.make_async_copy(source, target, self.sems.at[self.used])
        copy.start()
        self.used += 1
        return copy

    def save(self, source, target):
        self.open.append(self.start(source, target))

    def close(self):
        finish(self.open)


def arrive(copies):
    for copy in copies:
        copy.wait_recv()


def neighbours(at):
    core, low, across = partners(at)
    return {
        CORE: core,
        LOW: low,
        ACROSS: across,
        DIAG: {**core, **low},
        HIGH: {CTX: at[CTX] + 2 - 4 * at["zh"]},
        ACROSS_X: {DP: at[DP] + 2 - 4 * at["x"]},
    }


def meet_all(near, names):
    barrier = pltpu.get_barrier_semaphore()
    for name in names:
        pl.semaphore_signal(barrier, inc=1, device_id=near[name], device_id_type=MESH)
    pl.semaphore_wait(barrier, len(names))


class Env:
    def __init__(self, at, near, lines, moves, ctx_count, block):
        self.at, self.near, self.lines, self.moves = at, near, lines, moves
        self.ctx_count, self.block = ctx_count, block


class Weight:
    def __init__(self, env, shard, target, by_rows, low, size):
        self.env, self.shard, self.target, self.by_rows, self.low, self.size = env, shard, target, by_rows, low, size
        self.over_z, self.own_x, self.far_x = [None, None], [None, None], [None, None]

    def mine(self):
        at, ctx_count, block = self.env.at, self.env.ctx_count, self.env.block
        spot = pl.ds(pl.multiple_of((at[DP] * ctx_count + at[CTX]) * block, block), block)
        return self.target.at[spot, pl.ds(self.low, self.size)] if self.by_rows else self.target.at[:, spot]

    def run(self, dx, dzh, dc):
        spot = pl.ds(run_start(self.env.at, dx, dzh, dc, self.env.ctx_count, self.env.block), 2 * self.env.block)
        return self.target.at[spot, pl.ds(self.low, self.size)] if self.by_rows else self.target.at[:, spot]

    def cut(self, dc, dzl):
        at = self.env.at
        start = pl.multiple_of((flip(at["c"], dc) * 2 + flip(at["zl"], dzl)) * self.size, 128)
        return self.shard.at[:, pl.ds(start, self.size)] if self.by_rows else self.shard.at[pl.ds(start, self.size), :]

    def exchange(self):
        near, lines = self.env.near, self.env.lines
        self.local = self.env.moves.start(self.cut(0, 0), self.mine())
        self.got = [
            lines.start(self.cut(dc, dzl), self.mine(), near[name])
            for dc, dzl, name in ((0, 1, LOW), (1, 0, CORE), (1, 1, DIAG))
        ]

    def ready(self):
        self.local.wait()
        arrive(self.got)

    def send_z(self, dc):
        self.over_z[dc] = self.env.lines.start(self.run(0, 0, dc), self.run(0, 0, dc), self.env.near[HIGH])

    def send_x(self, dc):
        self.own_x[dc] = self.env.lines.start(self.run(0, 0, dc), self.run(0, 0, dc), self.env.near[ACROSS_X])

    def pass_x(self, dc):
        self.over_z[dc].wait_recv()
        self.far_x[dc] = self.env.lines.start(self.run(0, 1, dc), self.run(0, 1, dc), self.env.near[ACROSS_X])

    def complete(self):
        arrive(self.own_x + self.far_x)


class Gains(Weight):
    def mine(self):
        return self.target.at[self.env.at[DP] * self.env.ctx_count + self.env.at[CTX]]

    def run(self, dx, dzh, dc):
        at = self.env.at
        return self.target.at[
            pl.ds((flip(at["x"], dx) * 2 + flip(at["c"], dc)) * self.env.ctx_count + flip(at["zh"], dzh) * 2, 2)
        ]

    def cut(self, dc, dzl):
        return self.shard


def tables(extra, n):
    packed = extra[n, 0]
    turned = pltpu.roll(packed, packed.shape[1] // 2, 1)
    first = lax.broadcasted_iota(jnp.int32, packed.shape, 1) < packed.shape[1] // 2
    return jnp.where(first, packed, turned), jnp.where(first, -turned, packed)


def forward_kernel(
    ctx_count, block, head,
    x_hbm, c_hbm, extra_hbm, gain_hbm, wq, wk, wv, wo, wg, wu, wd,
    a_out, raw_out, q_out, kv_out, kvp_out, o_out, lse_out, h_out, b_out, z_out, gu_out, c_out, extra_out, gains_out,
    wqkv_out, wo_out, wgu_out, wd_out, work_d_out,
    x, extra, gain_all, wqkv, w_o, wgu, w_d, a, raw, q, kv, kvp, o, lse, from_core, kept, second_a, second_b, from_z, from_y, last_a, last_b,
    h, b_all, z, gu, c, gains, work_d, send, recv, local,
):
    at = place()
    near = neighbours(at)
    lines, moves = Lines(send, recv), Moves(local)
    env = Env(at, near, lines, moves, ctx_count, block)
    part, width = x.shape[1], x.shape[2]
    q_width = q.shape[1]
    hidden = z.shape[1]
    rows = 2 * part
    meet_all(near, (CORE, LOW, ACROSS, DIAG, HIGH, ACROSS_X))

    seq = [flip(at["y"], ds) for ds in (0, 1)]
    units = (
        Weight(env, wq, wqkv, True, 0, q_width),
        Weight(env, wk, wqkv, True, q_width, head),
        Weight(env, wv, wqkv, True, q_width + head, head),
    )
    scale = Gains(env, gain_hbm, gain_all, True, 0, 0)
    w_out = Weight(env, wo, w_o, False, 0, q_width)
    w_gate = Weight(env, wg, wgu, True, 0, hidden)
    w_up = Weight(env, wu, wgu, True, hidden, hidden)
    w_down = Weight(env, wd, w_d, False, 0, hidden)
    for unit in (scale, *units, w_out):
        unit.exchange()
    x_low = lines.start(x_hbm.at[seq[0]], x.at[2], near[LOW])
    e_low = lines.start(extra_hbm.at[0], extra.at[2], near[LOW])
    w_gate.exchange()
    x_core = [lines.start(x_hbm.at[seq[ds]], x.at[4 + ds], near[CORE]) for ds in (0, 1)]
    e_core = lines.start(extra_hbm, extra.at[pl.ds(4, 2)], near[CORE])
    x_own = [moves.start(x_hbm.at[seq[ds]], x.at[ds]) for ds in (0, 1)]
    e_own = moves.start(extra_hbm, extra.at[pl.ds(0, 2)])
    for unit in (scale, *units):
        unit.ready()
    in_qkv = Weight(env, None, wqkv, True, 0, wqkv.shape[1])
    for dc in (0, 1):
        scale.send_z(dc)
        scale.send_x(dc)
        in_qkv.send_z(dc)
        in_qkv.send_x(dc)
    w_out.ready()
    for dc in (0, 1):
        w_out.send_z(dc)
        w_out.send_x(dc)
    x_far, x_across = share(near, lines, x, x_low)
    e_far, e_across = share(near, lines, extra, e_low)
    w_up.exchange()
    w_down.exchange()
    x_far.append(pass_on(near, lines, x, x_across))
    e_far.append(pass_on(near, lines, extra, e_across))
    for dc in (0, 1):
        scale.pass_x(dc)
        in_qkv.pass_x(dc)
    w_gate.ready()
    w_gate.send_z(0)
    scale.complete()
    gains[...] = jnp.zeros_like(gains)
    ranks = gain_all.shape[0]
    small = gain_all[0, 2:4, :]
    for n in range(ranks):
        gains[0:2, n * block : (n + 1) * block] = gain_all[n, 0:2, :]
        if n:
            small = small + gain_all[n, 2:4, :]
    gains[2:4, 0:head] = small

    finish(x_own)
    arrive(x_core + x_far)
    e_own.wait()
    arrive([e_core, *e_far])
    h[...] = x[0].astype(f32)

    @pl.loop(0, 8)
    def _(n):
        wide = x[n].astype(f32)
        span = pl.ds(pl.multiple_of(n * part, part), part)
        a[span, :] = (wide * root_scale(wide) * gains[0:1, :]).astype(bf16)

    in_qkv.complete()
    moves.save(wqkv, wqkv_out)
    gain_q = gains[2:3, 0:head]
    gain_k = gains[3:4, 0:head]

    @pl.loop(0, 4)
    def _(m):
        big = pl.ds(pl.multiple_of(m * rows, rows), rows)
        product = nn(a[big, :], wqkv[...])
        raw[big, :] = product[:, : q_width + head]
        for half in (0, 1):
            n = 2 * m + half
            span = pl.ds(pl.multiple_of(n * part, part), part)
            cos, sin = tables(extra, n)
            piece = product[half * part : (half + 1) * part]
            for j in range(q_width // head):
                u = piece[:, j * head : (j + 1) * head]
                q[span, pl.ds(j * head, head)] = turn(u * root_scale(u) * gain_q, cos, sin).astype(bf16)
            u = piece[:, q_width : q_width + head]
            kv[span, pl.ds(0, head)] = turn(u * root_scale(u) * gain_k, cos, sin).astype(bf16)
            kv[span, pl.ds(head, head)] = piece[:, q_width + head :].astype(bf16)

    kv_far = lines.start(kv, kvp, near[HIGH])
    for source, target in ((a, a_out), (raw, raw_out), (q, q_out), (kv, kv_out), (extra, extra_out), (gains, gains_out)):
        moves.save(source, target)
    for dc in (0, 1):
        w_out.pass_x(dc)
    for dc in (0, 1):
        w_gate.send_x(dc)
    kv_far.wait_recv()
    w_gate.send_z(1)
    c_own = [moves.start(c_hbm.at[seq[ds]], c.at[ds]) for ds in (0, 1)]
    c_core = [lines.start(c_hbm.at[seq[ds]], c.at[4 + ds], near[CORE]) for ds in (0, 1)]
    c_low = lines.start(c_hbm.at[seq[0]], c.at[2], near[LOW])
    w_up.ready()
    for dc in (0, 1):
        w_up.send_x(dc)
    moves.save(kvp, kvp_out)
    scaling = head ** (-0.5)

    @pl.loop(0, 2)
    def _(n):
        @pl.loop(0, 2)
        def _(m):
            base = pl.multiple_of(n * (4 * part) + m * part, part)
            keys = jnp.concatenate([pair_rows(kv, base, part, (0, head)), pair_rows(kvp, base, part, (0, head))], axis=0)
            values = jnp.concatenate(
                [pair_rows(kv, base, part, (head, 2 * head)), pair_rows(kvp, base, part, (head, 2 * head))], axis=0
            )
            allowed = allowed_pairs(at, n, m, part, q_width // head, extra)
            scores = jnp.where(allowed, nt(stack_heads(q, base, part, head), keys) * scaling, -jnp.inf)
            peak = jnp.max(scores, axis=-1, keepdims=True)
            weights = jnp.exp(scores - peak)
            total = jnp.sum(weights, axis=-1, keepdims=True)
            mixed = nn(weights.astype(bf16), values) / total
            unstack(o, base, part, head, mixed)
            unstack(lse, base, part, head, jnp.broadcast_to(peak + jnp.log(total), mixed.shape))

    moves.save(o, o_out)
    moves.save(lse, lse_out)
    w_out.complete()
    moves.save(w_o, wo_out)
    out = x
    lines.settle([*x_far, x_across])

    def project(first):
        @pl.loop(0, 4)
        def _(m):
            n = first + m
            span = pl.ds(pl.multiple_of(n * part, part), part)
            out[n] = nn(o[span, :], w_o[...]).astype(bf16)

    project(4)
    sent = {k: lines.start(out.at[4 + k], from_core.at[k], near[CORE]) for k in (3, 1, 2, 0)}
    project(0)

    def pump_gate():
        w_up.send_z(1)
        for dc in (0, 1):
            w_gate.pass_x(dc)
        w_down.ready()
        for dc in (0, 1):
            w_down.send_x(dc)
        return share(near, lines, c, c_low)

    sums, (c_far, c_across) = sum_lines(near, lines, out, sent, (from_core, kept, second_a, second_b, from_z, from_y, last_a, last_b), lambda: w_up.send_z(0), pump_gate)
    h[...] = h[...] + sums
    moves.save(h, h_out)
    wide = h[...]
    b_all[0] = (wide * root_scale(wide) * gains[1:2, :]).astype(bf16)

    def pump_up():
        for dc in (0, 1):
            w_down.send_z(dc)
        for dc in (0, 1):
            w_up.pass_x(dc)
        c_far.append(pass_on(near, lines, c, c_across))

    spread_lines(near, lines, b_all, from_z.shape[2], pump_up)
    moves.save(b_all, b_out)

    w_gate.complete()

    w_up.complete()
    moves.save(wgu, wgu_out)
    w_down.pass_x(0)

    @pl.loop(0, 4)
    def _(m):
        span = pl.ds(pl.multiple_of(m * rows, rows), rows)
        b = pair(b_all, m)
        g = nn(b, wgu[:, 0:hidden])
        u = nn(b, wgu[:, hidden : 2 * hidden])
        gu[span, pl.ds(0, hidden)] = g.astype(bf16)
        gu[span, pl.ds(hidden, hidden)] = u.astype(bf16)
        z[span, :] = (g * jax.nn.sigmoid(g) * u).astype(bf16)

    moves.save(z, z_out)
    moves.save(gu, gu_out)
    finish(c_own)
    arrive(c_core + c_far)
    moves.save(c, c_out)
    down = Grad(env, work_d, False, None, None, ())
    w_down.pass_x(1)
    eighths_of(down, 1, lambda run: tn(z[...], columns(c, run)))
    eighths_of(down, 0, lambda run: tn(z[...], columns(c, run)))
    moves.save(work_d, work_d_out)
    w_down.complete()
    moves.save(w_d, wd_out)
    lines.close()
    moves.close()


def share(near, lines, ref, low):
    low.wait_recv()
    across = lines.start(ref.at[2], ref.at[3], near[ACROSS])
    return [lines.start(ref.at[2], ref.at[6], near[CORE])], across


def pass_on(near, lines, ref, across):
    across.wait_recv()
    return lines.start(ref.at[3], ref.at[7], near[CORE])


def pair(ref, m):
    return jnp.concatenate([ref[2 * m], ref[2 * m + 1]], axis=0)


class Sum:
    def __init__(self, near, lines, part, first, rooms):
        self.near, self.lines, self.part, self.first = near, lines, part, first
        self.from_core, self.kept, self.second_a, self.second_b, self.from_z, self.from_y, self.last_a, self.last_b = rooms
        width, self.cut = part.shape[2], self.from_z.shape[2]
        self.a, self.b = pl.ds(0, self.cut), pl.ds(self.cut, width - self.cut)

    def total(self, k):
        self.first[k].wait_recv()
        return self.part[k].astype(f32) + self.from_core[k].astype(f32)

    def begin(self):
        lines, near, kept = self.lines, self.near, self.kept
        kept[2] = self.total(3).astype(bf16)
        self.y1 = lines.start(kept.at[2, :, self.b], self.from_y.at[1], near[ACROSS])
        self.z1 = lines.start(kept.at[2, :, self.a], self.from_z.at[1], near[LOW])
        kept[0] = self.total(1).astype(bf16)
        self.y0 = lines.start(kept.at[0, :, self.b], self.from_y.at[0], near[ACROSS])
        kept[1] = self.total(2).astype(bf16)
        self.z0 = lines.start(kept.at[1, :, self.a], self.from_z.at[0], near[LOW])

    def middle(self):
        lines, near, kept = self.lines, self.near, self.kept
        self.y1.wait_recv()
        self.second_b[...] = (kept[1, :, self.b].astype(f32) + self.from_y[1].astype(f32)).astype(bf16)
        self.z2 = lines.start(self.second_b, self.last_b, near[LOW])
        self.z1.wait_recv()
        self.second_a[...] = (kept[0, :, self.a].astype(f32) + self.from_z[1].astype(f32)).astype(bf16)
        self.y2 = lines.start(self.second_a, self.last_a, near[ACROSS])

    def end(self):
        arrive((self.z0, self.y0, self.y2, self.z2))
        self.lines.settle([self.z1, self.y1, self.y0, self.z0, self.y2, self.z2])
        left = self.from_z[0].astype(f32) + self.last_a[...].astype(f32)
        right = self.from_y[0].astype(f32) + self.last_b[...].astype(f32)
        return jnp.concatenate([left, right], axis=1)


def sum_lines(near, lines, part, first, rooms, early, pump):
    parts = Sum(near, lines, part, first, rooms)
    parts.begin()
    early()
    parts.middle()
    extra = pump()
    mine = parts.total(0)
    lines.settle(list(first.values()))
    return mine + parts.end(), extra


def spread_lines(near, lines, out, cut, pump):
    width = out.shape[2]
    a, b = pl.ds(0, cut), pl.ds(cut, width - cut)
    zb = lines.start(out.at[0, :, b], out.at[2, :, b], near[LOW])
    ya = lines.start(out.at[0, :, a], out.at[1, :, a], near[ACROSS])
    yb = lines.start(out.at[0, :, b], out.at[1, :, b], near[ACROSS])
    za = lines.start(out.at[0, :, a], out.at[2, :, a], near[LOW])
    c0 = lines.start(out.at[0], out.at[4], near[CORE])
    ya.wait_recv()
    zc = lines.start(out.at[1, :, a], out.at[3, :, a], near[LOW])
    zb.wait_recv()
    yc = lines.start(out.at[2, :, b], out.at[3, :, b], near[ACROSS])
    yb.wait_recv()
    c1 = lines.start(out.at[1], out.at[5], near[CORE])
    za.wait_recv()
    c2 = lines.start(out.at[2], out.at[6], near[CORE])
    zc.wait_recv()
    yc.wait_recv()
    c3 = lines.start(out.at[3], out.at[7], near[CORE])
    pump()
    arrive((c0, c1, c2, c3))
    return [ya, zb, yb, za, c0, zc, yc, c1, c2, c3]


class Grad:
    def __init__(self, env, work, by_rows, over_x, over_z, outs, span=slice(None)):
        self.env, self.work, self.by_rows, self.outs, self.span = env, work, by_rows, outs, span
        self.from_x, self.from_z = over_x, over_z
        self.x, self.z, self.last, self.local = {}, {}, [], []

    def index(self, dx, dzh, dc):
        spot = pl.ds(run_start(self.env.at, dx, dzh, dc, self.env.ctx_count, self.env.block), 2 * self.env.block)
        return (spot, self.span) if self.by_rows else (self.span, spot)

    def send_x(self, dzh, dc):
        self.x[dzh, dc] = self.env.lines.start(
            self.work.at[self.index(1, dzh, dc)], self.from_x.at[2 * dzh + dc], self.env.near[ACROSS_X]
        )

    def pass_z(self, dc):
        self.x[1, dc].wait_recv()
        spot = self.index(0, 1, dc)
        self.work[spot] = (self.work[spot].astype(f32) + self.from_x[2 + dc].astype(f32)).astype(bf16)
        self.z[dc] = self.env.lines.start(self.work.at[spot], self.from_z.at[dc], self.env.near[HIGH])

    def deliver(self, dc):
        at, block = self.env.at, self.env.block
        self.x[0, dc].wait_recv()
        self.z[dc].wait_recv()
        spot = self.index(0, 0, dc)
        self.work[spot] = (
            self.work[spot].astype(f32) + self.from_x[dc].astype(f32) + self.from_z[dc].astype(f32)
        ).astype(bf16)
        slot = at["c"] * 2 + at["zl"]
        for dzl, name in ((1, (LOW, DIAG)[dc]), (0, (None, CORE)[dc])):
            start = run_start(at, 0, 0, dc, self.env.ctx_count, block) + flip(at["zl"], dzl) * block
            mine = pl.ds(pl.multiple_of(start, block), block)
            for out, low, size in self.outs:
                there = pl.ds(pl.multiple_of(slot * size, 128), size)
                if self.by_rows:
                    source, target = self.work.at[mine, pl.ds(low, size)], out.at[:, there]
                else:
                    source, target = self.work.at[:, mine], out.at[there, :]
                if name is None:
                    self.local.append(self.env.moves.start(source, target))
                else:
                    self.last.append(self.env.lines.start(source, target, self.env.near[name]))

    def finish(self):
        arrive(self.last)
        finish(self.local)


def eighths_of(unit, dx, make):
    @pl.loop(0, 2)
    def _(dzh):
        @pl.loop(0, 2)
        def _(dc):
            at, count = unit.env.at, unit.env.ctx_count
            near_zh = at["zh"] + dzh - 2 * at["zh"] * dzh
            near_c = at["c"] + dc - 2 * at["c"] * dc
            start = ((flip(at["x"], dx) * 2 + near_c) * count + near_zh * 2) * unit.env.block
            spot = pl.ds(pl.multiple_of(start, 2 * unit.env.block), 2 * unit.env.block)
            value = make(spot).astype(bf16)
            if unit.by_rows:
                unit.work[spot, :] = value
            else:
                unit.work[:, spot] = value


def columns(ref, run):
    block = ref[:, :, run]
    return block.reshape(block.shape[0] * block.shape[1], block.shape[2])


def backward_kernel(
    ctx_count, block, head,
    x_hbm, a_hbm, raw_hbm, q_hbm, kv_hbm, kvp_hbm, o_hbm, lse_hbm, h_hbm, b_hbm, z_hbm, gu_hbm, c_hbm, extra_hbm, gains_hbm,
    wqkv_hbm, wo_hbm, wgu_hbm, wd_hbm, work_hbm,
    out_hbm, in_hbm, g_query, g_key, g_value, g_out, g_gate, g_up, g_down, small_out,
    c, wd, z, gu, wgu, b, q, kv, kvp, o, lse, raw, extra, gains, wqkv, wo, h, dh, x_mine, dq, dkv, dkvp, got, do, dqkv,
    work_d, work_o, work_q, rx_d, rz_d, rx_g, rz_g, rx_u, rz_u, rx_o, rz_o, rx_q, rz_q,
    from_core, kept, second_a, second_b, from_z, from_y, last_a, last_b, own_out, own_in, sums, small, rx_s, rz_s, ry_s,
    send, recv, local, ready, done, free,
):
    at = place()
    near = neighbours(at)
    lines, moves = Lines(send, recv), Moves(local)
    env = Env(at, near, lines, moves, ctx_count, block)
    part, width = c.shape[1], c.shape[2]
    q_width = q.shape[1]
    hidden = z.shape[1]
    rows = 2 * part
    scaling = head ** (-0.5)
    fetch = moves.start
    get_work = fetch(work_hbm, work_d)
    get_c, get_d, get_gu = fetch(c_hbm, c), fetch(wd_hbm, wd), fetch(gu_hbm, gu)
    get_w, get_b, get_z = fetch(wgu_hbm, wgu), fetch(b_hbm, b), fetch(z_hbm, z)
    get_more = [fetch(*p) for p in ((h_hbm, h), (gains_hbm, gains), (wo_hbm, wo), (o_hbm, o))]
    get_rest = [
        fetch(*p)
        for p in ((q_hbm, q), (kv_hbm, kv), (kvp_hbm, kvp), (lse_hbm, lse), (raw_hbm, raw), (extra_hbm, extra), (wqkv_hbm, wqkv))
    ]
    get_x = fetch(x_hbm.at[at["y"]], x_mine)
    meet_all(near, (CORE, LOW, ACROSS, DIAG, HIGH, ACROSS_X))
    down = Grad(env, work_d, False, rx_d, rz_d, ((g_down, 0, hidden),))
    gate = Grad(env, wgu, True, rx_g, rz_g, ((g_gate, 0, hidden),), pl.ds(0, hidden))
    up = Grad(env, wgu, True, rx_u, rz_u, ((g_up, hidden, hidden),), pl.ds(hidden, hidden))
    outward = Grad(env, work_o, False, rx_o, rz_o, ((g_out, 0, q_width),))
    inward = Grad(env, work_q, True, rx_q, rz_q, ((g_query, 0, q_width), (g_key, q_width, head), (g_value, q_width + head, head)))

    get_work.wait()
    for dc in (0, 1):
        down.send_x(1, dc)
    get_c.wait()
    get_d.wait()
    get_gu.wait()
    dh[...] = c[0].astype(f32)

    @pl.loop(0, 4)
    def _(m):
        span = pl.ds(pl.multiple_of(m * rows, rows), rows)
        dz = nt(pair(c, m), wd[...])
        g = gu[span, pl.ds(0, hidden)].astype(f32)
        u = gu[span, pl.ds(hidden, hidden)].astype(f32)
        s = jax.nn.sigmoid(g)
        gu[span, pl.ds(0, hidden)] = (dz * u * s * (1.0 + g * (1.0 - s))).astype(bf16)
        gu[span, pl.ds(hidden, hidden)] = (dz * g * s).astype(bf16)

    get_w.wait()

    def spill(first, source, weight, back):
        @pl.loop(0, 2)
        def _(m):
            n = first // 2 + m
            span = pl.ds(pl.multiple_of(n * rows, rows), rows)
            product = (nt if back else nn)(source[span, :], weight[...]).astype(bf16)
            c[2 * n] = product[:part]
            c[2 * n + 1] = product[part:]

    def to_core():
        return {k: lines.start(c.at[4 + k], from_core.at[k], near[CORE]) for k in (3, 1, 2, 0)}

    spill(4, gu, wgu, True)
    sent = to_core()
    spill(0, gu, wgu, True)
    get_b.wait()
    both = Grad(env, wgu, True, None, None, ())
    eighths_of(both, 1, lambda run: tn(columns(b, run), gu[...]))
    for unit in (gate, up):
        for dc in (0, 1):
            unit.send_x(1, dc)
    finish(get_more)
    rooms = (from_core, kept, second_a, second_b, from_z, from_y, last_a, last_b)

    def tell(flag):
        for name in (CORE, LOW, ACROSS):
            pl.semaphore_signal(flag, inc=1, device_id=near[name], device_id_type=MESH)

    def pump_gate():
        for dc in (0, 1):
            down.send_x(0, dc)
        for unit in (gate, up):
            for dc in (0, 1):
                unit.send_x(0, dc)
        eighths_of(both, 0, lambda run: tn(columns(b, run), gu[...]))
        tell(ready)
        down.pass_z(0)
        down.pass_z(1)

    db, _ = sum_lines(near, lines, c, sent, rooms, lambda: None, pump_gate)
    wide = h[...]
    r = root_scale(wide)
    n_m = wide * r
    sums[1:2, :] = jnp.sum(db * n_m, axis=0, keepdims=True)
    t = db * gains[1:2, :]
    middle = dh[...] + r * (t - n_m * jnp.mean(t * n_m, axis=-1, keepdims=True))
    dh[...] = middle
    pl.semaphore_wait(ready, 3)
    b[0] = middle.astype(bf16)

    def pump_spread():
        gate.pass_z(0)
        up.pass_z(0)

    spread = spread_lines(near, lines, b, from_z.shape[2], pump_spread)

    @pl.loop(0, 4)
    def _(m):
        span = pl.ds(pl.multiple_of(m * rows, rows), rows)
        do[span, :] = nt(pair(b, m), wo[...]).astype(bf16)

    finish(get_rest)

    @pl.loop(0, 2)
    def _(n):
        @pl.loop(0, 2)
        def _(m):
            base = pl.multiple_of(n * (4 * part) + m * part, part)
            query = stack_heads(q, base, part, head)
            mixed = stack_heads(o, base, part, head)
            grad = stack_heads(do, base, part, head)
            level = stack_heads(lse, base, part, head)[:, :1]
            keys = jnp.concatenate([pair_rows(kv, base, part, (0, head)), pair_rows(kvp, base, part, (0, head))], axis=0)
            values = jnp.concatenate(
                [pair_rows(kv, base, part, (head, 2 * head)), pair_rows(kvp, base, part, (head, 2 * head))], axis=0
            )
            allowed = allowed_pairs(at, n, m, part, q_width // head, extra)
            probs = jnp.where(allowed, jnp.exp(jnp.where(allowed, nt(query, keys) * scaling - level, 0.0)), 0.0)
            dv = tn(probs.astype(bf16), grad)
            row_dot = jnp.sum(grad.astype(f32) * mixed.astype(f32), axis=-1, keepdims=True)
            ds = (probs * (nt(grad, values) - row_dot)).astype(bf16)
            unstack(dq, base, part, head, nn(ds, keys) * scaling)
            dk = tn(ds, query) * scaling
            for ref, top in ((dkv, 0), (dkvp, 2 * part)):
                for i in (0, 1):
                    spot = pl.ds(base + i * 2 * part, part)
                    low = top + i * part
                    ref[spot, pl.ds(0, head)] = dk[low : low + part].astype(ref.dtype)
                    ref[spot, pl.ds(head, head)] = dv[low : low + part].astype(ref.dtype)

    kv_far = lines.start(dkvp, got, near[HIGH])
    get_z.wait()
    gate.pass_z(1)
    eighths_of(outward, 1, lambda run: tn(o[...], columns(b, run)))
    for dzh, dc in ((1, 0), (1, 1), (0, 0), (0, 1)):
        outward.send_x(dzh, dc)
    eighths_of(outward, 0, lambda run: tn(o[...], columns(b, run)))
    lines.settle(spread)
    get_a = fetch(a_hbm, b)

    spill(4, z, wd, False)
    sent = to_core()
    spill(0, z, wd, False)
    outer = Sum(near, lines, c, sent, rooms)
    outer.begin()
    up.pass_z(1)
    h[...] = h[...] + outer.total(0)
    lines.settle(list(sent.values()))
    tell(done)
    outer.middle()

    kv_far.wait_recv()
    gain_q = gains[2:3, 0:head]
    gain_k = gains[3:4, 0:head]

    def through(u, w, gain, cos, sin):
        scale = root_scale(u)
        n = u * scale
        e = turn_back(w, cos, sin)
        f = e * gain
        grad = (scale * (f - n * jnp.mean(f * n, axis=-1, keepdims=True))).astype(bf16)
        return grad, jnp.sum(e * n, axis=0, keepdims=True)

    sums[2:4, 0:head] = jnp.zeros((2, head), f32)

    @pl.loop(0, 8)
    def _(n):
        span = pl.ds(pl.multiple_of(n * part, part), part)
        cos, sin = tables(extra, n)
        for j in range(q_width // head):
            cols = pl.ds(j * head, head)
            dqkv[span, cols], add = through(raw[span, cols], dq[span, cols], gain_q, cos, sin)
            sums[2:3, 0:head] += add
        dk = dkv[span, pl.ds(0, head)] + got[span, pl.ds(0, head)].astype(f32)
        dv = dkv[span, pl.ds(head, head)] + got[span, pl.ds(head, head)].astype(f32)
        cols = pl.ds(q_width, head)
        dqkv[span, cols], add = through(raw[span, cols], dk, gain_k, cos, sin)
        sums[3:4, 0:head] += add
        dqkv[span, pl.ds(q_width + head, head)] = dv.astype(bf16)

    spill(4, dqkv, wqkv, True)
    pl.semaphore_wait(done, 3)
    sent = to_core()
    get_a.wait()
    eighths_of(inward, 1, lambda run: tn(columns(b, run), dqkv[...]))
    for dzh, dc in ((1, 0), (1, 1), (0, 0), (0, 1)):
        inward.send_x(dzh, dc)
    spill(0, dqkv, wqkv, True)
    own_out[...] = (h[...] + outer.end()).astype(bf16)
    tell(free)
    out_far = lines.start(own_out, out_hbm.at[at["y"]], near[ACROSS])
    moves.save(own_out, out_hbm.at[at["y"]])
    for dc in (0, 1):
        outward.pass_z(dc)
    get_x.wait()

    def pump_in():
        eighths_of(inward, 0, lambda run: tn(columns(b, run), dqkv[...]))
        for dc in (0, 1):
            inward.pass_z(dc)
        for dc in (0, 1):
            down.deliver(dc)

    pl.semaphore_wait(free, 3)
    da, _ = sum_lines(near, lines, c, sent, rooms, lambda: None, pump_in)
    wide = x_mine[...].astype(f32)
    r = root_scale(wide)
    n_a = wide * r
    sums[0:1, :] = jnp.sum(da * n_a, axis=0, keepdims=True)
    f = da * gains[0:1, :]
    own_in[...] = (dh[...] + r * (f - n_a * jnp.mean(f * n_a, axis=-1, keepdims=True))).astype(bf16)
    in_far = lines.start(own_in, in_hbm.at[at["y"]], near[ACROSS])
    moves.save(own_in, in_hbm.at[at["y"]])

    ranks = small.shape[0]
    for n in range(ranks):
        small[n, 0:2, :] = sums[0:2, n * block : (n + 1) * block]
        small[n, 2:4, :] = sums[2:4, 0:head]
        small[n, 4:8, :] = jnp.zeros((4, block), f32)

    def few(dx, dzh, dc):
        return pl.ds((flip(at["x"], dx) * 2 + flip(at["c"], dc)) * ctx_count + flip(at["zh"], dzh) * 2, 2)

    over_x = {k: lines.start(small.at[few(1, *k)], rx_s.at[2 * k[0] + k[1]], near[ACROSS_X]) for k in ((1, 0), (1, 1), (0, 0), (0, 1))}
    over_z = []
    for dc in (0, 1):
        over_x[1, dc].wait_recv()
        small[few(0, 1, dc)] += rx_s[2 + dc]
        over_z.append(lines.start(small.at[few(0, 1, dc)], rz_s.at[dc], near[HIGH]))
    for unit in (gate, up):
        for dc in (0, 1):
            unit.deliver(dc)
    for dc in (0, 1):
        over_x[0, dc].wait_recv()
        over_z[dc].wait_recv()
        small[few(0, 0, dc)] += rx_s[dc] + rz_s[dc]
    base = few(0, 0, 0).start
    side = few(0, 0, 1).start
    spread = [
        lines.start(small.at[base + 1 - at["zl"]], ry_s.at[0], near[LOW]),
        lines.start(small.at[side + at["zl"]], ry_s.at[1], near[CORE]),
        lines.start(small.at[side + 1 - at["zl"]], ry_s.at[2], near[DIAG]),
    ]
    for dc in (0, 1):
        outward.deliver(dc)
    arrive(spread)
    ry_s[3] = small[base + at["zl"]] + ry_s[0] + ry_s[1] + ry_s[2]
    across = lines.start(ry_s.at[3], ry_s.at[4], near[ACROSS])
    for dc in (0, 1):
        inward.deliver(dc)
    across.wait_recv()
    small_out[...] = ry_s[3] + ry_s[4]
    for unit in (down, gate, up, outward, inward):
        unit.finish()
    arrive((out_far, in_far))
    lines.close()
    moves.close()


def widen_kernel(count, *refs):
    source, target, narrow, wide = (refs[n * count : (n + 1) * count] for n in range(4))
    moves = Moves(refs[4 * count])
    begun = [moves.start(source[n], narrow[n]) for n in range(count)]
    for n in range(count):
        begun[n].wait()
        steps = 8
        rows = narrow[n].shape[0] // steps

        @pl.loop(0, steps)
        def _(m):
            span = pl.ds(pl.multiple_of(m * rows, rows), rows)
            wide[n][span, :] = narrow[n][span, :].astype(f32)

        moves.save(wide[n], target[n])
    moves.close()


VM = pl.BlockSpec(memory_space=pltpu.VMEM)
HB = pl.BlockSpec(memory_space=pl.ANY)


def shaped(shape, dtype):
    return jax.ShapeDtypeStruct(shape, dtype)


def split_device(
    block_input, doc_positions, out_cotangent, attn_gain, mlp_gain, query_gain, key_gain,
    w_query, w_key, w_value, w_out, w_gate, w_up, w_down,
):
    dp_count = lax.axis_size(DP)
    ctx_count = lax.axis_size(CTX)
    rank_count = dp_count * ctx_count
    at = place()
    rank = at[DP] * ctx_count + at[CTX]
    upper = at["y"] == 1
    seqs, part, width = block_input.shape
    block = attn_gain.shape[0]
    head_piece = query_gain.shape[0]
    head = head_piece * rank_count
    own_p = jnp.where(upper, doc_positions[::-1], doc_positions).astype(f32)
    inverse = rope_base ** (-2.0 * jnp.arange(head // 2).astype(f32) / head)
    angles = own_p[:, :, None] * inverse
    extra = jnp.stack(
        [jnp.concatenate([jnp.cos(angles), jnp.sin(angles)], axis=2), jnp.broadcast_to(own_p[:, :, None], (seqs, part, head))],
        axis=1,
    )
    small = jnp.stack([query_gain, key_gain]).astype(f32)
    small = lax.dynamic_update_slice(jnp.zeros((2, head), f32), small, (0, rank * head_piece))
    own_gains = jnp.concatenate([jnp.stack([attn_gain, mlp_gain]).astype(f32), small, jnp.zeros((4, block), f32)])

    tokens = 4 * seqs * part
    q_width = w_query.shape[1] // 4
    hidden = w_gate.shape[1] // 4
    bound = functools.partial
    eighths = (8, part, width)
    cut = width // 4
    sum_room = [
        pltpu.VMEM((4, part, width), bf16), pltpu.VMEM((3, part, width), bf16),
        pltpu.VMEM((part, cut), bf16), pltpu.VMEM((part, width - cut), bf16),
        pltpu.VMEM((2, part, cut), bf16), pltpu.VMEM((2, part, width - cut), bf16),
        pltpu.VMEM((part, cut), bf16), pltpu.VMEM((part, width - cut), bf16),
    ]
    shapes = {
        "a": ((tokens, width), bf16), "raw": ((tokens, q_width + head), f32), "q": ((tokens, q_width), bf16),
        "kv": ((tokens, 2 * head), bf16), "kvp": ((tokens, 2 * head), bf16), "o": ((tokens, q_width), bf16),
        "lse": ((tokens, q_width), f32), "h": ((part, width), f32), "b": (eighths, bf16), "z": ((tokens, hidden), bf16),
        "gu": ((tokens, 2 * hidden), bf16), "c": (eighths, bf16), "extra": ((8, 2, part, head), f32), "gains": ((8, width), f32),
        "wqkv": ((width, q_width + 2 * head), bf16), "wo": ((q_width, width), bf16),
        "wgu": ((width, 2 * hidden), bf16), "wd": ((hidden, width), bf16), "work": ((hidden, width), bf16),
    }
    room = {name: pltpu.VMEM(*spec) for name, spec in shapes.items()}
    kept = pl.pallas_call(
        bound(forward_kernel, ctx_count, block, head),
        out_shape=[shaped(*spec) for spec in shapes.values()],
        in_specs=[HB] * 11,
        out_specs=[HB] * len(shapes),
        scratch_shapes=[
            pltpu.VMEM(eighths, bf16), room["extra"], pltpu.VMEM((rank_count, 8, block), f32),
            room["wqkv"], room["wo"], room["wgu"], room["wd"], room["a"], room["raw"], room["q"], room["kv"], room["kvp"],
            room["o"], room["lse"], *sum_room,
            room["h"], room["b"], room["z"], room["gu"], room["c"], room["gains"], room["work"],
            pltpu.SemaphoreType.DMA((160,)), pltpu.SemaphoreType.DMA((160,)), pltpu.SemaphoreType.DMA((64,)),
        ],
        compiler_params=pltpu.CompilerParams(collective_id=0, has_side_effects=True, vmem_limit_bytes=63 * 1024 * 1024),
    )(block_input, out_cotangent, extra, own_gains, w_query, w_key, w_value, w_out, w_gate, w_up, w_down)
    kept = dict(zip(shapes, kept))
    pair_shape = (seqs, part, width)
    names = (
        "a", "raw", "q", "kv", "kvp", "o", "lse", "h", "b", "z", "gu", "c", "extra", "gains", "wqkv", "wo", "wgu", "wd", "work",
    )
    run = 2 * block
    vmem = pltpu.VMEM
    wide_q = q_width + 2 * head
    outs = pl.pallas_call(
        bound(backward_kernel, ctx_count, block, head),
        out_shape=[
            shaped(pair_shape, bf16), shaped(pair_shape, bf16),
            shaped(w_query.shape, bf16), shaped(w_key.shape, bf16), shaped(w_value.shape, bf16), shaped(w_out.shape, bf16),
            shaped(w_gate.shape, bf16), shaped(w_up.shape, bf16), shaped(w_down.shape, bf16), shaped((8, block), f32),
        ],
        in_specs=[HB] * (1 + len(names)),
        out_specs=[HB] * 9 + [VM],
        scratch_shapes=[
            *(room[k] for k in ("c", "wd", "z", "gu", "wgu", "b", "q", "kv", "kvp", "o", "lse", "raw", "extra", "gains", "wqkv", "wo", "h")),
            vmem((part, width), f32), vmem((part, width), bf16),
            vmem((tokens, q_width), f32), vmem((tokens, 2 * head), f32), vmem((tokens, 2 * head), bf16), vmem((tokens, 2 * head), bf16),
            vmem((tokens, q_width), bf16), vmem((tokens, wide_q), bf16),
            vmem((hidden, width), bf16), vmem((q_width, width), bf16), vmem((width, wide_q), bf16),
            vmem((4, hidden, run), bf16), vmem((2, hidden, run), bf16),
            vmem((4, run, hidden), bf16), vmem((2, run, hidden), bf16),
            vmem((4, run, hidden), bf16), vmem((2, run, hidden), bf16),
            vmem((4, q_width, run), bf16), vmem((2, q_width, run), bf16),
            vmem((4, run, wide_q), bf16), vmem((2, run, wide_q), bf16),
            *sum_room,
            vmem((part, width), bf16), vmem((part, width), bf16), vmem((8, width), f32),
            vmem((rank_count, 8, block), f32), vmem((4, 2, 8, block), f32), vmem((2, 2, 8, block), f32), vmem((5, 8, block), f32),
            pltpu.SemaphoreType.DMA((160,)), pltpu.SemaphoreType.DMA((160,)), pltpu.SemaphoreType.DMA((64,)),
            pltpu.SemaphoreType.REGULAR, pltpu.SemaphoreType.REGULAR, pltpu.SemaphoreType.REGULAR,
        ],
        compiler_params=pltpu.CompilerParams(collective_id=1, has_side_effects=True, vmem_limit_bytes=67043328),
    )(block_input, kept["a"].reshape(eighths), *(kept[k] for k in names[1:]))
    small = outs[9]
    slots = small[2:4].reshape(2, rank_count, head_piece)
    slots = lax.dynamic_index_in_dim(slots, rank, 1, keepdims=False)
    narrow = (outs[1].reshape(seqs * part, width), *outs[2:9])
    wide = pl.pallas_call(
        bound(widen_kernel, len(narrow)),
        out_shape=[shaped(array.shape, f32) for array in narrow],
        in_specs=[HB] * len(narrow),
        out_specs=[HB] * len(narrow),
        scratch_shapes=[
            *(vmem(array.shape, bf16) for array in narrow), *(vmem(array.shape, f32) for array in narrow),
            pltpu.SemaphoreType.DMA((2 * len(narrow),)),
        ],
        compiler_params=pltpu.CompilerParams(vmem_limit_bytes=48 * 1024 * 1024),
    )(*narrow)
    return (outs[0], wide[0].reshape(pair_shape), small[0], small[1], slots[0], slots[1], *wide[1:])


def rms_scale(value_rows):
    return lax.rsqrt(jnp.mean(value_rows * value_rows, axis=-1, keepdims=True) + eps_norm)


def rope_tables(places, head_size):
    half_size = head_size // 2
    inverse = rope_base ** (-2.0 * jnp.arange(half_size).astype(jnp.float32) / head_size)
    angles = places.astype(jnp.float32)[:, None] * inverse[None, :]
    angles = jnp.concatenate([angles, angles], axis=-1)
    return (jnp.cos(angles), jnp.sin(angles))


def rotate(values, cosine, sine):
    half_size = values.shape[-1] // 2
    turned = jnp.concatenate([-values[..., half_size:], values[..., :half_size]], axis=-1)
    return values * cosine[:, None, :] + turned * sine[:, None, :]


def rotate_back(grads, cosine, sine):
    half_size = grads.shape[-1] // 2
    weighted = grads * sine[:, None, :]
    return grads * cosine[:, None, :] + jnp.concatenate(
        [weighted[..., half_size:], -weighted[..., :half_size]], axis=-1
    )


def block_mask(query_index, lowest, key_index):
    return (key_index[None, :] <= query_index[:, None]) & (key_index[None, :] >= lowest[:, None])


def dot_nt(left, right):
    return lax.dot_general(
        left, right, (((1,), (1,)), ((), ())), preferred_element_type=jnp.float32
    )


def dot_tn(left, right):
    return lax.dot_general(
        left, right, (((0,), (0,)), ((), ())), preferred_element_type=jnp.float32
    )


def micro_pass(inputs_seq, places, cotangent, shards, totals):
    float_type = jnp.float32
    half_type = jnp.bfloat16
    fetched = (
        lax.all_gather(shards[0], (DP, CTX), axis=0, tiled=True),
        lax.all_gather(shards[1], (DP, CTX), axis=0, tiled=True),
        lax.all_gather(shards[2], (DP, CTX), axis=0, tiled=True),
        lax.all_gather(shards[3], (DP, CTX), axis=0, tiled=True),
        lax.all_gather(shards[4], (DP, CTX), axis=0, tiled=True),
        lax.all_gather(shards[5], (DP, CTX), axis=0, tiled=True),
        lax.all_gather(shards[6], (DP, CTX), axis=0, tiled=True),
        lax.all_gather(shards[7], (DP, CTX), axis=1, tiled=True),
        lax.all_gather(shards[8], (DP, CTX), axis=0, tiled=True),
        lax.all_gather(shards[9], (DP, CTX), axis=0, tiled=True),
        lax.all_gather(shards[10], (DP, CTX), axis=1, tiled=True),
    )
    gain_attn = fetched[0].astype(float_type)
    gain_mlp = fetched[1].astype(float_type)
    gain_query = fetched[2].astype(float_type)
    gain_key = fetched[3].astype(float_type)
    query_proj, key_proj, value_proj, out_proj, gate_proj, up_proj, down_proj = fetched[4:]
    head_size = gain_query.shape[0]
    head_count = query_proj.shape[1] // head_size
    kv_count = key_proj.shape[1] // head_size
    group_size = head_count // kv_count
    token_count = inputs_seq.shape[0]
    ctx_count = lax.axis_size(CTX)
    ctx_rank = lax.axis_index(CTX)
    scaling = head_size ** (-0.5)
    query_index = ctx_rank * token_count + jnp.arange(token_count, dtype=jnp.int32)
    lowest = query_index - places
    last_query = ctx_rank * token_count + token_count - 1
    residual_in = inputs_seq.astype(float_type)
    scale_attn = rms_scale(residual_in)
    normed_attn = residual_in * scale_attn
    attn_input = (normed_attn * gain_attn).astype(half_type)
    query_raw = jnp.dot(attn_input, query_proj, preferred_element_type=float_type).reshape(
        token_count, head_count, head_size
    )
    key_raw = jnp.dot(attn_input, key_proj, preferred_element_type=float_type).reshape(
        token_count, kv_count, head_size
    )
    value_rows = jnp.dot(attn_input, value_proj, preferred_element_type=float_type).astype(
        half_type
    )
    query_scale = rms_scale(query_raw)
    query_normed = query_raw * query_scale
    key_scale = rms_scale(key_raw)
    key_normed = key_raw * key_scale
    cosine, sine = rope_tables(places, head_size)
    query_rot = rotate(query_normed * gain_query, cosine, sine).astype(half_type)
    key_rot = (
        rotate(key_normed * gain_key, cosine, sine)
        .astype(half_type)
        .reshape(token_count, kv_count * head_size)
    )
    query_group = query_rot.reshape(token_count, kv_count, group_size, head_size)
    initial = (
        jnp.full((kv_count, group_size, token_count), -1e30, float_type),
        jnp.zeros((kv_count, group_size, token_count), float_type),
        jnp.zeros((token_count, kv_count, group_size, head_size), float_type),
    )
    pieces = (
        lax.all_gather(key_rot, CTX, axis=0, tiled=True),
        lax.all_gather(value_rows, CTX, axis=0, tiled=True),
    )
    row_count = pieces[0].shape[0]
    key_piece = pieces[0].reshape(row_count, kv_count, head_size)
    value_piece = pieces[1].reshape(row_count, kv_count, head_size)

    def fold_attend(state):
        peak, total, running = state
        scores = (
            jnp.einsum("qkgd,jkd->kgqj", query_group, key_piece, preferred_element_type=float_type)
            * scaling
        )
        allowed = block_mask(query_index, lowest, jnp.arange(row_count, dtype=jnp.int32))
        new_peak = jnp.maximum(peak, jnp.max(jnp.where(allowed, scores, -jnp.inf), axis=-1))
        weights = jnp.where(allowed, jnp.exp(scores - new_peak[..., None]), 0.0)
        total = jnp.sum(weights, axis=-1)
        running = jnp.einsum(
            "kgqj,jkd->qkgd",
            weights.astype(half_type),
            value_piece,
            preferred_element_type=float_type,
        )
        return (new_peak, total, running)

    peak, total, running = lax.cond(
        jnp.int32(0) <= last_query, fold_attend, lambda state: state, initial
    )
    attn_rows = (
        (running / jnp.transpose(total, (2, 0, 1))[..., None])
        .astype(half_type)
        .reshape(token_count, head_count * head_size)
    )
    log_total = peak + jnp.log(total)
    attn_out = lax.psum(
        jnp.dot(attn_rows, out_proj, preferred_element_type=float_type).astype(jnp.bfloat16), MP
    ).astype(jnp.float32)
    middle = residual_in + attn_out
    scale_mlp = rms_scale(middle)
    normed_mlp = middle * scale_mlp
    mlp_input = (normed_mlp * gain_mlp).astype(half_type)
    gate_rows = jnp.dot(mlp_input, gate_proj, preferred_element_type=float_type)
    up_rows = jnp.dot(mlp_input, up_proj, preferred_element_type=float_type)
    sigmoid_gate = jax.nn.sigmoid(gate_rows)
    hidden_rows = (gate_rows * sigmoid_gate * up_rows).astype(half_type)
    mlp_out = lax.psum(
        jnp.dot(hidden_rows, down_proj, preferred_element_type=float_type).astype(jnp.bfloat16),
        MP,
    ).astype(jnp.float32)
    block_output = (middle + mlp_out).astype(half_type)
    refetched = (
        lax.all_gather(shards[0], (DP, CTX), axis=0, tiled=True),
        lax.all_gather(shards[1], (DP, CTX), axis=0, tiled=True),
        lax.all_gather(shards[2], (DP, CTX), axis=0, tiled=True),
        lax.all_gather(shards[3], (DP, CTX), axis=0, tiled=True),
        lax.all_gather(shards[4], (DP, CTX), axis=0, tiled=True),
        lax.all_gather(shards[5], (DP, CTX), axis=0, tiled=True),
        lax.all_gather(shards[6], (DP, CTX), axis=0, tiled=True),
        lax.all_gather(shards[7], (DP, CTX), axis=1, tiled=True),
        lax.all_gather(shards[8], (DP, CTX), axis=0, tiled=True),
        lax.all_gather(shards[9], (DP, CTX), axis=0, tiled=True),
        lax.all_gather(shards[10], (DP, CTX), axis=1, tiled=True),
    )
    gain_attn = refetched[0].astype(float_type)
    gain_mlp = refetched[1].astype(float_type)
    gain_query = refetched[2].astype(float_type)
    gain_key = refetched[3].astype(float_type)
    query_proj, key_proj, value_proj, out_proj, gate_proj, up_proj, down_proj = refetched[4:]
    down_grad = dot_tn(hidden_rows, cotangent)
    hidden_grad = dot_nt(cotangent, down_proj)
    gate_grad = (
        hidden_grad * up_rows * sigmoid_gate * (1.0 + gate_rows * (1.0 - sigmoid_gate))
    ).astype(half_type)
    up_grad = (hidden_grad * gate_rows * sigmoid_gate).astype(half_type)
    gate_proj_grad = dot_tn(mlp_input, gate_grad)
    up_proj_grad = dot_tn(mlp_input, up_grad)
    mlp_in_grad = lax.psum(
        (dot_nt(gate_grad, gate_proj) + dot_nt(up_grad, up_proj)).astype(jnp.bfloat16), MP
    ).astype(jnp.float32)
    mlp_gain_grad = jnp.sum(mlp_in_grad * normed_mlp, axis=0)
    normed_grad = mlp_in_grad * gain_mlp
    middle_grad = cotangent.astype(float_type) + scale_mlp * (
        normed_grad - normed_mlp * jnp.mean(normed_grad * normed_mlp, axis=-1, keepdims=True)
    )
    middle_half = middle_grad.astype(half_type)
    out_proj_grad = dot_tn(attn_rows, middle_half)
    attn_grad = dot_nt(middle_half, out_proj).astype(half_type)
    grad_group = attn_grad.reshape(token_count, kv_count, group_size, head_size)
    attn_group = attn_rows.reshape(token_count, kv_count, group_size, head_size)
    row_dot = jnp.einsum(
        "qkgd,qkgd->kgq", grad_group, attn_group, preferred_element_type=float_type
    )
    key_back, value_back = (
        lax.all_gather(key_rot, CTX, axis=0, tiled=True),
        lax.all_gather(value_rows, CTX, axis=0, tiled=True),
    )

    def back_block(query_sum, block_id):
        start = block_id * token_count
        key_piece = lax.dynamic_slice_in_dim(key_back, start, token_count, 0).reshape(
            token_count, kv_count, head_size
        )
        value_piece = lax.dynamic_slice_in_dim(value_back, start, token_count, 0).reshape(
            token_count, kv_count, head_size
        )

        def back_attend(running):
            scores = (
                jnp.einsum(
                    "qkgd,jkd->kgqj", query_group, key_piece, preferred_element_type=float_type
                )
                * scaling
            )
            allowed = block_mask(
                query_index, lowest, start + jnp.arange(token_count, dtype=jnp.int32)
            )
            probs = jnp.where(allowed, jnp.exp(scores - log_total[..., None]), 0.0)
            value_part = jnp.einsum(
                "kgqj,qkgd->jkd",
                probs.astype(half_type),
                grad_group,
                preferred_element_type=float_type,
            )
            prob_grad = jnp.einsum(
                "qkgd,jkd->kgqj", grad_group, value_piece, preferred_element_type=float_type
            )
            score_half = (probs * (prob_grad - row_dot[..., None])).astype(half_type)
            query_part = (
                jnp.einsum(
                    "kgqj,jkd->qkgd", score_half, key_piece, preferred_element_type=float_type
                )
                * scaling
            )
            key_part = (
                jnp.einsum(
                    "kgqj,qkgd->jkd", score_half, query_group, preferred_element_type=float_type
                )
                * scaling
            )
            return (
                running + query_part,
                jnp.concatenate(
                    [
                        key_part.reshape(token_count, kv_count * head_size),
                        value_part.reshape(token_count, kv_count * head_size),
                    ],
                    axis=-1,
                ),
            )

        def passing(running):
            return (running, jnp.zeros((token_count, 2 * kv_count * head_size), float_type))

        return lax.cond(start <= last_query, back_attend, passing, query_sum)

    query_grad, kv_terms = lax.scan(
        back_block,
        jnp.zeros((token_count, kv_count, group_size, head_size), float_type),
        jnp.arange(ctx_count, dtype=jnp.int32),
    )
    kv_grad = lax.psum_scatter(
        kv_terms.reshape(ctx_count * token_count, 2 * kv_count * head_size).astype(jnp.bfloat16),
        CTX,
        scatter_dimension=0,
        tiled=True,
    ).astype(jnp.float32)
    key_rot_grad = kv_grad[:, : kv_count * head_size].reshape(token_count, kv_count, head_size)
    value_half = kv_grad[:, kv_count * head_size :].astype(half_type)
    query_back = rotate_back(query_grad.reshape(token_count, head_count, head_size), cosine, sine)
    key_grad_back = rotate_back(key_rot_grad, cosine, sine)
    query_gain_part = jnp.sum(query_back * query_normed, axis=(0, 1))
    key_gain_part = jnp.sum(key_grad_back * key_normed, axis=(0, 1))
    query_ngrad = query_back * gain_query
    key_ngrad = key_grad_back * gain_key
    query_half = (
        (
            query_scale
            * (
                query_ngrad
                - query_normed * jnp.mean(query_ngrad * query_normed, axis=-1, keepdims=True)
            )
        )
        .reshape(token_count, head_count * head_size)
        .astype(half_type)
    )
    key_half = (
        (
            key_scale
            * (key_ngrad - key_normed * jnp.mean(key_ngrad * key_normed, axis=-1, keepdims=True))
        )
        .reshape(token_count, kv_count * head_size)
        .astype(half_type)
    )
    query_proj_grad = dot_tn(attn_input, query_half)
    key_proj_grad = dot_tn(attn_input, key_half)
    value_proj_grad = dot_tn(attn_input, value_half)
    attn_in_grad, query_gain_sum, key_gain_sum = (
        lax.psum(
            (
                dot_nt(query_half, query_proj)
                + dot_nt(key_half, key_proj)
                + dot_nt(value_half, value_proj)
            ).astype(jnp.bfloat16),
            MP,
        ).astype(jnp.float32),
        lax.psum(query_gain_part.astype(jnp.bfloat16), MP).astype(jnp.float32),
        lax.psum(key_gain_part.astype(jnp.bfloat16), MP).astype(jnp.float32),
    )
    attn_gain_grad = jnp.sum(attn_in_grad * normed_attn, axis=0)
    normed_in_grad = attn_in_grad * gain_attn
    input_grad = middle_grad + scale_attn * (
        normed_in_grad
        - normed_attn * jnp.mean(normed_in_grad * normed_attn, axis=-1, keepdims=True)
    )
    addition = (
        attn_gain_grad,
        mlp_gain_grad,
        query_gain_sum,
        key_gain_sum,
        query_proj_grad,
        key_proj_grad,
        value_proj_grad,
        out_proj_grad,
        gate_proj_grad,
        up_proj_grad,
        down_grad,
    )
    totals = tuple((earlier + later for earlier, later in zip(totals, addition)))
    return (block_output, input_grad, totals)


def on_device(
    block_input,
    doc_positions,
    out_cotangent,
    attn_gain,
    mlp_gain,
    query_gain,
    key_gain,
    w_query,
    w_key,
    w_value,
    w_out,
    w_gate,
    w_up,
    w_down,
):
    shards = (
        attn_gain,
        mlp_gain,
        query_gain,
        key_gain,
        w_query,
        w_key,
        w_value,
        w_out,
        w_gate,
        w_up,
        w_down,
    )
    head_size = query_gain.shape[0] * lax.axis_size((DP, CTX))
    model_width = block_input.shape[2]
    query_width = w_query.shape[1]
    kv_width = w_key.shape[1]
    hidden_width = w_gate.shape[1]
    totals = (
        jnp.zeros((model_width,), jnp.float32),
        jnp.zeros((model_width,), jnp.float32),
        jnp.zeros((head_size,), jnp.float32),
        jnp.zeros((head_size,), jnp.float32),
        jnp.zeros((model_width, query_width), jnp.float32),
        jnp.zeros((model_width, kv_width), jnp.float32),
        jnp.zeros((model_width, kv_width), jnp.float32),
        jnp.zeros((query_width, model_width), jnp.float32),
        jnp.zeros((model_width, hidden_width), jnp.float32),
        jnp.zeros((model_width, hidden_width), jnp.float32),
        jnp.zeros((hidden_width, model_width), jnp.float32),
    )
    output_list = []
    grad_list = []
    for micro in range(block_input.shape[0]):
        output_rows, input_rows, totals = micro_pass(
            block_input[micro], doc_positions[micro], out_cotangent[micro], shards, totals
        )
        output_list.append(output_rows)
        grad_list.append(input_rows)
    owned = (
        lax.psum_scatter(totals[0], (DP, CTX), scatter_dimension=0, tiled=True),
        lax.psum_scatter(totals[1], (DP, CTX), scatter_dimension=0, tiled=True),
        lax.psum_scatter(totals[2], (DP, CTX), scatter_dimension=0, tiled=True),
        lax.psum_scatter(totals[3], (DP, CTX), scatter_dimension=0, tiled=True),
        lax.psum_scatter(totals[4], (DP, CTX), scatter_dimension=0, tiled=True),
        lax.psum_scatter(totals[5], (DP, CTX), scatter_dimension=0, tiled=True),
        lax.psum_scatter(totals[6], (DP, CTX), scatter_dimension=0, tiled=True),
        lax.psum_scatter(totals[7], (DP, CTX), scatter_dimension=1, tiled=True),
        lax.psum_scatter(totals[8], (DP, CTX), scatter_dimension=0, tiled=True),
        lax.psum_scatter(totals[9], (DP, CTX), scatter_dimension=0, tiled=True),
        lax.psum_scatter(totals[10], (DP, CTX), scatter_dimension=1, tiled=True),
    )
    return (
        jnp.stack(output_list),
        jnp.stack(grad_list),
        owned[0],
        owned[1],
        owned[2],
        owned[3],
        owned[4],
        owned[5],
        owned[6],
        owned[7],
        owned[8],
        owned[9],
        owned[10],
    )


def choose(mesh, arrays):
    dp, ctx, mp = mesh.shape[DP], mesh.shape[CTX], mesh.shape[MP]
    width = arrays[0].shape[2]
    paired = dp == 4 and ctx == 4 and mp == 2
    return split_device if paired and width % (dp * ctx * 128) == 0 else on_device


def solution(mesh):
    in_specs = (
        P(DP, CTX, None),
        P(DP, CTX),
        P(DP, CTX, None),
        P((DP, CTX)),
        P((DP, CTX)),
        P((DP, CTX)),
        P((DP, CTX)),
        P((DP, CTX), MP),
        P((DP, CTX), MP),
        P((DP, CTX), MP),
        P(MP, (DP, CTX)),
        P((DP, CTX), MP),
        P((DP, CTX), MP),
        P(MP, (DP, CTX)),
    )
    out_specs = (
        P(DP, CTX, None),
        P(DP, CTX, None),
        P((DP, CTX)),
        P((DP, CTX)),
        P((DP, CTX)),
        P((DP, CTX)),
        P((DP, CTX), MP),
        P((DP, CTX), MP),
        P((DP, CTX), MP),
        P(MP, (DP, CTX)),
        P((DP, CTX), MP),
        P((DP, CTX), MP),
        P(MP, (DP, CTX)),
    )

    def run(*arrays):
        return jax.shard_map(
            choose(mesh, arrays), mesh=mesh, in_specs=in_specs, out_specs=out_specs, check_vma=False
        )(*arrays)

    return run
```
